32 devices in a mesh: grp: 8 (over y, x, core), shard: 4 (over z).
Axes of the slice: x: 2, y: 2, z: 4, core: 2. Of those that a mesh axis runs over, the one named last changes fastest.
Arguments:
- hidden_states: bfloat16 [16384, 1024], P(('grp', 'shard')), may hold values from -6 to 6
- output_cotangent: bfloat16 [16384, 1024], P(('grp', 'shard')), may hold values from -6 to 6
- first_gain: float32 [1024], P('shard'), may hold values from 0.5 to 1.5
- first_bias: float32 [1024], P('shard'), may hold values from -0.1875 to 0.1875
- second_gain: float32 [1024], P('shard'), may hold values from 0.5 to 1.5
- second_bias: float32 [1024], P('shard'), may hold values from -0.1875 to 0.1875
- triple_weight: float32 [1024, 3072], P('shard'), may hold values from -0.1875 to 0.1875
- triple_bias: float32 [3072], P('shard'), may hold values from -0.1875 to 0.1875
- output_weight: float32 [1024, 1024], P('shard'), may hold values from -0.5 to 0.5
- output_bias: float32 [1024], P('shard'), may hold values from -0.1875 to 0.1875
- expand_weight: float32 [1024, 4096], P('shard'), may hold values from -0.1875 to 0.1875
- expand_bias: float32 [4096], P('shard'), may hold values from -0.1875 to 0.1875
- shrink_weight: float32 [4096, 1024], P('shard'), may hold values from -0.09375 to 0.09375
- shrink_bias: float32 [1024], P('shard'), may hold values from -0.1875 to 0.1875
- first_gain_momentum: float32 [1024], P('shard'), may hold values from -6 to 6
- first_bias_momentum: float32 [1024], P('shard'), may hold values from -6 to 6
- second_gain_momentum: float32 [1024], P('shard'), may hold values from -6 to 6
- second_bias_momentum: float32 [1024], P('shard'), may hold values from -6 to 6
- triple_weight_momentum: float32 [1024, 3072], P('shard'), may hold values from -6 to 6
- triple_bias_momentum: float32 [3072], P('shard'), may hold values from -6 to 6
- output_weight_momentum: float32 [1024, 1024], P('shard'), may hold values from -6 to 6
- output_bias_momentum: float32 [1024], P('shard'), may hold values from -6 to 6
- expand_weight_momentum: float32 [1024, 4096], P('shard'), may hold values from -6 to 6
- expand_bias_momentum: float32 [4096], P('shard'), may hold values from -6 to 6
- shrink_weight_momentum: float32 [4096, 1024], P('shard'), may hold values from -6 to 6
- shrink_bias_momentum: float32 [1024], P('shard'), may hold values from -6 to 6
- first_gain_variance: float32 [1024], P('shard'), may hold values from 163.84 to 3276.8
- first_bias_variance: float32 [1024], P('shard'), may hold values from 1 to 10
- second_gain_variance: float32 [1024], P('shard'), may hold values from 163.84 to 3276.8
- second_bias_variance: float32 [1024], P('shard'), may hold values from 1 to 10
- triple_weight_variance: float32 [1024, 3072], P('shard'), may hold values from 1 to 10
- triple_bias_variance: float32 [3072], P('shard'), may hold values from 1 to 10
- output_weight_variance: float32 [1024, 1024], P('shard'), may hold values from 1 to 10
- output_bias_variance: float32 [1024], P('shard'), may hold values from 1 to 10
- expand_weight_variance: float32 [1024, 4096], P('shard'), may hold values from 1 to 10
- expand_bias_variance: float32 [4096], P('shard'), may hold values from 1 to 10
- shrink_weight_variance: float32 [4096, 1024], P('shard'), may hold values from 1 to 10
- shrink_bias_variance: float32 [1024], P('shard'), may hold values from 1 to 10
Outputs:
- block_output: bfloat16 [16384, 1024], P(('grp', 'shard'))
- input_gradient: bfloat16 [16384, 1024], P(('grp', 'shard'))
- first_gain_gradient: float32 [1024], P('shard')
- first_bias_gradient: float32 [1024], P('shard')
- second_gain_gradient: float32 [1024], P('shard')
- second_bias_gradient: float32 [1024], P('shard')
- triple_weight_gradient: float32 [1024, 3072], P('shard')
- triple_bias_gradient: float32 [3072], P('shard')
- output_weight_gradient: float32 [1024, 1024], P('shard')
- output_bias_gradient: float32 [1024], P('shard')
- expand_weight_gradient: float32 [1024, 4096], P('shard')
- expand_bias_gradient: float32 [4096], P('shard')
- shrink_weight_gradient: float32 [4096, 1024], P('shard')
- shrink_bias_gradient: float32 [1024], P('shard')
- first_gain_change: float32 [1024], P('shard')
- first_bias_updated: float32 [1024], P('shard')
- second_gain_change: float32 [1024], P('shard')
- second_bias_updated: float32 [1024], P('shard')
- triple_weight_updated: float32 [1024, 3072], P('shard')
- triple_bias_updated: float32 [3072], P('shard')
- output_weight_updated: float32 [1024, 1024], P('shard')
- output_bias_updated: float32 [1024], P('shard')
- expand_weight_updated: float32 [1024, 4096], P('shard')
- expand_bias_updated: float32 [4096], P('shard')
- shrink_weight_updated: float32 [4096, 1024], P('shard')
- shrink_bias_updated: float32 [1024], P('shard')
- first_gain_momentum_updated: float32 [1024], P('shard')
- first_bias_momentum_updated: float32 [1024], P('shard')
- second_gain_momentum_updated: float32 [1024], P('shard')
- second_bias_momentum_updated: float32 [1024], P('shard')
- triple_weight_momentum_updated: float32 [1024, 3072], P('shard')
- triple_bias_momentum_updated: float32 [3072], P('shard')
- output_weight_momentum_updated: float32 [1024, 1024], P('shard')
- output_bias_momentum_updated: float32 [1024], P('shard')
- expand_weight_momentum_updated: float32 [1024, 4096], P('shard')
- expand_bias_momentum_updated: float32 [4096], P('shard')
- shrink_weight_momentum_updated: float32 [4096, 1024], P('shard')
- shrink_bias_momentum_updated: float32 [1024], P('shard')
- first_gain_variance_updated: float32 [1024], P('shard')
- first_bias_variance_updated: float32 [1024], P('shard')
- second_gain_variance_updated: float32 [1024], P('shard')
- second_bias_variance_updated: float32 [1024], P('shard')
- triple_weight_variance_updated: float32 [1024, 3072], P('shard')
- triple_bias_variance_updated: float32 [3072], P('shard')
- output_weight_variance_updated: float32 [1024, 1024], P('shard')
- output_bias_variance_updated: float32 [1024], P('shard')
- expand_weight_variance_updated: float32 [1024, 4096], P('shard')
- expand_bias_variance_updated: float32 [4096], P('shard')
- shrink_weight_variance_updated: float32 [4096, 1024], P('shard')
- shrink_bias_variance_updated: float32 [1024], P('shard')
The draws below stay inside these ranges and needn't reach their ends.
All inputs are finite; a program needn't handle non-finite values.
Results may differ from the reference program's by a relative error of at most 0.006.
The reference program's roundings to bfloat16 on the way count: a program that leaves them out, or rounds other values in their place, can miss the bound.
Values may be sent and summed in bfloat16 or wider, within the bound.
A program may use at most 320 MiB of HBM per device.

```python
import math
import jax
import jax.numpy as jnp
from jax import lax

D = 1024
HEAD_DIM = 64
FF = 4096
ROTARY = 16
LEN = 512
STEP = 10
SEQS = 32
TOKENS = 16384


def block_levels(stream_key, dims, shards, low, high):
    loudness, own = 1.0, jax.random.fold_in(stream_key, 6)
    for dim, parts in shards:
        draws = jnp.exp(jax.random.uniform(jax.random.fold_in(own, dim), (parts,), jnp.float32, low / len(shards), high / len(shards)))
        loudness = loudness * jnp.repeat(draws, dims[dim] // parts).reshape([-1 if axis == dim else 1 for axis in range(len(dims))])
    return loudness


def scatter_about(stream_key, extent, spread, bound, cuts=(), held_as=jnp.bfloat16):
    loudness = block_levels(stream_key, extent, cuts, -0.22, 0.18) if cuts else 1.0
    values = jax.random.normal(stream_key, extent, jnp.float32) * spread * loudness
    return jnp.minimum(jnp.maximum(values, -bound), bound).astype(held_as)


def setup_inputs(seed: int = 0) -> dict:
    key_of = jax.random.split(jax.random.key(seed), 39)
    hidden_states = scatter_about(key_of[0], (TOKENS, D), 1.0, 6.0, ((0, 32),))
    output_cotangent = scatter_about(key_of[1], (TOKENS, D), 1.0, 6.0, ((0, 32),))
    first_gain = jnp.clip(1.0 + 0.1 * jax.random.normal(key_of[2], (D,), jnp.float32), 0.5, 1.5)
    first_bias = scatter_about(key_of[3], (D,), 0.03, 0.1875, ((0, 4),), jnp.float32)
    second_gain = jnp.clip(1.0 + 0.1 * jax.random.normal(key_of[4], (D,), jnp.float32), 0.5, 1.5)
    second_bias = scatter_about(key_of[5], (D,), 0.03, 0.1875, ((0, 4),), jnp.float32)
    triple_weight = scatter_about(key_of[6], (D, 3 * D), D ** -0.5, 0.1875, ((0, 4),), jnp.float32)
    triple_bias = scatter_about(key_of[7], (3 * D,), 0.03, 0.1875, ((0, 4),), jnp.float32)
    output_weight = scatter_about(key_of[8], (D, D), (D // 8) ** -0.5, 0.5, ((0, 4),), jnp.float32)
    output_bias = scatter_about(key_of[9], (D,), 0.03, 0.1875, ((0, 4),), jnp.float32)
    expand_weight = scatter_about(key_of[10], (D, FF), D ** -0.5, 0.1875, ((0, 4),), jnp.float32)
    expand_bias = scatter_about(key_of[11], (FF,), 0.03, 0.1875, ((0, 4),), jnp.float32)
    shrink_weight = scatter_about(key_of[12], (FF, D), FF ** -0.5, 0.09375, ((0, 4),), jnp.float32)
    shrink_bias = scatter_about(key_of[13], (D,), 0.03, 0.1875, ((0, 4),), jnp.float32)
    first_gain_momentum = scatter_about(key_of[14], (D,), 1.0, 6.0, ((0, 4),), jnp.float32)
    first_bias_momentum = scatter_about(key_of[15], (D,), 1.0, 6.0, ((0, 4),), jnp.float32)
    second_gain_momentum = scatter_about(key_of[16], (D,), 1.0, 6.0, ((0, 4),), jnp.float32)
    second_bias_momentum = scatter_about(key_of[17], (D,), 1.0, 6.0, ((0, 4),), jnp.float32)
    triple_weight_momentum = scatter_about(key_of[18], (D, 3 * D), 1.0, 6.0, ((0, 4),), jnp.float32)
    triple_bias_momentum = scatter_about(key_of[19], (3 * D,), 1.0, 6.0, ((0, 4),), jnp.float32)
    output_weight_momentum = scatter_about(key_of[20], (D, D), 1.0, 6.0, ((0, 4),), jnp.float32)
    output_bias_momentum = scatter_about(key_of[21], (D,), 1.0, 6.0, ((0, 4),), jnp.float32)
    expand_weight_momentum = scatter_about(key_of[22], (D, FF), 1.0, 6.0, ((0, 4),), jnp.float32)
    expand_bias_momentum = scatter_about(key_of[23], (FF,), 1.0, 6.0, ((0, 4),), jnp.float32)
    shrink_weight_momentum = scatter_about(key_of[24], (FF, D), 1.0, 6.0, ((0, 4),), jnp.float32)
    shrink_bias_momentum = scatter_about(key_of[25], (D,), 1.0, 6.0, ((0, 4),), jnp.float32)
    first_gain_variance = jnp.clip(jnp.exp(math.log(3276.8) - 2.9957323 * jax.random.uniform(key_of[26], (D,), jnp.float32) ** block_levels(key_of[26], (D,), ((0, 4),), -0.2, 0.2)), 163.84, 3276.8)
    first_bias_variance = jnp.clip(jnp.exp(math.log(10.0) - 2.3025851 * jax.random.uniform(key_of[27], (D,), jnp.float32) ** block_levels(key_of[27], (D,), ((0, 4),), -0.2, 0.2)), 1.0, 10.0)
    second_gain_variance = jnp.clip(jnp.exp(math.log(3276.8) - 2.9957323 * jax.random.uniform(key_of[28], (D,), jnp.float32) ** block_levels(key_of[28], (D,), ((0, 4),), -0.2, 0.2)), 163.84, 3276.8)
    second_bias_variance = jnp.clip(jnp.exp(math.log(10.0) - 2.3025851 * jax.random.uniform(key_of[29], (D,), jnp.float32) ** block_levels(key_of[29], (D,), ((0, 4),), -0.2, 0.2)), 1.0, 10.0)
    triple_weight_variance = jnp.clip(jnp.exp(math.log(10.0) - 2.3025851 * jax.random.uniform(key_of[30], (D, 3 * D), jnp.float32) ** block_levels(key_of[30], (D, 3 * D), ((0, 4),), -0.2, 0.2)), 1.0, 10.0)
    triple_bias_variance = jnp.clip(jnp.exp(math.log(10.0) - 2.3025851 * jax.random.uniform(key_of[31], (3 * D,), jnp.float32) ** block_levels(key_of[31], (3 * D,), ((0, 4),), -0.2, 0.2)), 1.0, 10.0)
    output_weight_variance = jnp.clip(jnp.exp(math.log(10.0) - 2.3025851 * jax.random.uniform(key_of[32], (D, D), jnp.float32) ** block_levels(key_of[32], (D, D), ((0, 4),), -0.2, 0.2)), 1.0, 10.0)
    output_bias_variance = jnp.clip(jnp.exp(math.log(10.0) - 2.3025851 * jax.random.uniform(key_of[33], (D,), jnp.float32) ** block_levels(key_of[33], (D,), ((0, 4),), -0.2, 0.2)), 1.0, 10.0)
    expand_weight_variance = jnp.clip(jnp.exp(math.log(10.0) - 2.3025851 * jax.random.uniform(key_of[34], (D, FF), jnp.float32) ** block_levels(key_of[34], (D, FF), ((0, 4),), -0.2, 0.2)), 1.0, 10.0)
    expand_bias_variance = jnp.clip(jnp.exp(math.log(10.0) - 2.3025851 * jax.random.uniform(key_of[35], (FF,), jnp.float32) ** block_levels(key_of[35], (FF,), ((0, 4),), -0.2, 0.2)), 1.0, 10.0)
    shrink_weight_variance = jnp.clip(jnp.exp(math.log(10.0) - 2.3025851 * jax.random.uniform(key_of[36], (FF, D), jnp.float32) ** block_levels(key_of[36], (FF, D), ((0, 4),), -0.2, 0.2)), 1.0, 10.0)
    shrink_bias_variance = jnp.clip(jnp.exp(math.log(10.0) - 2.3025851 * jax.random.uniform(key_of[37], (D,), jnp.float32) ** block_levels(key_of[37], (D,), ((0, 4),), -0.2, 0.2)), 1.0, 10.0)
    return dict(hidden_states=hidden_states, output_cotangent=output_cotangent, first_gain=first_gain, first_bias=first_bias, second_gain=second_gain, second_bias=second_bias, triple_weight=triple_weight, triple_bias=triple_bias, output_weight=output_weight, output_bias=output_bias, expand_weight=expand_weight, expand_bias=expand_bias, shrink_weight=shrink_weight, shrink_bias=shrink_bias, first_gain_momentum=first_gain_momentum, first_bias_momentum=first_bias_momentum, second_gain_momentum=second_gain_momentum, second_bias_momentum=second_bias_momentum, triple_weight_momentum=triple_weight_momentum, triple_bias_momentum=triple_bias_momentum, output_weight_momentum=output_weight_momentum, output_bias_momentum=output_bias_momentum, expand_weight_momentum=expand_weight_momentum, expand_bias_momentum=expand_bias_momentum, shrink_weight_momentum=shrink_weight_momentum, shrink_bias_momentum=shrink_bias_momentum, first_gain_variance=first_gain_variance, first_bias_variance=first_bias_variance, second_gain_variance=second_gain_variance, second_bias_variance=second_bias_variance, triple_weight_variance=triple_weight_variance, triple_bias_variance=triple_bias_variance, output_weight_variance=output_weight_variance, output_bias_variance=output_bias_variance, expand_weight_variance=expand_weight_variance, expand_bias_variance=expand_bias_variance, shrink_weight_variance=shrink_weight_variance, shrink_bias_variance=shrink_bias_variance)


highest = lax.Precision.HIGHEST
eps_norm = 1e-05
rope_base = 10000.0
beta_one = 0.9
beta_two = 0.95
learn_rate = 0.01
adam_eps = 1e-08
weight_decay = 0.01

@jax.custom_vjp
def low(v):
    return lax.optimization_barrier(v.astype(jnp.bfloat16)).astype(jnp.float32)

@jax.custom_vjp
def low_back(v):
    return v

def low_keep(v):
    return (low(v), None)

def low_pass(kept, grad):
    return (grad,)

def back_keep(v):
    return (v, None)

def back_low(kept, grad):
    return (low(grad),)
low.defvjp(low_keep, low_pass)
low_back.defvjp(back_keep, back_low)

def normalize(entries, gain_vec, shift_vec):
    centered = entries - lax.optimization_barrier(jnp.mean(entries, -1, keepdims=True))
    variance_row = lax.optimization_barrier(jnp.mean(centered * centered, -1, keepdims=True))
    return centered * lax.rsqrt(variance_row + eps_norm) * gain_vec + shift_vec

def rotary_tables(seq_length):
    position = jnp.arange(seq_length).astype(jnp.float32)[:, None]
    half_rotary = ROTARY // 2
    inverse_freq = rope_base ** (-(jnp.arange(half_rotary).astype(jnp.float32) * 2.0 / ROTARY))
    angles = position * inverse_freq[None, :]
    return (jnp.cos(angles), jnp.sin(angles))

def rotate(tensor, cosine_table, sine_table):
    half_rotary = ROTARY // 2
    first_part = tensor[..., :half_rotary]
    second = tensor[..., half_rotary:ROTARY]
    remain = tensor[..., ROTARY:]
    cos_rows = cosine_table[:, None, :]
    sin_rows = sine_table[:, None, :]
    return jnp.concatenate([first_part * cos_rows - second * sin_rows, second * cos_rows + first_part * sin_rows, remain], -1)

def project(left_side, right_side):
    return jnp.einsum('...d,de->...e', left_side, right_side, precision=highest)

def attend(queries, keys, values):
    batch_size = queries.shape[0]
    seq_length = queries.shape[1]
    block_rows = min(512, seq_length)
    block_count = seq_length // block_rows
    score_scale = 1.0 / math.sqrt(HEAD_DIM)

    def one_block(block_index):
        row_start = block_index * block_rows
        rows_query = lax.dynamic_slice_in_dim(queries, row_start, block_rows, 1)
        scores = low_back(jnp.einsum('bqhe,bkhe->bhqk', rows_query, keys, precision=highest) * score_scale)
        row_pos = row_start + jnp.arange(block_rows).astype(jnp.int32)
        col_pos = jnp.arange(seq_length).astype(jnp.int32)
        allowed = col_pos[None, :] <= row_pos[:, None]
        scores = jnp.where(allowed, scores, -1e+30)
        probs = low(jax.nn.softmax(scores, axis=-1))
        return jnp.einsum('bhqk,bkhe->bqhe', probs, values, precision=highest)
    blocks = lax.map(jax.checkpoint(one_block), jnp.arange(block_count).astype(jnp.int32))
    return jnp.moveaxis(blocks, 0, 1).reshape(batch_size, seq_length, -1)

def forward(weights, inputs):
    first_gain, first_bias, second_gain, second_bias, triple_weight, triple_bias, output_weight, output_bias, expand_weight, expand_bias, shrink_weight, shrink_bias = tuple((low(item) for item in weights))
    batch_size, seq_length, model_width = inputs.shape
    head_count = model_width // HEAD_DIM
    normed_one = low(normalize(inputs, first_gain, first_bias))
    normed_two = low(normalize(inputs, second_gain, second_bias))
    triple = low_back(project(normed_one, triple_weight) + triple_bias)
    cosine_table, sine_table = rotary_tables(seq_length)
    head_shape = (batch_size, seq_length, head_count, HEAD_DIM)
    queries = low(rotate(triple[..., :model_width].reshape(head_shape), cosine_table, sine_table))
    keys = low(rotate(triple[..., model_width:2 * model_width].reshape(head_shape), cosine_table, sine_table))
    values = low(triple[..., 2 * model_width:].reshape(head_shape))
    context = low_back(low(attend(queries, keys, values)))
    attention = project(context, output_weight) + output_bias
    hidden = low_back(project(normed_two, expand_weight) + expand_bias)
    activated = low(jax.nn.gelu(hidden, approximate=False))
    feed = project(activated, shrink_weight) + shrink_bias
    return inputs + attention + feed

def adam_step(weight, gradient, momentum, variance, decayed):
    momentum_new = beta_one * momentum + (1.0 - beta_one) * gradient
    variance_new = beta_two * variance + (1.0 - beta_two) * gradient * gradient
    mean_hat = momentum_new / (1.0 - beta_one ** STEP)
    var_hat = variance_new / (1.0 - beta_two ** STEP)
    change = mean_hat / (jnp.sqrt(var_hat) + adam_eps)
    if decayed:
        change = change + weight_decay * weight
    delta = -learn_rate * change
    return (weight + delta, delta, momentum_new, variance_new)

def reference(hidden_states, output_cotangent, first_gain, first_bias, second_gain, second_bias, triple_weight, triple_bias, output_weight, output_bias, expand_weight, expand_bias, shrink_weight, shrink_bias, first_gain_momentum, first_bias_momentum, second_gain_momentum, second_bias_momentum, triple_weight_momentum, triple_bias_momentum, output_weight_momentum, output_bias_momentum, expand_weight_momentum, expand_bias_momentum, shrink_weight_momentum, shrink_bias_momentum, first_gain_variance, first_bias_variance, second_gain_variance, second_bias_variance, triple_weight_variance, triple_bias_variance, output_weight_variance, output_bias_variance, expand_weight_variance, expand_bias_variance, shrink_weight_variance, shrink_bias_variance):
    weights = (first_gain, first_bias, second_gain, second_bias, triple_weight, triple_bias, output_weight, output_bias, expand_weight, expand_bias, shrink_weight, shrink_bias)
    weights = tuple((item.astype(jnp.float32) for item in weights))
    momenta = (first_gain_momentum, first_bias_momentum, second_gain_momentum, second_bias_momentum, triple_weight_momentum, triple_bias_momentum, output_weight_momentum, output_bias_momentum, expand_weight_momentum, expand_bias_momentum, shrink_weight_momentum, shrink_bias_momentum)
    variances = (first_gain_variance, first_bias_variance, second_gain_variance, second_bias_variance, triple_weight_variance, triple_bias_variance, output_weight_variance, output_bias_variance, expand_weight_variance, expand_bias_variance, shrink_weight_variance, shrink_bias_variance)
    group_size = max(1, min(SEQS, 4096 // LEN))
    inputs = hidden_states.astype(jnp.float32).reshape(SEQS // group_size, group_size, LEN, D)
    cotangent = output_cotangent.astype(jnp.float32).reshape(SEQS // group_size, group_size, LEN, D)

    def accumulate(totals, pair):
        group_in, group_cot = pair
        result, pullback = jax.vjp(forward, weights, group_in)
        weight_grads, input_grads = pullback(group_cot)
        totals = tuple((left_term + right_term for left_term, right_term in zip(totals, weight_grads)))
        return (totals, (result, input_grads))
    start_totals = tuple((jnp.zeros(item.shape, jnp.float32) for item in weights))
    gradients, (results, input_grads) = lax.scan(accumulate, start_totals, (inputs, cotangent))
    block_output = results.reshape(TOKENS, D).astype(jnp.bfloat16)
    input_gradient = input_grads.reshape(TOKENS, D).astype(jnp.bfloat16)
    updated = []
    moment_one = []
    moment_two = []
    for position_index in range(12):
        new_weight, delta, new_momentum, new_variance = adam_step(weights[position_index], gradients[position_index], momenta[position_index], variances[position_index], position_index in (4, 6, 8, 10))
        if position_index in (0, 2):
            updated.append(delta)
        else:
            updated.append(new_weight)
        moment_one.append(new_momentum)
        moment_two.append(new_variance)
    return (block_output, input_gradient, gradients[0], gradients[1], gradients[2], gradients[3], gradients[4], gradients[5], gradients[6], gradients[7], gradients[8], gradients[9], gradients[10], gradients[11], updated[0], updated[1], updated[2], updated[3], updated[4], updated[5], updated[6], updated[7], updated[8], updated[9], updated[10], updated[11], moment_one[0], moment_one[1], moment_one[2], moment_one[3], moment_one[4], moment_one[5], moment_one[6], moment_one[7], moment_one[8], moment_one[9], moment_one[10], moment_one[11], moment_two[0], moment_two[1], moment_two[2], moment_two[3], moment_two[4], moment_two[5], moment_two[6], moment_two[7], moment_two[8], moment_two[9], moment_two[10], moment_two[11])
```

```python
import math

import jax
import jax.numpy as jnp
from jax import lax
from jax.experimental import pallas as pl
from jax.experimental.pallas import tpu as pltpu
from jax.sharding import Mesh, PartitionSpec as P

HEAD_DIM = 64
ROTARY = 16
STEP = 10
eps_norm = 1e-05
rope_base = 10000.0
beta_one = 0.9
beta_two = 0.95
learn_rate = 0.01
adam_eps = 1e-08
weight_decay = 0.01

bf16 = jnp.bfloat16
f32 = jnp.float32


def adam_step(weight, gradient, momentum, variance, decayed):
    momentum_new = beta_one * momentum + (1.0 - beta_one) * gradient
    variance_new = beta_two * variance + (1.0 - beta_two) * gradient * gradient
    mean_hat = momentum_new / (1.0 - beta_one**STEP)
    var_hat = variance_new / (1.0 - beta_two**STEP)
    change = mean_hat / (jnp.sqrt(var_hat) + adam_eps)
    if decayed:
        change = change + weight_decay * weight
    delta = -learn_rate * change
    return (weight + delta, delta, momentum_new, variance_new)


def rotary_tables(length):
    position = jnp.arange(length).astype(f32)[:, None]
    half = ROTARY // 2
    inverse_freq = rope_base ** (-(jnp.arange(half).astype(f32) * 2.0 / ROTARY))
    angles = position * inverse_freq[None, :]
    return jnp.cos(angles), jnp.sin(angles)


def rotate(tensor, cosine, sine):
    half = ROTARY // 2
    a, b, rest = tensor[..., :half], tensor[..., half:ROTARY], tensor[..., ROTARY:]
    return jnp.concatenate([a * cosine - b * sine, b * cosine + a * sine, rest], -1)


def dot32(a, b, dims):
    return lax.dot_general(a, b, (dims, ((), ())), preferred_element_type=f32)


MESH = pl.DeviceIdType.MESH
ANY = pl.BlockSpec(memory_space=pl.ANY)
VM = pl.BlockSpec(memory_space=pltpu.VMEM)
ONE = ((1,), (0,))
NT = ((1,), (1,))
TN = ((0,), (0,))


def rows_of(start, size):
    return pl.ds(pl.multiple_of(start, math.gcd(size, 512)), size)


class Links:
    def __init__(self, R, X, S):
        self.R, self.X, self.S = R, X, S
        self.rep = lax.axis_index("rep")
        self.tx = lax.axis_index("tx")
        self.core = lax.axis_index("core")
        self.z = lax.axis_index("shard")

    def at_core(self):
        return {"core": 1 - self.core}

    def at_tx(self):
        return {"tx": 1 - self.tx}

    def at_rep(self, dr):
        return {"rep": lax.rem(self.rep + dr, self.R)}

    def at_z(self, z):
        return {"shard": z}

    def barrier(self):
        sem = pltpu.get_barrier_semaphore()

        def tell(where):
            pl.semaphore_signal(sem, inc=1, device_id=where, device_id_type=MESH)

        count = 1 + (self.X - 1) + (self.R - 1)
        tell(self.at_core())
        if self.X > 1:
            tell(self.at_tx())
        for dr in range(1, self.R):
            tell(self.at_rep(dr))

        @pl.when(self.z > 0)
        def _():
            tell(self.at_z(self.z - 1))

        @pl.when(self.z < self.S - 1)
        def _():
            tell(self.at_z(self.z + 1))

        ends = (self.z > 0).astype(jnp.int32) + (self.z < self.S - 1).astype(jnp.int32)
        pl.semaphore_wait(sem, count + ends)


def remote(src, dst, send, recv, where):
    return pltpu.make_async_remote_copy(
        src_ref=src, dst_ref=dst, send_sem=send, recv_sem=recv, device_id=where, device_id_type=MESH
    )


def local(src, dst, sem):
    return pltpu.make_async_copy(src, dst, sem)


class LineGather:
    def __init__(self, links, own, buf, n, zs, zr, ys, yr, split):
        self.k = links
        self.own, self.buf, self.n = own, buf, n
        self.parts = links.R if split else 1
        self.m = n // self.parts
        self.zs, self.zr, self.ys, self.yr = zs, zr, ys, yr

    def block(self, p, r):
        return self.buf.at[rows_of(p * self.n + r * self.m, self.m)]

    def mine(self):
        return self.k.rep if self.parts > 1 else 0

    def hop(self, src, p, step, way):
        to = self.k.z + 1 if way == 0 else self.k.z - 1
        return remote(
            src, self.block(p, self.mine()), self.zs.at[step, way], self.zr.at[p], self.k.at_z(to)
        )

    def across(self, p, dr):
        b = self.block(p, self.k.rep)
        return remote(b, b, self.ys.at[p, dr], self.yr.at[p, self.k.rep], self.k.at_rep(dr))

    def each_way(self, step, fn):
        z, S = self.k.z, self.k.S
        for way in (0, 1):
            p = z - step if way == 0 else z + step
            here = (step <= z) if way == 0 else (z + step <= S - 1)
            on = (z < S - 1) if way == 0 else (z > 0)
            fn(way, p, here, on)

    def start(self):
        mine = self.mine()

        def go(way, p, here, on):
            @pl.when(on)
            def _():
                self.hop(self.own.at[rows_of(mine * self.m, self.m)], p, 0, way).start()

        self.each_way(0, go)

    def event(self, step):
        def go(way, p, here, on):
            @pl.when(here)
            def _():
                b = self.block(p, self.mine())
                self.hop(b, p, step, way).wait_recv()

                @pl.when(on)
                def _():
                    self.hop(b, p, step, way).start()

                if self.parts > 1:
                    for dr in range(1, self.k.R):
                        self.across(p, dr).start()

        self.each_way(step, go)

    def arrived(self):
        if self.parts == 1:
            return
        for p in range(self.k.S):
            @pl.when(p != self.k.z)
            def _():
                for dr in range(1, self.k.R):
                    r = lax.rem(self.k.rep + dr, self.k.R)
                    b = self.block(p, r)
                    remote(b, b, self.ys.at[p, dr], self.yr.at[p, r], self.k.at_rep(dr)).wait_recv()

    def drain(self):
        for step in range(self.k.S):
            def go(way, p, here, on):
                @pl.when(jnp.logical_and(here, on))
                def _():
                    self.hop(self.block(p, self.mine()), p, step, way).wait_send()

                if step > 0 and self.parts > 1:
                    @pl.when(here)
                    def _():
                        for dr in range(1, self.k.R):
                            self.across(p, dr).wait_send()

            self.each_way(step, go)


def layer_norm_rows(xb):
    xf = xb.astype(f32)
    cen = xf - jnp.mean(xf, -1, keepdims=True)
    return cen * lax.rsqrt(jnp.mean(cen * cen, -1, keepdims=True) + eps_norm)


SMALL_ROWS = 24


def small_row(sm, S, first, count):
    return jnp.concatenate(
        [sm[p * SMALL_ROWS + first + j : p * SMALL_ROWS + first + j + 1, :] for p in range(S) for j in range(count)],
        -1,
    )


def attention_kernel(R, X, S, L, D, FT, *refs):
    (x_ref, dy_ref, wt_ref, wo_ref, we_ref, ws_ref, sm_ref, rc_ref, ra_ref, rb_ref) = refs[:10]
    (xg, dyg, wt_o, wo_o, we_o, ws_o, vec_o, ctx_o, gt_o, wtg_o, wog_o, tbg_o) = refs[10:22]
    (
        xs, dys, n1, gt, wtb, wob, smb, q_s, k_s, v_s, gc_s, kT, vT, ctxT, gqT, gk_a, gv_a, wtg, wog,
        zs, zr, ys, yr, tok_s, tok_r, loc,
    ) = refs[22:]
    T = 2 * X
    rows = D // S
    DT = S * HEAD_DIM
    links = Links(R, X, S)
    chunks = []
    for c, (own, buf) in enumerate(
        [(sm_ref, smb), (wt_ref, wtb), (wo_ref, wob), (we_ref, we_o), (ws_ref, ws_o)]
    ):
        chunks.append(
            LineGather(links, own, buf, own.shape[0], zs.at[c], zr.at[c], ys.at[c], yr.at[c], c > 0)
        )
    g_sm, g_wt, g_wo, g_we, g_ws = chunks
    links.barrier()

    own_copies = [
        local(x_ref, xs.at[pl.ds(0, L)], loc.at[0]),
        local(dy_ref, dys.at[pl.ds(0, L)], loc.at[1]),
    ]
    for c, g in enumerate(chunks):
        own_copies.append(local(g.own, g.buf.at[rows_of(links.z * g.n, g.n)], loc.at[2 + c]))

    def token_copy(a, slot):
        buf = (xs, dys)[a]
        src = (x_ref, dy_ref)[a]
        if slot == 1:
            return remote(src, buf.at[pl.ds(L, L)], tok_s.at[a, 1], tok_r.at[a, 1], links.at_core())
        if slot == 2:
            return remote(src, buf.at[pl.ds(2 * L, L)], tok_s.at[a, 2], tok_r.at[a, 2], links.at_tx())
        return remote(
            buf.at[pl.ds(2 * L, L)], buf.at[pl.ds(3 * L, L)], tok_s.at[a, 3], tok_r.at[a, 3], links.at_core()
        )

    g_sm.start()
    g_wt.start()
    g_wo.start()
    if X > 1:
        token_copy(0, 2).start()
        token_copy(1, 2).start()
    token_copy(0, 1).start()
    token_copy(1, 1).start()
    for c in own_copies:
        c.start()

    own_copies[0].wait()
    own_copies[2].wait()
    for step in range(1, S):
        g_sm.event(step)
    per = rows // 128
    vec_o[...] = jnp.zeros_like(vec_o)
    sm = smb[...]
    for j in range(6):
        vec_o[j : j + 1, 0:D] = small_row(sm, S, j * per, per)
    fper = FT // S // 128
    vec_o[8 : 8 + 1, 0:FT] = small_row(sm, S, 6 * per, fper)
    lane = lax.broadcasted_iota(jnp.int32, (1, 128), 1)
    rank = links.tx * 2 + links.core

    def head_bias(j, p):
        block = j * (D // 128) + (T * p + rank) // 2
        at = (block // (3 * per)) * SMALL_ROWS + 6 * per + fper + lax.rem(block, 3 * per)
        row = smb[pl.ds(at, 1), :]
        return jnp.where(lax.rem(rank, 2) == p % 2, row, pltpu.roll(row, HEAD_DIM, 1))

    for j in range(3):
        for a in range(S // 2):
            both = jnp.where(lane < HEAD_DIM, head_bias(j, 2 * a), head_bias(j, 2 * a + 1))
            vec_o[9 + j : 10 + j, a * 128 : (a + 1) * 128] = both

    def norm_one(i):
        gain, shift = vec_o[0:1, 0:D], vec_o[1:2, 0:D]

        @pl.loop(0, L // 64)
        def _(b):
            at = rows_of(i * L + b * 64, 64)
            n1[at, :] = (layer_norm_rows(xs[at, :]) * gain + shift).astype(bf16)

    norm_one(0)
    g_wt.event(1)
    g_wo.event(1)
    g_we.start()
    for step in range(2, S):
        g_wt.event(step)
        g_wo.event(step)
    g_ws.start()
    own_copies[1].wait()
    own_copies[3].wait()
    own_copies[4].wait()
    g_wt.arrived()
    g_wo.arrived()
    late = [(g, step) for step in range(1, S) for g in (g_we, g_ws)]

    def pump(i, turn):
        for index in range(T):
            at = 2 * (2 * index + turn)
            todo = late[at : at + 2]
            if todo:
                @pl.when(i == index)
                def _():
                    for g, step in todo:
                        g.event(step)

    half = L // 2
    lane_head = lax.broadcasted_iota(jnp.int32, (1, DT), 1) // HEAD_DIM
    key_at = lax.broadcasted_iota(jnp.int32, (half, half), 0)
    query_at = lax.broadcasted_iota(jnp.int32, (half, half), 1)
    causal = key_at <= query_at

    def slot_body(i, carry):
        here = rows_of(i * L, L)
        for j, dst in enumerate((q_s, k_s, v_s)):
            val = dot32(n1[here, :], wtb[:, j * DT : (j + 1) * DT], ONE) + vec_o[9 + j : 10 + j, 0:DT]
            if j < 2:
                val = (
                    val * rc_ref[...]
                    + pltpu.roll(val, DT - 8, 1) * ra_ref[...]
                    + pltpu.roll(val, 8, 1) * rb_ref[...]
                )
            vb = val.astype(bf16)
            if j == 0:
                q_s[...] = vb * bf16(0.125)
            else:
                dst[...] = vb
                (kT if j == 1 else vT)[...] = vb.T
        gc_s[...] = dot32(dys[here, :], wob[...], NT).astype(bf16)
        gk_a[...] = jnp.zeros_like(gk_a)
        gv_a[...] = jnp.zeros_like(gv_a)
        pump(i, 0)

        def head_body(h, c2):
            mine = (lane_head == h).astype(f32).astype(bf16)
            hrows = rows_of(h * HEAD_DIM, HEAD_DIM)
            for b in range(2):
                qs = pl.ds(b * half, half)
                kl = (b + 1) * half
                km = k_s[0:kl, :] * mine
                sT = dot32(km, q_s[qs, :], NT)
                diag = jnp.where(causal, sT[kl - half :], -1e30)
                sT = diag if b == 0 else jnp.concatenate([sT[: kl - half], diag], 0)
                e = jnp.exp(sT - jnp.max(sT, 0, keepdims=True))
                p = e * (1.0 / jnp.sum(e, 0, keepdims=True))
                pb = p.astype(bf16)
                ctxT[hrows, qs] = dot32(vT[hrows, 0:kl], pb, ONE).astype(bf16)
                gv_a[0:kl, :] += dot32(pb, gc_s[qs, :] * mine, ONE)
                gp = dot32(v_s[0:kl, :] * mine, gc_s[qs, :], NT)
                gs = (p * (gp - jnp.sum(p * gp, 0, keepdims=True))).astype(bf16)
                gk_a[0:kl, :] += dot32(gs, q_s[qs, :] * mine, ONE)
                gqT[hrows, qs] = dot32(kT[hrows, 0:kl], gs, ONE) * 0.125
            return c2

        lax.fori_loop(0, S, head_body, 0)
        pump(i, 1)
        for j in range(3):
            if j == 2:
                val = gv_a[...]
            else:
                val = gqT[...].T if j == 0 else gk_a[...]
                val = (
                    val * rc_ref[...]
                    - pltpu.roll(val, DT - 8, 1) * ra_ref[...]
                    - pltpu.roll(val, 8, 1) * rb_ref[...]
                )
            gt[here, j * DT : (j + 1) * DT] = val.astype(bf16)
        ctx_o[:, rows_of(i * L, L)] = ctxT[...]
        grad = dot32(ctxT[...], dys[here, :], ONE)

        @pl.when(i == 0)
        def _():
            wog[...] = grad

        @pl.when(i > 0)
        def _():
            wog[...] += grad

        if X > 1:
            @pl.when(i == 1)
            def _():
                for a in (0, 1):
                    token_copy(a, 2).wait_recv()
                    token_copy(a, 3).start()

        for nxt in range(1, T):
            @pl.when(i + 1 == nxt)
            def _():
                for a in (0, 1):
                    if nxt != 2:
                        token_copy(a, nxt).wait_recv()

        @pl.when(i + 1 < T)
        def _():
            norm_one(i + 1)

        return carry

    lax.fori_loop(0, T, slot_body, 0)
    outs = [
        local(xs, xg, loc.at[0]),
        local(dys, dyg, loc.at[1]),
        local(wtb, wt_o, loc.at[3]),
        local(wob, wo_o, loc.at[4]),
        local(gt, gt_o, loc.at[7]),
        local(wog, wog_o, loc.at[8]),
    ]
    for o in outs:
        o.start()
    for g, step in late[4 * T :]:
        g.event(step)
    ones = jnp.ones((8, T * L), bf16)
    tbg_o[...] = dot32(ones, gt[...], ONE)

    @pl.loop(0, D // 256)
    def _(b):
        at = rows_of(b * 256, 256)
        wtg[at, :] = dot32(n1[:, pl.ds(pl.multiple_of(b * 256, 256), 256)], gt[...], TN)

    last = local(wtg, wtg_o, loc.at[9])
    last.start()
    own_copies[5].wait()
    own_copies[6].wait()
    g_we.arrived()
    g_ws.arrived()
    for g in chunks:
        g.drain()
    for a in (0, 1):
        for slot in range(1, T):
            token_copy(a, slot).wait_send()
    for o in outs:
        o.wait()
    last.wait()


def attention_phase(R, X, S, x, dy, wt, wo, we, ws, small, tables):
    L, D = x.shape
    T = 2 * X
    DT = S * HEAD_DIM
    FT = we.shape[1]
    fs = ws.shape[0]
    n = T * L
    sds = jax.ShapeDtypeStruct
    dma = pltpu.SemaphoreType.DMA
    outs = [
        sds((n, D), bf16), sds((n, D), bf16), sds((D, 3 * DT), bf16), sds((DT, D), bf16),
        sds((D, FT), bf16), sds((FT, D), bf16), sds((16, max(D, FT)), f32), sds((DT, n), bf16),
        sds((n, 3 * DT), bf16), sds((D, 3 * DT), f32), sds((DT, D), f32), sds((8, 3 * DT), f32),
    ]
    specs = [ANY] * 6 + [VM, VM] + [ANY] * 3 + [VM]
    vmem = pltpu.VMEM
    scratch = [
        vmem((n, D), bf16), vmem((n, D), bf16), vmem((n, D), bf16), vmem((n, 3 * DT), bf16),
        vmem((D, 3 * DT), bf16), vmem((DT, D), bf16), vmem((S * SMALL_ROWS, 128), f32),
        vmem((L, DT), bf16), vmem((L, DT), bf16), vmem((L, DT), bf16), vmem((L, DT), bf16),
        vmem((DT, L), bf16), vmem((DT, L), bf16), vmem((DT, L), bf16), vmem((DT, L), f32),
        vmem((L, DT), f32), vmem((L, DT), f32), vmem((D, 3 * DT), f32), vmem((DT, D), f32),
        dma((5, S, 2)), dma((5, S)), dma((5, S, R)), dma((5, S, R)), dma((2, 4)), dma((2, 4)), dma((10,)),
    ]
    body = lambda *refs: attention_kernel(R, X, S, L, D, FT, *refs)
    return pl.pallas_call(
        body,
        name="attention_phase",
        out_shape=outs,
        in_specs=[ANY] * 7 + [VM] * 3,
        out_specs=specs,
        scratch_shapes=scratch,
        compiler_params=pltpu.CompilerParams(
            collective_id=1, has_side_effects=True, vmem_limit_bytes=60 * 1024 * 1024
        ),
    )(x, dy, wt, wo, we, ws, small, *tables)


TP = ("tx", "core")


def make_step(R, X, S):
    T = 2 * X

    def step(*args):
        x, dy = args[0], args[1]
        masters, momenta, variances = args[2:14], args[14:26], args[26:38]
        L, D = x.shape
        H = D // HEAD_DIM
        t = lax.axis_index(TP)
        z = lax.axis_index("shard")
        rep = lax.axis_index("rep")
        wt, wo, we, ws = masters[4], masters[6], masters[8], masters[10]
        rows = wt.shape[0]
        F = we.shape[1]
        fs = F // S // T
        HT = H // T

        low = [lax.reduce_precision(m, 8, 7) for m in masters]
        eb_own = lax.dynamic_index_in_dim(low[9].reshape(T, fs), t, 0, False)
        packed = [low[i].reshape(-1, 128) for i in (0, 1, 2, 3, 7, 11)] + [eb_own.reshape(-1, 128)]
        packed.append(low[5].reshape(-1, 128))
        packed = jnp.concatenate(packed)
        small = jnp.pad(packed, ((0, SMALL_ROWS - packed.shape[0]), (0, 0)))

        wt_t = lax.dynamic_index_in_dim(wt.reshape(rows, 3, S, T, HEAD_DIM), t, 3, False)
        wt_t = wt_t.reshape(rows, 3 * S * HEAD_DIM).astype(bf16)
        we_t = lax.dynamic_index_in_dim(we.reshape(rows, S, T, fs), t, 2, False)
        we_t = we_t.reshape(rows, S * fs).astype(bf16)
        wo_t = lax.dynamic_index_in_dim(wo.reshape(T, rows // T, D), t, 0, False).astype(bf16)
        ws_t = lax.dynamic_index_in_dim(ws.reshape(T, fs, D), t, 0, False).astype(bf16)

        cosine, sine = rotary_tables(L)
        zero, one = jnp.zeros((L, 8), f32), jnp.ones((L, HEAD_DIM - 16), f32)
        pad = jnp.zeros((L, HEAD_DIM - 16), f32)
        tables = (
            jnp.tile(jnp.concatenate([cosine, cosine, one], 1), (1, S)),
            jnp.tile(jnp.concatenate([-sine, zero, pad], 1), (1, S)),
            jnp.tile(jnp.concatenate([zero, sine, pad], 1), (1, S)),
        )
        (xg, dyg, wt_f, wo_f, we_f, ws_f, vecs, ctxT, gt, wt_g, wo_g, tb_g) = attention_phase(
            R, X, S, x, dy, wt_t, wo_t, we_t, ws_t, small, tables
        )
        g1v, b1v, g2v, b2v, obv, sbv = [vecs[i, :D] for i in range(6)]
        eb_t = vecs[8, :F // T]
        tb_g = tb_g[0]
        xf = xg.astype(f32)
        cen = xf - jnp.mean(xf, -1, keepdims=True)
        rstd = lax.rsqrt(jnp.mean(cen * cen, -1, keepdims=True) + eps_norm)
        xhat = cen * rstd
        n2 = (xhat * g2v + b2v).astype(bf16)
        hidden = dot32(n2, we_f, ((1,), (0,))) + eb_t
        act32, gelu_pull = jax.vjp(lambda e: jax.nn.gelu(e, approximate=False), hidden)
        act = act32.astype(bf16)
        out_part = dot32(ctxT, wo_f, TN) + dot32(act, ws_f, ((1,), (0,)))

        def scatter_tokens(part):
            part = part.astype(bf16)
            slots = part.reshape(T, L, D)
            order = jnp.bitwise_xor(jnp.arange(T), t)
            part = jnp.take(slots, order, axis=0).reshape(X, 2, L, D)
            part = lax.psum_scatter(part, "core", scatter_dimension=1, tiled=False)
            part = lax.psum_scatter(part, "tx", scatter_dimension=0, tiled=False)
            return part.astype(f32)

        xl = x.astype(f32)
        out = (xl + scatter_tokens(out_part) + (obv + sbv)).astype(bf16)

        dact = dot32(dyg, ws_f, ((1,), (1,)))
        gh = gelu_pull(dact)[0].astype(bf16)
        ws_g = dot32(act, dyg, ((0,), (0,)))
        we_g = dot32(n2, gh, ((0,), (0,)))
        gn2 = dot32(gh, we_f, ((1,), (1,)))
        eb_g = jnp.sum(gh.astype(f32), 0)
        gn1 = dot32(gt, wt_f, ((1,), (1,)))

        dxhat = scatter_tokens(gn1 * g1v + gn2 * g2v)
        cl = xl - jnp.mean(xl, -1, keepdims=True)
        rl = lax.rsqrt(jnp.mean(cl * cl, -1, keepdims=True) + eps_norm)
        xh = cl * rl
        dx = rl * (
            dxhat
            - jnp.mean(dxhat, -1, keepdims=True)
            - xh * jnp.mean(dxhat * xh, -1, keepdims=True)
        )
        in_grad = (dy.astype(f32) + dx).astype(bf16)

        vec = jnp.concatenate(
            [
                jnp.sum(gn1 * xhat, 0),
                jnp.sum(gn1, 0),
                jnp.sum(gn2 * xhat, 0),
                jnp.sum(gn2, 0),
                jnp.sum(dy.astype(f32), 0),
                jnp.where(
                    jnp.arange(T)[None, None, :, None] == t,
                    tb_g.reshape(3, S, 1, HEAD_DIM),
                    0.0,
                ).reshape(-1),
                jnp.where(
                    jnp.arange(T)[None, :, None] == t, eb_g.reshape(S, 1, fs), 0.0
                ).reshape(-1),
            ]
        )
        vec = lax.psum(vec, ("rep", "tx", "core", "shard"))
        vparts = [D] * 5 + [3 * D, F]
        voffs = [sum(vparts[:i]) for i in range(8)]
        vown = [
            lax.dynamic_slice_in_dim(vec, voffs[i] + z * (vparts[i] // S), vparts[i] // S, 0)
            for i in range(7)
        ]

        def reduce_w(grad):
            n = grad.shape[0] // S
            grad = grad.reshape(S, R, n // R, grad.shape[1])
            grad = lax.psum_scatter(grad, "rep", scatter_dimension=1, tiled=False)
            grad = lax.psum_scatter(grad, "shard", scatter_dimension=0, tiled=False)
            grad = lax.all_gather(grad.astype(bf16), "rep", axis=0, tiled=True)
            return lax.all_gather(grad, TP, axis=0).astype(f32)

        wt_s = reduce_w(wt_g).reshape(T, rows, 3, S, HEAD_DIM).transpose(1, 2, 3, 0, 4)
        wt_s = wt_s.reshape(rows, 3 * D)
        wo_s = reduce_w(wo_g).reshape(rows, D)
        we_s = reduce_w(we_g).reshape(T, rows, S, fs).transpose(1, 2, 0, 3).reshape(rows, F)
        ws_s = reduce_w(ws_g).reshape(F // S, D)

        summed = [
            vown[0], vown[1], vown[2], vown[3], wt_s, vown[5], wo_s, vown[4], we_s, vown[6], ws_s, vown[4],
        ]
        updated, ones, twos = [], [], []
        for i in range(12):
            new_weight, delta, m_new, v_new = adam_step(
                masters[i], summed[i], momenta[i], variances[i], i in (4, 6, 8, 10)
            )
            updated.append(delta if i in (0, 2) else new_weight)
            ones.append(m_new)
            twos.append(v_new)
        return (out, in_grad, *summed, *updated, *ones, *twos)

    return step


def solution(mesh):
    G, S = mesh.shape["grp"], mesh.shape["shard"]
    X = 2 if S <= 4 else 1
    R = G // (2 * X)
    full = Mesh(mesh.devices.reshape(R, X, 2, S), ("rep", "tx", "core", "shard"))
    tok = P(("rep", "tx", "core", "shard"), None)
    vecs, mats = P("shard"), P("shard", None)
    group = tuple(mats if i in (4, 6, 8, 10) else vecs for i in range(12))
    return jax.shard_map(
        make_step(R, X, S),
        mesh=full,
        in_specs=(tok, tok) + group * 3,
        out_specs=(tok, tok) + group * 4,
        check_vma=False,
    )
```

```python
import math

import jax
import jax.numpy as jnp
from jax import lax
from jax.experimental import pallas as pl
from jax.experimental.pallas import tpu as pltpu
from jax.sharding import Mesh, PartitionSpec as P

HEAD_DIM = 64
ROTARY = 16
STEP = 10
eps_norm = 1e-05
rope_base = 10000.0
beta_one = 0.9
beta_two = 0.95
learn_rate = 0.01
adam_eps = 1e-08
weight_decay = 0.01

bf16 = jnp.bfloat16
f32 = jnp.float32


def adam_step(weight, gradient, momentum, variance, decayed):
    momentum_new = beta_one * momentum + (1.0 - beta_one) * gradient
    variance_new = beta_two * variance + (1.0 - beta_two) * gradient * gradient
    mean_hat = momentum_new / (1.0 - beta_one**STEP)
    var_hat = variance_new / (1.0 - beta_two**STEP)
    change = mean_hat / (jnp.sqrt(var_hat) + adam_eps)
    if decayed:
        change = change + weight_decay * weight
    delta = -learn_rate * change
    return (weight + delta, delta, momentum_new, variance_new)


def rotary_tables(length):
    position = jnp.arange(length).astype(f32)[:, None]
    half = ROTARY // 2
    inverse_freq = rope_base ** (-(jnp.arange(half).astype(f32) * 2.0 / ROTARY))
    angles = position * inverse_freq[None, :]
    return jnp.cos(angles), jnp.sin(angles)


def rotate(tensor, cosine, sine):
    half = ROTARY // 2
    a, b, rest = tensor[..., :half], tensor[..., half:ROTARY], tensor[..., ROTARY:]
    return jnp.concatenate([a * cosine - b * sine, b * cosine + a * sine, rest], -1)


def dot32(a, b, dims):
    return lax.dot_general(a, b, (dims, ((), ())), preferred_element_type=f32)


MESH = pl.DeviceIdType.MESH
ANY = pl.BlockSpec(memory_space=pl.ANY)
VM = pl.BlockSpec(memory_space=pltpu.VMEM)
ONE = ((1,), (0,))
NT = ((1,), (1,))
TN = ((0,), (0,))


def rows_of(start, size):
    return pl.ds(pl.multiple_of(start, math.gcd(size, 512)), size)


class Links:
    def __init__(self, R, X, S):
        self.R, self.X, self.S = R, X, S
        self.rep = lax.axis_index("rep")
        self.tx = lax.axis_index("tx")
        self.core = lax.axis_index("core")
        self.z = lax.axis_index("shard")

    def at_core(self):
        return {"core": 1 - self.core}

    def at_tx(self):
        return {"tx": 1 - self.tx}

    def at_rep(self, dr):
        return {"rep": lax.rem(self.rep + dr, self.R)}

    def at_z(self, z):
        return {"shard": z}

    def barrier(self, every_plane=False):
        sem = pltpu.get_barrier_semaphore()

        def tell(where):
            pl.semaphore_signal(sem, inc=1, device_id=where, device_id_type=MESH)

        count = 1 + (self.X - 1) + (self.R - 1)
        tell(self.at_core())
        if self.X > 1:
            tell(self.at_tx())
        for dr in range(1, self.R):
            tell(self.at_rep(dr))

        if every_plane:
            for dz in range(1, self.S):
                tell(self.at_z(lax.rem(self.z + dz, self.S)))
            pl.semaphore_wait(sem, count + self.S - 1)
            return

        @pl.when(self.z > 0)
        def _():
            tell(self.at_z(self.z - 1))

        @pl.when(self.z < self.S - 1)
        def _():
            tell(self.at_z(self.z + 1))

        ends = (self.z > 0).astype(jnp.int32) + (self.z < self.S - 1).astype(jnp.int32)
        pl.semaphore_wait(sem, count + ends)


def remote(src, dst, send, recv, where):
    return pltpu.make_async_remote_copy(
        src_ref=src, dst_ref=dst, send_sem=send, recv_sem=recv, device_id=where, device_id_type=MESH
    )


def local(src, dst, sem):
    return pltpu.make_async_copy(src, dst, sem)


class LineGather:
    def __init__(self, links, own, buf, n, zs, zr, ys, yr, split):
        self.k = links
        self.own, self.buf, self.n = own, buf, n
        self.parts = links.R if split else 1
        self.m = n // self.parts
        self.zs, self.zr, self.ys, self.yr = zs, zr, ys, yr

    def block(self, p, r):
        return self.buf.at[rows_of(p * self.n + r * self.m, self.m)]

    def mine(self):
        return self.k.rep if self.parts > 1 else 0

    def hop(self, src, p, step, way):
        to = self.k.z + 1 if way == 0 else self.k.z - 1
        return remote(
            src, self.block(p, self.mine()), self.zs.at[step, way], self.zr.at[p], self.k.at_z(to)
        )

    def across(self, p, dr):
        b = self.block(p, self.k.rep)
        return remote(b, b, self.ys.at[p, dr], self.yr.at[p, self.k.rep], self.k.at_rep(dr))

    def each_way(self, step, fn):
        z, S = self.k.z, self.k.S
        for way in (0, 1):
            p = z - step if way == 0 else z + step
            here = (step <= z) if way == 0 else (z + step <= S - 1)
            on = (z < S - 1) if way == 0 else (z > 0)
            fn(way, p, here, on)

    def start(self):
        mine = self.mine()

        def go(way, p, here, on):
            @pl.when(on)
            def _():
                self.hop(self.own.at[rows_of(mine * self.m, self.m)], p, 0, way).start()

        self.each_way(0, go)

    def event(self, step):
        def go(way, p, here, on):
            @pl.when(here)
            def _():
                b = self.block(p, self.mine())
                self.hop(b, p, step, way).wait_recv()

                @pl.when(on)
                def _():
                    self.hop(b, p, step, way).start()

                if self.parts > 1:
                    for dr in range(1, self.k.R):
                        self.across(p, dr).start()

        self.each_way(step, go)

    def arrived(self):
        if self.parts == 1:
            return
        for p in range(self.k.S):
            @pl.when(p != self.k.z)
            def _():
                for dr in range(1, self.k.R):
                    r = lax.rem(self.k.rep + dr, self.k.R)
                    b = self.block(p, r)
                    remote(b, b, self.ys.at[p, dr], self.yr.at[p, r], self.k.at_rep(dr)).wait_recv()

    def drain(self):
        for step in range(self.k.S):
            def go(way, p, here, on):
                @pl.when(jnp.logical_and(here, on))
                def _():
                    self.hop(self.block(p, self.mine()), p, step, way).wait_send()

                if step > 0 and self.parts > 1:
                    @pl.when(here)
                    def _():
                        for dr in range(1, self.k.R):
                            self.across(p, dr).wait_send()

            self.each_way(step, go)


def layer_norm_rows(xb):
    xf = xb.astype(f32)
    cen = xf - jnp.mean(xf, -1, keepdims=True)
    return cen * lax.rsqrt(jnp.mean(cen * cen, -1, keepdims=True) + eps_norm)


SMALL_ROWS = 24


def small_row(sm, S, first, count):
    return jnp.concatenate(
        [sm[p * SMALL_ROWS + first + j : p * SMALL_ROWS + first + j + 1, :] for p in range(S) for j in range(count)],
        -1,
    )


def attention_kernel(R, X, S, L, D, FT, *refs):
    (x_ref, dy_ref, wt_ref, wo_ref, we_ref, ws_ref, sm_ref, rc_ref, ra_ref, rb_ref) = refs[:10]
    (xg, dyg, wt_o, wo_o, we_o, ws_o, vec_o, ctx_o, gt_o, wtl_o, wth_o, wol_o, woh_o, tbg_o) = refs[10:24]
    (
        xs, dys, n1, gt, wtb, wob, smb, q_s, k_s, v_s, gc_s, kT, vT, ctxT, gqT, gk_a, gv_a, wtl, wth, wol, woh, wog,
        zs, zr, ys, yr, tok_s, tok_r, loc,
    ) = refs[24:]
    T = 2 * X
    rows = D // S
    DT = S * HEAD_DIM
    links = Links(R, X, S)
    chunks = []
    for c, (own, buf) in enumerate(
        [(sm_ref, smb), (wt_ref, wtb), (wo_ref, wob), (we_ref, we_o), (ws_ref, ws_o)]
    ):
        chunks.append(
            LineGather(links, own, buf, own.shape[0], zs.at[c], zr.at[c], ys.at[c], yr.at[c], c > 0)
        )
    g_sm, g_wt, g_wo, g_we, g_ws = chunks
    links.barrier()

    own_copies = [
        local(x_ref, xs.at[pl.ds(0, L)], loc.at[0]),
        local(dy_ref, dys.at[pl.ds(0, L)], loc.at[1]),
    ]
    for c, g in enumerate(chunks):
        own_copies.append(local(g.own, g.buf.at[rows_of(links.z * g.n, g.n)], loc.at[2 + c]))

    def token_copy(a, slot):
        buf = (xs, dys)[a]
        src = (x_ref, dy_ref)[a]
        if slot == 1:
            return remote(src, buf.at[pl.ds(L, L)], tok_s.at[a, 1], tok_r.at[a, 1], links.at_core())
        if slot == 2:
            return remote(src, buf.at[pl.ds(2 * L, L)], tok_s.at[a, 2], tok_r.at[a, 2], links.at_tx())
        return remote(
            buf.at[pl.ds(2 * L, L)], buf.at[pl.ds(3 * L, L)], tok_s.at[a, 3], tok_r.at[a, 3], links.at_core()
        )

    g_sm.start()
    g_wt.start()
    g_wo.start()
    if X > 1:
        token_copy(0, 2).start()
        token_copy(1, 2).start()
    token_copy(0, 1).start()
    token_copy(1, 1).start()
    for c in own_copies:
        c.start()

    own_copies[0].wait()
    own_copies[2].wait()
    for step in range(1, S):
        g_sm.event(step)
    per = rows // 128
    vec_o[...] = jnp.zeros_like(vec_o)
    sm = smb[...]
    for j in range(6):
        vec_o[j : j + 1, 0:D] = small_row(sm, S, j * per, per)
    fper = FT // S // 128
    vec_o[8 : 8 + 1, 0:FT] = small_row(sm, S, 6 * per, fper)
    lane = lax.broadcasted_iota(jnp.int32, (1, 128), 1)
    rank = links.tx * 2 + links.core

    def head_bias(j, p):
        block = j * (D // 128) + (T * p + rank) // 2
        at = (block // (3 * per)) * SMALL_ROWS + 6 * per + fper + lax.rem(block, 3 * per)
        row = smb[pl.ds(at, 1), :]
        return jnp.where(lax.rem(rank, 2) == p % 2, row, pltpu.roll(row, HEAD_DIM, 1))

    for j in range(3):
        for a in range(S // 2):
            both = jnp.where(lane < HEAD_DIM, head_bias(j, 2 * a), head_bias(j, 2 * a + 1))
            vec_o[9 + j : 10 + j, a * 128 : (a + 1) * 128] = both

    def norm_one(i):
        gain, shift = vec_o[0:1, 0:D], vec_o[1:2, 0:D]

        @pl.loop(0, L // 64)
        def _(b):
            at = rows_of(i * L + b * 64, 64)
            n1[at, :] = (layer_norm_rows(xs[at, :]) * gain + shift).astype(bf16)

    norm_one(0)
    g_wt.event(1)
    g_wo.event(1)
    g_we.start()
    for step in range(2, S):
        g_wt.event(step)
        g_wo.event(step)
    g_ws.start()
    own_copies[1].wait()
    own_copies[3].wait()
    own_copies[4].wait()
    g_wt.arrived()
    g_wo.arrived()
    late = [(g, step) for step in range(1, S) for g in (g_we, g_ws)]

    def pump(i, turn):
        for index in range(T):
            at = 2 * (2 * index + turn)
            todo = late[at : at + 2]
            if todo:
                @pl.when(i == index)
                def _():
                    for g, step in todo:
                        g.event(step)

    half = L // 2
    lane_head = lax.broadcasted_iota(jnp.int32, (1, DT), 1) // HEAD_DIM
    key_at = lax.broadcasted_iota(jnp.int32, (half, half), 0)
    query_at = lax.broadcasted_iota(jnp.int32, (half, half), 1)
    causal = key_at <= query_at

    def slot_body(i, carry):
        here = rows_of(i * L, L)
        for j, dst in enumerate((q_s, k_s, v_s)):
            val = dot32(n1[here, :], wtb[:, j * DT : (j + 1) * DT], ONE) + vec_o[9 + j : 10 + j, 0:DT]
            if j < 2:
                val = (
                    val * rc_ref[...]
                    + pltpu.roll(val, DT - 8, 1) * ra_ref[...]
                    + pltpu.roll(val, 8, 1) * rb_ref[...]
                )
            vb = val.astype(bf16)
            if j == 0:
                q_s[...] = vb * bf16(0.125)
            else:
                dst[...] = vb
                (kT if j == 1 else vT)[...] = vb.T
        gc_s[...] = dot32(dys[here, :], wob[...], NT).astype(bf16)
        gk_a[...] = jnp.zeros_like(gk_a)
        gv_a[...] = jnp.zeros_like(gv_a)
        pump(i, 0)

        def head_body(h, c2):
            mine = (lane_head == h).astype(f32).astype(bf16)
            hrows = rows_of(h * HEAD_DIM, HEAD_DIM)
            for b in range(2):
                qs = pl.ds(b * half, half)
                kl = (b + 1) * half
                km = k_s[0:kl, :] * mine
                sT = dot32(km, q_s[qs, :], NT)
                diag = jnp.where(causal, sT[kl - half :], -1e30)
                sT = diag if b == 0 else jnp.concatenate([sT[: kl - half], diag], 0)
                e = jnp.exp(sT - jnp.max(sT, 0, keepdims=True))
                p = e * (1.0 / jnp.sum(e, 0, keepdims=True))
                pb = p.astype(bf16)
                ctxT[hrows, qs] = dot32(vT[hrows, 0:kl], pb, ONE).astype(bf16)
                gv_a[0:kl, :] += dot32(pb, gc_s[qs, :] * mine, ONE)
                gp = dot32(v_s[0:kl, :] * mine, gc_s[qs, :], NT)
                gs = (p * (gp - jnp.sum(p * gp, 0, keepdims=True))).astype(bf16)
                gk_a[0:kl, :] += dot32(gs, q_s[qs, :] * mine, ONE)
                gqT[hrows, qs] = dot32(kT[hrows, 0:kl], gs, ONE) * 0.125
            return c2

        lax.fori_loop(0, S, head_body, 0)
        pump(i, 1)
        for j in range(3):
            if j == 2:
                val = gv_a[...]
            else:
                val = gqT[...].T if j == 0 else gk_a[...]
                val = (
                    val * rc_ref[...]
                    - pltpu.roll(val, DT - 8, 1) * ra_ref[...]
                    - pltpu.roll(val, 8, 1) * rb_ref[...]
                )
            gt[here, j * DT : (j + 1) * DT] = val.astype(bf16)
        ctx_o[:, rows_of(i * L, L)] = ctxT[...]
        grad = dot32(ctxT[...], dys[here, :], ONE)

        @pl.when(i == 0)
        def _():
            wog[...] = grad

        @pl.when(i > 0)
        def _():
            wog[...] += grad

        if X > 1:
            @pl.when(i == 1)
            def _():
                for a in (0, 1):
                    token_copy(a, 2).wait_recv()
                    token_copy(a, 3).start()

        for nxt in range(1, T):
            @pl.when(i + 1 == nxt)
            def _():
                for a in (0, 1):
                    if nxt != 2:
                        token_copy(a, nxt).wait_recv()

        @pl.when(i + 1 < T)
        def _():
            norm_one(i + 1)

        return carry

    lax.fori_loop(0, T, slot_body, 0)
    outs = [
        local(xs, xg, loc.at[0]),
        local(dys, dyg, loc.at[1]),
        local(wtb, wt_o, loc.at[3]),
        local(wob, wo_o, loc.at[4]),
        local(gt, gt_o, loc.at[7]),
    ]
    for o in outs:
        o.start()
    for g, step in late[4 * T :]:
        g.event(step)
    ones = jnp.ones((8, T * L), bf16)
    tbg_o[...] = dot32(ones, gt[...], ONE)

    m = rows // R

    @pl.loop(0, S)
    def _(p):
        grad = dot32(n1[:, pl.ds(pl.multiple_of(p * rows, rows), rows)], gt[...], TN)
        for r in range(R):
            part = grad[r * m : (r + 1) * m]
            wtl[rows_of((r * S + p) * m, m), :] = part.astype(bf16)

            @pl.when(links.rep == r)
            def _():
                wth[rows_of(p * m, m), :] = part

    mo = HEAD_DIM // R
    for p in range(S):
        for r in range(R):
            part = wog[p * HEAD_DIM + r * mo : p * HEAD_DIM + (r + 1) * mo, :]
            wol[(r * S + p) * mo : (r * S + p + 1) * mo, :] = part.astype(bf16)

            @pl.when(links.rep == r)
            def _():
                woh[p * mo : (p + 1) * mo, :] = part

    last = [
        local(wtl, wtl_o, loc.at[8]),
        local(wth, wth_o, loc.at[9]),
        local(wol, wol_o, loc.at[10]),
        local(woh, woh_o, loc.at[11]),
    ]
    for o in last:
        o.start()
    own_copies[5].wait()
    own_copies[6].wait()
    g_we.arrived()
    g_ws.arrived()
    for g in chunks:
        g.drain()
    for a in (0, 1):
        for slot in range(1, T):
            token_copy(a, slot).wait_send()
    for o in outs + last:
        o.wait()


def attention_phase(R, X, S, x, dy, wt, wo, we, ws, small, tables):
    L, D = x.shape
    T = 2 * X
    DT = S * HEAD_DIM
    FT = we.shape[1]
    fs = ws.shape[0]
    n = T * L
    sds = jax.ShapeDtypeStruct
    dma = pltpu.SemaphoreType.DMA
    outs = [
        sds((n, D), bf16), sds((n, D), bf16), sds((D, 3 * DT), bf16), sds((DT, D), bf16),
        sds((D, FT), bf16), sds((FT, D), bf16), sds((16, max(D, FT)), f32), sds((DT, n), bf16),
        sds((n, 3 * DT), bf16), sds((D, 3 * DT), bf16), sds((D // R, 3 * DT), f32),
        sds((DT, D), bf16), sds((DT // R, D), f32), sds((8, 3 * DT), f32),
    ]
    specs = [ANY] * 6 + [VM, VM] + [ANY] * 5 + [VM]
    vmem = pltpu.VMEM
    scratch = [
        vmem((n, D), bf16), vmem((n, D), bf16), vmem((n, D), bf16), vmem((n, 3 * DT), bf16),
        vmem((D, 3 * DT), bf16), vmem((DT, D), bf16), vmem((S * SMALL_ROWS, 128), f32),
        vmem((L, DT), bf16), vmem((L, DT), bf16), vmem((L, DT), bf16), vmem((L, DT), bf16),
        vmem((DT, L), bf16), vmem((DT, L), bf16), vmem((DT, L), bf16), vmem((DT, L), f32),
        vmem((L, DT), f32), vmem((L, DT), f32), vmem((D, 3 * DT), bf16), vmem((D // R, 3 * DT), f32),
        vmem((DT, D), bf16), vmem((DT // R, D), f32), vmem((DT, D), f32),
        dma((5, S, 2)), dma((5, S)), dma((5, S, R)), dma((5, S, R)), dma((2, 4)), dma((2, 4)), dma((12,)),
    ]
    body = lambda *refs: attention_kernel(R, X, S, L, D, FT, *refs)
    return pl.pallas_call(
        body,
        name="attention_phase",
        out_shape=outs,
        in_specs=[ANY] * 7 + [VM] * 3,
        out_specs=specs,
        scratch_shapes=scratch,
        compiler_params=pltpu.CompilerParams(
            collective_id=1, has_side_effects=True, vmem_limit_bytes=60 * 1024 * 1024
        ),
    )(x, dy, wt, wo, we, ws, small, *tables)


class GradSum:
    def __init__(self, links, blocks, m, bufs, sems, piece, only=None):
        self.k, self.B, self.m = links, blocks, m
        self.lo, self.keep, self.yr, self.zs, self.zr, self.fin = bufs
        self.sems, self.piece, self.only = sems, piece, only

    def across(self, f, dr):
        size = self.B * self.m
        r = lax.rem(self.k.rep + dr, self.k.R)
        return remote(
            self.lo.at[rows_of((f * self.k.R + r) * size, size)],
            self.yr.at[rows_of((f * (self.k.R - 1) + dr - 1) * size, size)],
            self.sems["ys"].at[f, dr], self.sems["yr"].at[f, dr], self.k.at_rep(dr),
        )

    def send_across(self, f):
        for dr in range(1, self.k.R):
            self.across(f, dr).start()

    def toward(self, f, p):
        b = 0 if self.only else p
        to = self.zr.at[rows_of(((0 if self.only else f) * self.k.S + self.k.z) * self.m, self.m)]
        return remote(
            self.zs.at[rows_of((f * self.B + b) * self.m, self.m)], to,
            self.sems["zs"].at[f, p], self.sems["zr"].at[f, self.k.z], self.k.at_z(p),
        )

    def owners(self, f, fn):
        if self.only:
            @pl.when(f != self.k.z)
            def _():
                fn(f)
        else:
            for dp in range(1, self.k.S):
                fn(lax.rem(self.k.z + dp, self.k.S))

    def if_owner(self, f, fn):
        if self.only:
            pl.when(f == self.k.z)(fn)
        else:
            fn()

    def sum_across(self, f):
        R, m = self.k.R, self.m
        for dr in range(1, R):
            self.across(f, dr).wait_recv()

        for b in range(self.B):
            at = rows_of((f * self.B + b) * m, m)
            total = self.keep[at, :]
            for dr in range(1, R):
                got = rows_of(((f * (R - 1) + dr - 1) * self.B + b) * m, m)
                total = total + self.yr[got, :].astype(f32)
            self.keep[at, :] = total
            self.zs[at, :] = total.astype(bf16)

        self.owners(f, lambda p: self.toward(f, p).start())

    def total(self, f):
        S, m = self.k.S, self.m

        def go():
            g = 0 if self.only else f
            at = rows_of((f * self.B + (0 if self.only else self.k.z)) * m, m)
            total = self.keep[at, :]
            for dp in range(1, S):
                p = lax.rem(self.k.z + dp, S)
                src = self.zr.at[rows_of((g * S + p) * m, m)]
                remote(src, src, self.sems["zs"].at[f, p], self.sems["zr"].at[f, p], self.k.at_z(p)).wait_recv()
                total = total + self.zr[rows_of((g * S + p) * m, m), :].astype(f32)
            fin = rows_of(g * m, m)
            self.fin[fin, :] = total.astype(bf16)
            src = self.fin.at[fin]
            local(src, self.piece(f, self.k.tx, self.k.core, self.k.rep), self.sems["gl"].at[f]).start()
            for c in self.spread(f, src, self.k.tx, self.k.rep, 0):
                c.start()

        self.if_owner(f, go)

    def spread(self, f, src, tx, r, stage):
        dst = self.piece(f, tx, self.k.core, r)
        src = dst if src is None else src
        out = []
        other = 1 if stage == 2 else 0
        out.append(
            remote(src, dst, self.sems["gcs"].at[f, other, r], self.sems["gcr"].at[f, other, r], self.k.at_core())
        )
        if stage < 2 and self.k.X > 1:
            out.append(remote(src, dst, self.sems["gxs"].at[f, r], self.sems["gxr"].at[f, r], self.k.at_tx()))
        if stage == 0:
            for dr in range(1, self.k.R):
                out.append(remote(src, dst, self.sems["gys"].at[f, dr], self.sems["gyr"].at[f, r], self.k.at_rep(dr)))
        return out

    def replicas(self, fn):
        for dr in range(1, self.k.R):
            fn(dr, lax.rem(self.k.rep + dr, self.k.R))

    def forward_rep(self, f):
        def go():
            def one(dr, r):
                b = self.piece(f, self.k.tx, self.k.core, r)
                remote(b, b, self.sems["gys"].at[f, dr], self.sems["gyr"].at[f, r], self.k.at_rep(dr)).wait_recv()
                for c in self.spread(f, None, self.k.tx, r, 1):
                    c.start()

            self.replicas(one)

        self.if_owner(f, go)

    def forward_tx(self, f):
        if self.k.X == 1:
            return

        def go():
            for r in range(self.k.R):
                b = self.piece(f, 1 - self.k.tx, self.k.core, r)
                remote(b, b, self.sems["gxs"].at[f, r], self.sems["gxr"].at[f, r], self.k.at_tx()).wait_recv()
                for c in self.spread(f, None, 1 - self.k.tx, r, 2):
                    c.start()

        self.if_owner(f, go)

    def finish(self, f):
        for dr in range(1, self.k.R):
            self.across(f, dr).wait_send()
        self.owners(f, lambda p: self.toward(f, p).wait_send())

        def go():
            src = self.fin.at[rows_of((0 if self.only else f) * self.m, self.m)]
            local(src, self.piece(f, self.k.tx, self.k.core, self.k.rep), self.sems["gl"].at[f]).wait()
            for c in self.spread(f, src, self.k.tx, self.k.rep, 0):
                c.wait_send()
            self.replicas(lambda dr, r: [c.wait_send() for c in self.spread(f, None, self.k.tx, r, 1)])
            for other in range(self.k.X):
                tx = self.k.tx if other == 0 else 1 - self.k.tx
                for r in range(self.k.R):
                    if other == 1:
                        for c in self.spread(f, None, tx, r, 2):
                            c.wait_send()
                    b = self.piece(f, tx, 1 - self.k.core, r)
                    remote(
                        b, b, self.sems["gcs"].at[f, other, r], self.sems["gcr"].at[f, other, r], self.k.at_core()
                    ).wait_recv()

        self.if_owner(f, go)


SEM_NAMES = ("ys", "yr", "zs", "zr", "gl", "gcs", "gcr", "gxs", "gxr", "gys", "gyr")


def grad_sems(count, R, X, S):
    dma = pltpu.SemaphoreType.DMA
    return [
        dma((count, R)), dma((count, R)), dma((count, S)), dma((count, S)), dma((count,)),
        dma((count, 2, R)), dma((count, 2, R)), dma((count, R)), dma((count, R)), dma((count, R)), dma((count, R)),
    ]


def feed_kernel(R, X, S, L, D, FT, *refs):
    (xg, dyg, wt_f, wo_f, we_f, ws_f, vec, ctx_i, gt_i, wtl, wth, wol, woh, tbg) = refs[:14]
    (out_o, ing_o, g_wt, g_wo, g_we, g_ws, v_o) = refs[14:21]
    rest = list(refs[21:])
    take = lambda count: [rest.pop(0) for _ in range(count)]
    (xb, dyb, n2b, actb, ghb, web, wsb, wob, ctb) = take(9)
    wt_bufs, wo_bufs, we_bufs, ws_bufs = take(5), take(5), take(6), take(6)
    (send_b, out_r, dx_r, xs_b, out_x, dx_x, vsum, vrecv) = take(8)
    sem_sets = [dict(zip(SEM_NAMES, take(len(SEM_NAMES)))) for _ in range(4)]
    (loc, tok, v_s, v_r, dxk) = take(5)
    T = 2 * X
    n = T * L
    rows = D // S
    DT = S * HEAD_DIM
    fs = FT // S
    k = Links(R, X, S)
    k.barrier(every_plane=True)
    rank = lambda tx, core: tx * 2 + core
    mt, mo, me, ms = rows // R, HEAD_DIM // R, rows // R, fs // R
    u_wt = GradSum(k, S, mt, [wtl] + wt_bufs, sem_sets[0],
                   lambda f, tx, c, r: g_wt.at[rows_of(rank(tx, c) * rows + r * mt, mt)])
    u_wo = GradSum(k, S, mo, [wol] + wo_bufs, sem_sets[1],
                   lambda f, tx, c, r: g_wo.at[rows_of(rank(tx, c) * HEAD_DIM + r * mo, mo)])
    u_we = GradSum(k, S, me, we_bufs, sem_sets[2],
                   lambda f, tx, c, r: g_we.at[rows_of(r * me, me), rows_of((f * T + rank(tx, c)) * fs, fs)])
    u_ws = GradSum(k, 1, ms, ws_bufs, sem_sets[3],
                   lambda f, tx, c, r: g_ws.at[rows_of(rank(tx, c) * fs + r * ms, ms)], only=True)
    first = (u_wt, u_wo)
    for u in first:
        u.send_across(0)

    def load_x(i, place):
        return local(xg.at[rows_of(i * L, L)], xb.at[pl.ds(place * L, L)], loc.at[place])

    load_x(0, 0).start()
    loads = [
        local(we_f, web, loc.at[2]), local(dyg, dyb, loc.at[3]), local(ws_f, wsb, loc.at[4]),
        local(wo_f, wob, loc.at[5]), local(ctx_i, ctb, loc.at[6]),
        local(wth, wt_bufs[0], loc.at[7]), local(woh, wo_bufs[0], loc.at[8]),
    ]
    for c in loads:
        c.start()

    gain1, gain2, shift2 = vec[0:1, 0:D], vec[2:3, 0:D], vec[3:4, 0:D]

    def norm_two(i, place):
        @pl.loop(0, L // 64)
        def _(b):
            n2b[rows_of(i * L + b * 64, 64), :] = (
                layer_norm_rows(xb[pl.ds(pl.multiple_of(place * L + b * 64, 64), 64), :]) * gain2 + shift2
            ).astype(bf16)

    for i in range(T):
        load_x(i, i % 2).wait()
        if i + 1 < T:
            load_x(i + 1, (i + 1) % 2).start()
        norm_two(i, i % 2)
    load_x(1, 0).start()
    for c in loads[:3]:
        c.wait()

    def hidden_body(it, carry):
        i, f = it // S, lax.rem(it, S)
        here, cols = rows_of(i * L, L), pl.ds(pl.multiple_of(f * fs, fs), fs)
        h = dot32(n2b[here, :], web[:, cols], ONE) + vec[8:9, cols]
        cdf = 0.5 * (1.0 + lax.erf(h * math.sqrt(0.5)))
        actb[here, cols] = (h * cdf).astype(bf16)
        slope = cdf + h * (jnp.exp(-0.5 * h * h) * (1.0 / math.sqrt(2.0 * math.pi)))
        ghb[here, cols] = (dot32(dyb[here, :], wsb[cols, :], NT) * slope).astype(bf16)
        return carry

    lax.fori_loop(0, T * S, hidden_body, 0)
    loads[3].wait()
    loads[4].wait()
    half = L // 2

    def feed_rows(i, b):
        at = i * L + b * half
        return dot32(actb[at : at + half, :], wsb[...], ONE) + dot32(ctb[:, at : at + half], wob[...], TN)

    def to_core(which, j):
        land = (out_r, dx_r)[which]
        return remote(
            send_b.at[pl.ds(j * L, L)], land.at[pl.ds(j * L, L)],
            tok.at[which, 0, j], tok.at[which, 1, j], k.at_core(),
        )

    def to_tx(which):
        return remote(
            xs_b.at[pl.ds(which * L, L)], (out_x, dx_x)[which], tok.at[which, 2, 0], tok.at[which, 2, 1], k.at_tx()
        )

    for j in range(X):
        for b in range(2):
            at = j * L + b * half
            send_b[at : at + half, :] = feed_rows(2 * j + 1, b).astype(bf16)
        to_core(0, j).start()
    if X > 1:
        to_core(0, 1).wait_recv()
        for b in range(2):
            got = out_r[L + b * half : L + (b + 1) * half, :].astype(f32)
            xs_b[b * half : (b + 1) * half, :] = (feed_rows(2, b) + got).astype(bf16)
        to_tx(0).start()

    for b in range(2):
        dxk[b * half : (b + 1) * half, :] = feed_rows(0, b)

    side = D // DT
    thirds = [wsb.at[pl.ds((j // side) * D, D), pl.ds((j % side) * DT, DT)] for j in range(3)]
    load_wt = [local(wt_f.at[:, pl.ds(j * DT, DT)], thirds[j], loc.at[(9, 11, 12)[j]]) for j in range(3)]
    for c in load_wt:
        c.start()

    def triple_back(at):
        total = None
        for j in range(0, 3, side):
            wide = min(side, 3 - j)
            part = dot32(
                actb[at, j * DT : (j + wide) * DT], wsb[(j // side) * D : (j // side + 1) * D, 0 : wide * DT], NT
            )
            total = part if total is None else total + part
        return total

    def store_grad(u, f, block, grad):
        for r in range(R):
            part = grad[r * u.m : (r + 1) * u.m]
            u.lo[rows_of(((f * R + r) * u.B + block) * u.m, u.m), :] = part.astype(bf16)

            @pl.when(k.rep == r)
            def _():
                u.keep[rows_of((f * u.B + block) * u.m, u.m), :] = part

    loads[5].wait()
    loads[6].wait()

    def chunk_body(f, carry):
        cols = pl.ds(pl.multiple_of(f * fs, fs), fs)
        store_grad(u_ws, f, 0, dot32(actb[:, cols], dyb[...], TN))
        u_ws.send_across(f)

        def block_body(p, c2):
            grad = dot32(n2b[:, pl.ds(pl.multiple_of(p * rows, rows), rows)], ghb[:, cols], TN)
            store_grad(u_we, f, p, grad)
            return c2

        lax.fori_loop(0, S, block_body, 0)
        u_we.send_across(f)

        @pl.when(f == 0)
        def _():
            for u in first:
                u.sum_across(0)

        return carry

    lax.fori_loop(0, S, chunk_body, 0)
    gtb = actb.at[:, pl.ds(0, 3 * DT)]
    load_gt = local(gt_i, gtb, loc.at[10])
    load_gt.start()
    for j in range(X):
        to_core(0, j).wait_send()
    load_gt.wait()
    for c in load_wt:
        c.wait()

    def pair(step, f):
        for u in (u_we, u_ws):
            getattr(u, step)(f)

    vsum[...] = jnp.zeros_like(vsum)

    def slot_grad(i, place, finish):
        for b in range(2):
            at = pl.ds(i * L + b * half, half)
            xhat = layer_norm_rows(xb[place * L + b * half : place * L + (b + 1) * half, :])
            g1 = triple_back(at)
            vsum[0:1, 0:D] += jnp.sum(g1 * xhat, 0, keepdims=True)
            vsum[1:2, 0:D] += jnp.sum(g1, 0, keepdims=True)
            g2 = dot32(ghb[at, :], web[...], NT)
            vsum[2:3, 0:D] += jnp.sum(g2 * xhat, 0, keepdims=True)
            vsum[3:4, 0:D] += jnp.sum(g2, 0, keepdims=True)
            finish(b, g1 * gain1 + g2 * gain2, xhat)

    order = [2 * j + 1 for j in range(X)] + ([2] if X > 1 else []) + [0]
    events = [("sum_across", f) for f in range(S)]
    for turn, i in enumerate(order):
        place = turn % 2
        load_x(i, place).wait()
        if turn + 1 < T:
            load_x(order[turn + 1], 1 - place).start()
        if i % 2 == 1:
            j = i // 2

            def finish(b, val, xhat):
                at = j * L + b * half
                send_b[at : at + half, :] = val.astype(bf16)

            slot_grad(i, place, finish)
            to_core(1, j).start()
        elif i == 2:
            to_core(1, 1).wait_recv()

            def finish(b, val, xhat):
                got = dx_r[L + b * half : L + (b + 1) * half, :].astype(f32)
                xs_b[L + b * half : L + (b + 1) * half, :] = (val + got).astype(bf16)

            slot_grad(2, place, finish)
            to_tx(1).start()
            pair("sum_across", 0)
            for u in first:
                u.total(0)
        else:
            to_core(0, 0).wait_recv()
            to_core(1, 0).wait_recv()
            if X > 1:
                to_tx(0).wait_recv()
            for j in range(X):
                to_core(1, j).wait_send()
            for b in range(2):
                rows_b = slice(b * half, (b + 1) * half)
                total = dxk[rows_b, :] + out_r[rows_b, :].astype(f32)
                if X > 1:
                    total = total + out_x[rows_b, :].astype(f32)
                total = total + xb[place * L + b * half : place * L + (b + 1) * half, :].astype(f32)
                send_b[rows_b, :] = (total + (vec[4:5, 0:D] + vec[5:6, 0:D])).astype(bf16)
            save_out = local(send_b.at[pl.ds(0, L)], out_o, loc.at[2])
            save_out.start()

            def finish(b, val, xhat):
                rows_b = slice(b * half, (b + 1) * half)
                dxk[rows_b, :] = val + dx_r[rows_b, :].astype(f32)

            slot_grad(0, place, finish)
            place0 = place
    ones = jnp.ones((8, L), bf16)
    vsum[4:5, 0:D] = dot32(ones, dyb[0:L, :], ONE)[0:1]
    mine = rank(k.tx, k.core)
    eb = dot32(jnp.ones((8, n), bf16), ghb[...], ONE)[0:1]
    for t in range(T):
        @pl.when(mine == t)
        def _():
            vsum[5 + t : 6 + t, 0 : 3 * DT] = tbg[0:1, :]
            vsum[5 + T + t : 6 + T + t, 0:FT] = eb

    def exchange(stage, copies):
        for c in copies:
            c.start()
        for c in copies:
            c.wait()
        for q in range(len(copies)):
            vsum[...] += vrecv[stage + q]

    at_stage = 0
    exchange(0, [remote(vsum, vrecv.at[0], v_s.at[0], v_r.at[0], k.at_core())])
    at_stage = 1
    if X > 1:
        exchange(1, [remote(vsum, vrecv.at[1], v_s.at[1], v_r.at[1], k.at_tx())])
        at_stage = 2
    rep_copies = [
        remote(vsum, vrecv.at[at_stage + dr - 1], v_s.at[at_stage + dr - 1], v_r.at[at_stage + dr - 1], k.at_rep(dr))
        for dr in range(1, R)
    ]
    exchange(at_stage, rep_copies)
    at_stage += R - 1
    pair("sum_across", 1)
    for u in first:
        u.forward_rep(0)
    z_copies = [
        remote(
            vsum, vrecv.at[at_stage + dz - 1], v_s.at[at_stage + dz - 1], v_r.at[at_stage + dz - 1],
            k.at_z(lax.rem(k.z + dz, S)),
        )
        for dz in range(1, S)
    ]
    for c in z_copies:
        c.start()
    pair("total", 0)
    for f in range(2, S):
        pair("sum_across", f)
        if f == 2:
            for u in first:
                u.forward_tx(0)
        pair("total", f - 1)
        pair("forward_rep", f - 2)
        if f > 2:
            pair("forward_tx", f - 3)
    for c in z_copies:
        c.wait()
    total = vsum[...]
    for q in range(S - 1):
        total = total + vrecv[at_stage + q]
    v_o[...] = total
    if X > 1:
        to_tx(1).wait_recv()
    for b in range(2):
        rows_b = slice(b * half, (b + 1) * half)
        dx = dxk[rows_b, :]
        if X > 1:
            dx = dx + dx_x[rows_b, :].astype(f32)
        xf = xb[place0 * L + b * half : place0 * L + (b + 1) * half, :].astype(f32)
        cen = xf - jnp.mean(xf, -1, keepdims=True)
        rstd = lax.rsqrt(jnp.mean(cen * cen, -1, keepdims=True) + eps_norm)
        xhat = cen * rstd
        back = dx - jnp.mean(dx, -1, keepdims=True) - xhat * jnp.mean(dx * xhat, -1, keepdims=True)
        send_b[L + b * half : L + (b + 1) * half, :] = (dyb[rows_b, :].astype(f32) + rstd * back).astype(bf16)
    save_ing = local(send_b.at[pl.ds(L, L)], ing_o, loc.at[3])
    save_ing.start()
    pair("total", S - 1)
    pair("forward_rep", S - 2)
    pair("forward_tx", S - 3)
    pair("forward_rep", S - 1)
    pair("forward_tx", S - 2)
    pair("forward_tx", S - 1)
    for u in first:
        u.finish(0)
    for f in range(S):
        pair("finish", f)
    if X > 1:
        to_tx(0).wait_send()
        to_tx(1).wait_send()
    save_out.wait()
    save_ing.wait()


def feed_phase(R, X, S, F, xg, dyg, wt_f, wo_f, we_f, ws_f, vecs, ctxT, gt, wtl, wth, wol, woh, tbg):
    T = 2 * X
    n, D = xg.shape
    L = n // T
    DT = S * HEAD_DIM
    FT = we_f.shape[1]
    fs = FT // S
    rows = D // S
    mt, mo, me, ms = rows // R, HEAD_DIM // R, rows // R, fs // R
    W = max(D, 3 * DT, FT)
    sds = jax.ShapeDtypeStruct
    vmem = pltpu.VMEM
    dma = pltpu.SemaphoreType.DMA
    outs = [
        sds((L, D), bf16), sds((L, D), bf16), sds((T * rows, 3 * DT), bf16), sds((rows, D), bf16),
        sds((rows, F), bf16), sds((F // S, D), bf16), sds((16, W), f32),
    ]

    def bufs(count, B, m, cols, lo, landing):
        made = [vmem((count * R * B * m, cols), bf16)] if lo else []
        return made + [
            vmem((count * B * m, cols), f32), vmem((count * (R - 1) * B * m, cols), bf16),
            vmem((count * B * m, cols), bf16), vmem((landing * S * m, cols), bf16), vmem((landing * m, cols), bf16),
        ]

    scratch = [
        vmem((2 * L, D), bf16), vmem((n, D), bf16), vmem((n, D), bf16), vmem((n, FT), bf16), vmem((n, FT), bf16),
        vmem((D, FT), bf16), vmem((FT, D), bf16), vmem((DT, D), bf16),
        vmem((DT, n), bf16),
    ]
    scratch += bufs(1, S, mt, 3 * DT, False, 1) + bufs(1, S, mo, D, False, 1)
    scratch += bufs(S, S, me, fs, True, S) + bufs(S, 1, ms, D, True, 1)
    scratch += [
        vmem((2 * L, D), bf16), vmem((X * L, D), bf16), vmem((X * L, D), bf16), vmem((2 * L, D), bf16),
        vmem((L, D), bf16), vmem((L, D), bf16), vmem((16, W), f32), vmem((2 + R - 1 + S - 1, 16, W), f32),
    ]
    for count in (1, 1, S, S):
        scratch += grad_sems(count, R, X, S)
    scratch += [dma((13,)), dma((2, 3, 2)), dma((2 + R - 1 + S - 1,)), dma((2 + R - 1 + S - 1,)), vmem((L, D), f32)]
    body = lambda *refs: feed_kernel(R, X, S, L, D, FT, *refs)
    return pl.pallas_call(
        body,
        name="feed_phase",
        out_shape=outs,
        in_specs=[ANY] * 6 + [VM] + [ANY] * 6 + [VM],
        out_specs=[ANY] * 6 + [VM],
        scratch_shapes=scratch,
        compiler_params=pltpu.CompilerParams(
            collective_id=2, has_side_effects=True, vmem_limit_bytes=67_000_000
        ),
    )(xg, dyg, wt_f, wo_f, we_f, ws_f, vecs, ctxT, gt, wtl, wth, wol, woh, tbg)


TP = ("tx", "core")


def make_step(R, X, S):
    T = 2 * X

    def step(*args):
        x, dy = args[0], args[1]
        masters, momenta, variances = args[2:14], args[14:26], args[26:38]
        L, D = x.shape
        H = D // HEAD_DIM
        t = lax.axis_index(TP)
        z = lax.axis_index("shard")
        rep = lax.axis_index("rep")
        wt, wo, we, ws = masters[4], masters[6], masters[8], masters[10]
        rows = wt.shape[0]
        F = we.shape[1]
        fs = F // S // T
        HT = H // T

        low = [lax.reduce_precision(m, 8, 7) for m in masters]
        eb_own = lax.dynamic_index_in_dim(low[9].reshape(T, fs), t, 0, False)
        packed = [low[i].reshape(-1, 128) for i in (0, 1, 2, 3, 7, 11)] + [eb_own.reshape(-1, 128)]
        packed.append(low[5].reshape(-1, 128))
        packed = jnp.concatenate(packed)
        small = jnp.pad(packed, ((0, SMALL_ROWS - packed.shape[0]), (0, 0)))

        wt_t = lax.dynamic_index_in_dim(wt.reshape(rows, 3, S, T, HEAD_DIM), t, 3, False)
        wt_t = wt_t.reshape(rows, 3 * S * HEAD_DIM).astype(bf16)
        we_t = lax.dynamic_index_in_dim(we.reshape(rows, S, T, fs), t, 2, False)
        we_t = we_t.reshape(rows, S * fs).astype(bf16)
        wo_t = lax.dynamic_index_in_dim(wo.reshape(T, rows // T, D), t, 0, False).astype(bf16)
        ws_t = lax.dynamic_index_in_dim(ws.reshape(T, fs, D), t, 0, False).astype(bf16)

        cosine, sine = rotary_tables(L)
        zero, one = jnp.zeros((L, 8), f32), jnp.ones((L, HEAD_DIM - 16), f32)
        pad = jnp.zeros((L, HEAD_DIM - 16), f32)
        tables = (
            jnp.tile(jnp.concatenate([cosine, cosine, one], 1), (1, S)),
            jnp.tile(jnp.concatenate([-sine, zero, pad], 1), (1, S)),
            jnp.tile(jnp.concatenate([zero, sine, pad], 1), (1, S)),
        )
        passed = attention_phase(R, X, S, x, dy, wt_t, wo_t, we_t, ws_t, small, tables)
        out, in_grad, wt_s, wo_s, we_s, ws_s, vec = feed_phase(R, X, S, F, *passed)
        wt_s = wt_s.reshape(T, rows, 3, S, HEAD_DIM).transpose(1, 2, 3, 0, 4).reshape(rows, 3 * D)
        DT, FT = S * HEAD_DIM, F // T
        tb_g = vec[5 : 5 + T, : 3 * DT].reshape(T, 3, S, HEAD_DIM).transpose(1, 2, 0, 3).reshape(-1)
        eb_g = vec[5 + T : 5 + 2 * T, :FT].reshape(T, S, fs).transpose(1, 0, 2).reshape(-1)

        def own(v):
            return lax.dynamic_slice_in_dim(v, z * (v.shape[0] // S), v.shape[0] // S, 0)

        vown = [own(vec[i, :D]) for i in range(5)] + [own(tb_g), own(eb_g)]
        wt_s, wo_s, we_s, ws_s = [g.astype(f32) for g in (wt_s, wo_s, we_s, ws_s)]
        summed = [
            vown[0], vown[1], vown[2], vown[3], wt_s, vown[5], wo_s, vown[4], we_s, vown[6], ws_s, vown[4],
        ]
        updated, ones, twos = [], [], []
        for i in range(12):
            new_weight, delta, m_new, v_new = adam_step(
                masters[i], summed[i], momenta[i], variances[i], i in (4, 6, 8, 10)
            )
            updated.append(delta if i in (0, 2) else new_weight)
            ones.append(m_new)
            twos.append(v_new)
        return (out, in_grad, *summed, *updated, *ones, *twos)

    return step


def solution(mesh):
    G, S = mesh.shape["grp"], mesh.shape["shard"]
    X = 2 if S <= 4 else 1
    R = G // (2 * X)
    full = Mesh(mesh.devices.reshape(R, X, 2, S), ("rep", "tx", "core", "shard"))
    tok = P(("rep", "tx", "core", "shard"), None)
    vecs, mats = P("shard"), P("shard", None)
    group = tuple(mats if i in (4, 6, 8, 10) else vecs for i in range(12))
    return jax.shard_map(
        make_step(R, X, S),
        mesh=full,
        in_specs=(tok, tok) + group * 3,
        out_specs=(tok, tok) + group * 4,
        check_vma=False,
    )
```

```python
import math

import jax
import jax.numpy as jnp
from jax import lax
from jax.experimental import pallas as pl
from jax.experimental.pallas import tpu as pltpu
from jax.sharding import Mesh, PartitionSpec as P

HEAD_DIM = 64
ROTARY = 16
STEP = 10
eps_norm = 1e-05
rope_base = 10000.0
beta_one = 0.9
beta_two = 0.95
learn_rate = 0.01
adam_eps = 1e-08
weight_decay = 0.01

bf16 = jnp.bfloat16
f32 = jnp.float32


def adam_step(weight, gradient, momentum, variance, decayed):
    momentum_new = beta_one * momentum + (1.0 - beta_one) * gradient
    variance_new = beta_two * variance + (1.0 - beta_two) * gradient * gradient
    mean_hat = momentum_new / (1.0 - beta_one**STEP)
    var_hat = variance_new / (1.0 - beta_two**STEP)
    change = mean_hat / (jnp.sqrt(var_hat) + adam_eps)
    if decayed:
        change = change + weight_decay * weight
    delta = -learn_rate * change
    return (weight + delta, delta, momentum_new, variance_new)


def rotary_tables(length):
    position = jnp.arange(length).astype(f32)[:, None]
    half = ROTARY // 2
    inverse_freq = rope_base ** (-(jnp.arange(half).astype(f32) * 2.0 / ROTARY))
    angles = position * inverse_freq[None, :]
    return jnp.cos(angles), jnp.sin(angles)


def rotate(tensor, cosine, sine):
    half = ROTARY // 2
    a, b, rest = tensor[..., :half], tensor[..., half:ROTARY], tensor[..., ROTARY:]
    return jnp.concatenate([a * cosine - b * sine, b * cosine + a * sine, rest], -1)


def dot32(a, b, dims):
    return lax.dot_general(a, b, (dims, ((), ())), preferred_element_type=f32)


MESH = pl.DeviceIdType.MESH
ANY = pl.BlockSpec(memory_space=pl.ANY)
VM = pl.BlockSpec(memory_space=pltpu.VMEM)
ONE = ((1,), (0,))
NT = ((1,), (1,))
TN = ((0,), (0,))


def rows_of(start, size):
    return pl.ds(pl.multiple_of(start, math.gcd(size, 512)), size)


class Links:
    def __init__(self, R, X, S):
        self.R, self.X, self.S = R, X, S
        self.rep = lax.axis_index("rep")
        self.tx = lax.axis_index("tx")
        self.core = lax.axis_index("core")
        self.z = lax.axis_index("shard")

    def at_core(self):
        return {"core": 1 - self.core}

    def at_tx(self):
        return {"tx": 1 - self.tx}

    def at_rep(self, dr):
        return {"rep": lax.rem(self.rep + dr, self.R)}

    def at_z(self, z):
        return {"shard": z}

    def barrier(self, every_plane=False):
        sem = pltpu.get_barrier_semaphore()

        def tell(where):
            pl.semaphore_signal(sem, inc=1, device_id=where, device_id_type=MESH)

        count = 1 + (self.X - 1) + (self.R - 1)
        tell(self.at_core())
        if self.X > 1:
            tell(self.at_tx())
        for dr in range(1, self.R):
            tell(self.at_rep(dr))

        if every_plane:
            for dz in range(1, self.S):
                tell(self.at_z(lax.rem(self.z + dz, self.S)))
            pl.semaphore_wait(sem, count + self.S - 1)
            return

        @pl.when(self.z > 0)
        def _():
            tell(self.at_z(self.z - 1))

        @pl.when(self.z < self.S - 1)
        def _():
            tell(self.at_z(self.z + 1))

        ends = (self.z > 0).astype(jnp.int32) + (self.z < self.S - 1).astype(jnp.int32)
        pl.semaphore_wait(sem, count + ends)


def remote(src, dst, send, recv, where):
    return pltpu.make_async_remote_copy(
        src_ref=src, dst_ref=dst, send_sem=send, recv_sem=recv, device_id=where, device_id_type=MESH
    )


def local(src, dst, sem):
    return pltpu.make_async_copy(src, dst, sem)


class LineGather:
    def __init__(self, links, own, buf, n, zs, zr, ys, yr, split):
        self.k = links
        self.own, self.buf, self.n = own, buf, n
        self.parts = links.R if split else 1
        self.m = n // self.parts
        self.zs, self.zr, self.ys, self.yr = zs, zr, ys, yr

    def block(self, p, r):
        return self.buf.at[rows_of(p * self.n + r * self.m, self.m)]

    def mine(self):
        return self.k.rep if self.parts > 1 else 0

    def hop(self, src, p, step, way):
        to = self.k.z + 1 if way == 0 else self.k.z - 1
        return remote(
            src, self.block(p, self.mine()), self.zs.at[step, way], self.zr.at[p], self.k.at_z(to)
        )

    def across(self, p, dr):
        b = self.block(p, self.k.rep)
        return remote(b, b, self.ys.at[p, dr], self.yr.at[p, self.k.rep], self.k.at_rep(dr))

    def each_way(self, step, fn):
        z, S = self.k.z, self.k.S
        for way in (0, 1):
            p = z - step if way == 0 else z + step
            here = (step <= z) if way == 0 else (z + step <= S - 1)
            on = (z < S - 1) if way == 0 else (z > 0)
            fn(way, p, here, on)

    def start(self):
        mine = self.mine()

        def go(way, p, here, on):
            @pl.when(on)
            def _():
                self.hop(self.own.at[rows_of(mine * self.m, self.m)], p, 0, way).start()

        self.each_way(0, go)

    def event(self, step):
        def go(way, p, here, on):
            @pl.when(here)
            def _():
                b = self.block(p, self.mine())
                self.hop(b, p, step, way).wait_recv()

                @pl.when(on)
                def _():
                    self.hop(b, p, step, way).start()

                if self.parts > 1:
                    for dr in range(1, self.k.R):
                        self.across(p, dr).start()

        self.each_way(step, go)

    def arrived(self):
        if self.parts == 1:
            return
        for p in range(self.k.S):
            @pl.when(p != self.k.z)
            def _():
                for dr in range(1, self.k.R):
                    r = lax.rem(self.k.rep + dr, self.k.R)
                    b = self.block(p, r)
                    remote(b, b, self.ys.at[p, dr], self.yr.at[p, r], self.k.at_rep(dr)).wait_recv()

    def drain(self):
        for step in range(self.k.S):
            def go(way, p, here, on):
                @pl.when(jnp.logical_and(here, on))
                def _():
                    self.hop(self.block(p, self.mine()), p, step, way).wait_send()

                if step > 0 and self.parts > 1:
                    @pl.when(here)
                    def _():
                        for dr in range(1, self.k.R):
                            self.across(p, dr).wait_send()

            self.each_way(step, go)


def layer_norm_rows(xb):
    xf = xb.astype(f32)
    cen = xf - jnp.mean(xf, -1, keepdims=True)
    return cen * lax.rsqrt(jnp.mean(cen * cen, -1, keepdims=True) + eps_norm)


SMALL_ROWS = 24


def small_row(sm, S, first, count):
    return jnp.concatenate(
        [sm[p * SMALL_ROWS + first + j : p * SMALL_ROWS + first + j + 1, :] for p in range(S) for j in range(count)],
        -1,
    )


def attention_kernel(R, X, S, L, D, FT, *refs):
    (x_ref, dy_ref, wt_m, wo_m, we_m, ws_m, sm_ref, rc_i, ra_i, rb_i) = refs[:10]
    (xg, dyg, wt_o, wo_o, we_o, ws_o, vec_o, ctx_o, gt_o, wtl_o, wth_o, wol_o, woh_o, tbg_o) = refs[10:24]
    (
        xs, dys, n1, gt, wtb, wob, smb, q_s, k_s, v_s, gc_s, kT, vT, ctxT, gqT, gk_a, gv_a, wtl, wth, wol, woh, wog,
        rc_ref, ra_ref, rb_ref, wt_w, wo_w, we_w, ws_w, wt_ref, wo_ref, we_ref, ws_ref,
        zs, zr, ys, yr, tok_s, tok_r, loc, cut,
    ) = refs[24:]
    T = 2 * X
    rows = D // S
    DT = S * HEAD_DIM
    links = Links(R, X, S)
    chunks = []
    for c, (own, buf) in enumerate(
        [(sm_ref, smb), (wt_ref, wtb), (wo_ref, wob), (we_ref, we_o), (ws_ref, ws_o)]
    ):
        chunks.append(
            LineGather(links, own, buf, own.shape[0], zs.at[c], zr.at[c], ys.at[c], yr.at[c], c > 0)
        )
    g_sm, g_wt, g_wo, g_we, g_ws = chunks
    lane = lax.broadcasted_iota(jnp.int32, (1, 128), 1)
    rank = links.tx * 2 + links.core
    fs = FT // S
    cuts = [[], [local(wo_m.at[rows_of(rank * HEAD_DIM, HEAD_DIM)], wo_w, cut.at[3 * S])], [],
            [local(ws_m.at[rows_of(rank * fs, fs)], ws_w, cut.at[3 * S + 1])]]
    for j in range(3):
        for p in range(S):
            block = ((j * S + p) * T + rank) // 2
            cuts[0].append(
                local(
                    wt_m.at[:, pl.ds(pl.multiple_of(block * 128, 128), 128)],
                    wt_w.at[:, pl.ds((j * S + p) * 128, 128)],
                    cut.at[j * S + p],
                )
            )
    for p in range(S):
        cuts[2].append(
            local(
                we_m.at[:, pl.ds(pl.multiple_of((p * T + rank) * fs, fs), fs)],
                we_w.at[:, pl.ds(p * fs, fs)],
                cut.at[3 * S + 2 + p],
            )
        )
    for group in cuts:
        for c in group:
            c.start()
    links.barrier()
    for c in cuts[0]:
        c.wait()

    def half_lanes(block, odd):
        val = wt_w[:, block * 128 : (block + 1) * 128]
        return jnp.where(lax.rem(rank, 2) == odd, val, pltpu.roll(val, HEAD_DIM, 1))

    for b in range(3 * S // 2):
        both = jnp.where(lane < HEAD_DIM, half_lanes(2 * b, 0), half_lanes(2 * b + 1, 1))
        wt_ref[:, b * 128 : (b + 1) * 128] = both.astype(bf16)
    cuts[1][0].wait()
    wo_ref[...] = wo_w[...].astype(bf16)

    own_copies = [
        local(x_ref, xs.at[pl.ds(0, L)], loc.at[0]),
        local(dy_ref, dys.at[pl.ds(0, L)], loc.at[1]),
    ]
    own_copies_late = []
    for c, g in enumerate(chunks):
        (own_copies if c < 3 else own_copies_late).append(local(g.own, g.buf.at[rows_of(links.z * g.n, g.n)], loc.at[2 + c]))

    def token_copy(a, slot):
        buf = (xs, dys)[a]
        src = (x_ref, dy_ref)[a]
        if slot == 1:
            return remote(src, buf.at[pl.ds(L, L)], tok_s.at[a, 1], tok_r.at[a, 1], links.at_core())
        if slot == 2:
            return remote(src, buf.at[pl.ds(2 * L, L)], tok_s.at[a, 2], tok_r.at[a, 2], links.at_tx())
        return remote(
            buf.at[pl.ds(2 * L, L)], buf.at[pl.ds(3 * L, L)], tok_s.at[a, 3], tok_r.at[a, 3], links.at_core()
        )

    g_sm.start()
    g_wt.start()
    g_wo.start()
    if X > 1:
        token_copy(0, 2).start()
        token_copy(1, 2).start()
    token_copy(0, 1).start()
    token_copy(1, 1).start()
    for c in own_copies:
        c.start()

    tables = [local(a, b, cut.at[4 * S + 2 + q]) for q, (a, b) in enumerate(((rc_i, rc_ref), (ra_i, ra_ref), (rb_i, rb_ref)))]
    for c in tables:
        c.start()
    for c in cuts[2] + cuts[3]:
        c.wait()
    we_ref[...] = we_w[...].astype(bf16)
    ws_ref[...] = ws_w[...].astype(bf16)
    for c in own_copies_late:
        c.start()
    own_copies[0].wait()
    own_copies[2].wait()
    for step in range(1, S):
        g_sm.event(step)
    per = rows // 128
    vec_o[...] = jnp.zeros_like(vec_o)
    sm = smb[...]
    for j in range(6):
        vec_o[j : j + 1, 0:D] = small_row(sm, S, j * per, per)
    fper = FT // S // 128
    vec_o[8 : 8 + 1, 0:FT] = small_row(sm, S, 6 * per, fper)
    def head_bias(j, p):
        block = j * (D // 128) + (T * p + rank) // 2
        at = (block // (3 * per)) * SMALL_ROWS + 6 * per + fper + lax.rem(block, 3 * per)
        row = smb[pl.ds(at, 1), :]
        return jnp.where(lax.rem(rank, 2) == p % 2, row, pltpu.roll(row, HEAD_DIM, 1))

    for j in range(3):
        for a in range(S // 2):
            both = jnp.where(lane < HEAD_DIM, head_bias(j, 2 * a), head_bias(j, 2 * a + 1))
            vec_o[9 + j : 10 + j, a * 128 : (a + 1) * 128] = both

    def norm_one(i):
        gain, shift = vec_o[0:1, 0:D], vec_o[1:2, 0:D]

        @pl.loop(0, L // 64)
        def _(b):
            at = rows_of(i * L + b * 64, 64)
            n1[at, :] = (layer_norm_rows(xs[at, :]) * gain + shift).astype(bf16)

    norm_one(0)
    g_wt.event(1)
    g_wo.event(1)
    g_we.start()
    for step in range(2, S):
        g_wt.event(step)
        g_wo.event(step)
    g_ws.start()
    own_copies[1].wait()
    own_copies[3].wait()
    own_copies[4].wait()
    for c in tables:
        c.wait()
    g_wt.arrived()
    g_wo.arrived()
    late = [(g, step) for step in range(1, S) for g in (g_we, g_ws)]

    def pump(i, turn):
        for index in range(T):
            at = 2 * (2 * index + turn)
            todo = late[at : at + 2]
            if todo:
                @pl.when(i == index)
                def _():
                    for g, step in todo:
                        g.event(step)

    half = L // 2
    lane_head = lax.broadcasted_iota(jnp.int32, (1, DT), 1) // HEAD_DIM
    key_at = lax.broadcasted_iota(jnp.int32, (half, half), 0)
    query_at = lax.broadcasted_iota(jnp.int32, (half, half), 1)
    causal = key_at <= query_at

    def slot_body(i, carry):
        here = rows_of(i * L, L)
        for j, dst in enumerate((q_s, k_s, v_s)):
            val = dot32(n1[here, :], wtb[:, j * DT : (j + 1) * DT], ONE) + vec_o[9 + j : 10 + j, 0:DT]
            if j < 2:
                val = (
                    val * rc_ref[...]
                    + pltpu.roll(val, DT - 8, 1) * ra_ref[...]
                    + pltpu.roll(val, 8, 1) * rb_ref[...]
                )
            vb = val.astype(bf16)
            if j == 0:
                q_s[...] = vb * bf16(0.125)
            else:
                dst[...] = vb
                (kT if j == 1 else vT)[...] = vb.T
        gc_s[...] = dot32(dys[here, :], wob[...], NT).astype(bf16)
        gk_a[...] = jnp.zeros_like(gk_a)
        gv_a[...] = jnp.zeros_like(gv_a)
        pump(i, 0)

        def head_body(h, c2):
            mine = (lane_head == h).astype(f32).astype(bf16)
            hrows = rows_of(h * HEAD_DIM, HEAD_DIM)
            for b in range(2):
                qs = pl.ds(b * half, half)
                kl = (b + 1) * half
                km = k_s[0:kl, :] * mine
                sT = dot32(km, q_s[qs, :], NT)
                diag = jnp.where(causal, sT[kl - half :], -1e30)
                sT = diag if b == 0 else jnp.concatenate([sT[: kl - half], diag], 0)
                e = jnp.exp(sT - jnp.max(sT, 0, keepdims=True))
                p = e * (1.0 / jnp.sum(e, 0, keepdims=True))
                pb = p.astype(bf16)
                ctxT[hrows, qs] = dot32(vT[hrows, 0:kl], pb, ONE).astype(bf16)
                gv_a[0:kl, :] += dot32(pb, gc_s[qs, :] * mine, ONE)
                gp = dot32(v_s[0:kl, :] * mine, gc_s[qs, :], NT)
                gs = (p * (gp - jnp.sum(p * gp, 0, keepdims=True))).astype(bf16)
                gk_a[0:kl, :] += dot32(gs, q_s[qs, :] * mine, ONE)
                gqT[hrows, qs] = dot32(kT[hrows, 0:kl], gs, ONE) * 0.125
            return c2

        lax.fori_loop(0, S, head_body, 0)
        pump(i, 1)
        for j in range(3):
            if j == 2:
                val = gv_a[...]
            else:
                val = gqT[...].T if j == 0 else gk_a[...]
                val = (
                    val * rc_ref[...]
                    - pltpu.roll(val, DT - 8, 1) * ra_ref[...]
                    - pltpu.roll(val, 8, 1) * rb_ref[...]
                )
            gt[here, j * DT : (j + 1) * DT] = val.astype(bf16)
        ctx_o[:, rows_of(i * L, L)] = ctxT[...]
        grad = dot32(ctxT[...], dys[here, :], ONE)

        @pl.when(i == 0)
        def _():
            wog[...] = grad

        @pl.when(i > 0)
        def _():
            wog[...] += grad

        if X > 1:
            @pl.when(i == 1)
            def _():
                for a in (0, 1):
                    token_copy(a, 2).wait_recv()
                    token_copy(a, 3).start()

        for nxt in range(1, T):
            @pl.when(i + 1 == nxt)
            def _():
                for a in (0, 1):
                    if nxt != 2:
                        token_copy(a, nxt).wait_recv()

        @pl.when(i + 1 < T)
        def _():
            norm_one(i + 1)

        return carry

    lax.fori_loop(0, T, slot_body, 0)
    outs = [
        local(xs, xg, loc.at[0]),
        local(dys, dyg, loc.at[1]),
        local(wtb, wt_o, loc.at[3]),
        local(wob, wo_o, loc.at[4]),
        local(gt, gt_o, loc.at[7]),
    ]
    for o in outs:
        o.start()
    for g, step in late[4 * T :]:
        g.event(step)
    ones = jnp.ones((8, T * L), bf16)
    tbg_o[...] = dot32(ones, gt[...], ONE)

    m = rows // R

    @pl.loop(0, S)
    def _(p):
        grad = dot32(n1[:, pl.ds(pl.multiple_of(p * rows, rows), rows)], gt[...], TN)
        for r in range(R):
            part = grad[r * m : (r + 1) * m]
            wtl[rows_of((r * S + p) * m, m), :] = part.astype(bf16)

            @pl.when(links.rep == r)
            def _():
                wth[rows_of(p * m, m), :] = part

    mo = HEAD_DIM // R
    for p in range(S):
        for r in range(R):
            part = wog[p * HEAD_DIM + r * mo : p * HEAD_DIM + (r + 1) * mo, :]
            wol[(r * S + p) * mo : (r * S + p + 1) * mo, :] = part.astype(bf16)

            @pl.when(links.rep == r)
            def _():
                woh[p * mo : (p + 1) * mo, :] = part

    last = [
        local(wtl, wtl_o, loc.at[8]),
        local(wth, wth_o, loc.at[9]),
        local(wol, wol_o, loc.at[10]),
        local(woh, woh_o, loc.at[11]),
    ]
    for o in last:
        o.start()
    for c in own_copies_late:
        c.wait()
    g_we.arrived()
    g_ws.arrived()
    for g in chunks:
        g.drain()
    for a in (0, 1):
        for slot in range(1, T):
            token_copy(a, slot).wait_send()
    for o in outs + last:
        o.wait()


def attention_phase(R, X, S, x, dy, wt, wo, we, ws, small, tables):
    L, D = x.shape
    T = 2 * X
    DT = S * HEAD_DIM
    FT = we.shape[1] // T
    fs = FT // S
    rows = D // S
    n = T * L
    sds = jax.ShapeDtypeStruct
    dma = pltpu.SemaphoreType.DMA
    outs = [
        sds((n, D), bf16), sds((n, D), bf16), sds((D, 3 * DT), bf16), sds((DT, D), bf16),
        sds((D, FT), bf16), sds((FT, D), bf16), sds((16, max(D, FT)), f32), sds((DT, n), bf16),
        sds((n, 3 * DT), bf16), sds((D, 3 * DT), bf16), sds((D // R, 3 * DT), f32),
        sds((DT, D), bf16), sds((DT // R, D), f32), sds((8, 3 * DT), f32),
    ]
    specs = [ANY] * 6 + [VM, VM] + [ANY] * 5 + [VM]
    vmem = pltpu.VMEM
    scratch = [
        vmem((n, D), bf16), vmem((n, D), bf16), vmem((n, D), bf16), vmem((n, 3 * DT), bf16),
        vmem((D, 3 * DT), bf16), vmem((DT, D), bf16), vmem((S * SMALL_ROWS, 128), f32),
        vmem((L, DT), bf16), vmem((L, DT), bf16), vmem((L, DT), bf16), vmem((L, DT), bf16),
        vmem((DT, L), bf16), vmem((DT, L), bf16), vmem((DT, L), bf16), vmem((DT, L), f32),
        vmem((L, DT), f32), vmem((L, DT), f32), vmem((D, 3 * DT), bf16), vmem((D // R, 3 * DT), f32),
        vmem((DT, D), bf16), vmem((DT // R, D), f32), vmem((DT, D), f32),
        vmem((L, DT), f32), vmem((L, DT), f32), vmem((L, DT), f32),
        vmem((rows, 3 * S * 128), f32), vmem((HEAD_DIM, D), f32), vmem((rows, FT), f32), vmem((fs, D), f32),
        vmem((rows, 3 * DT), bf16), vmem((HEAD_DIM, D), bf16), vmem((rows, FT), bf16), vmem((fs, D), bf16),
        dma((5, S, 2)), dma((5, S)), dma((5, S, R)), dma((5, S, R)), dma((2, 4)), dma((2, 4)), dma((12,)), dma((4 * S + 5,)),
    ]
    body = lambda *refs: attention_kernel(R, X, S, L, D, FT, *refs)
    return pl.pallas_call(
        body,
        name="attention_phase",
        out_shape=outs,
        in_specs=[ANY] * 10,
        out_specs=specs,
        scratch_shapes=scratch,
        compiler_params=pltpu.CompilerParams(
            collective_id=1, has_side_effects=True, vmem_limit_bytes=60 * 1024 * 1024
        ),
    )(x, dy, wt, wo, we, ws, small, *tables)


class GradSum:
    def __init__(self, links, blocks, m, bufs, sems, piece, only=None):
        self.k, self.B, self.m = links, blocks, m
        self.lo, self.keep, self.yr, self.zs, self.zr, self.fin = bufs
        self.sems, self.piece, self.only = sems, piece, only

    def across(self, f, dr):
        size = self.B * self.m
        r = lax.rem(self.k.rep + dr, self.k.R)
        return remote(
            self.lo.at[rows_of((f * self.k.R + r) * size, size)],
            self.yr.at[rows_of((f * (self.k.R - 1) + dr - 1) * size, size)],
            self.sems["ys"].at[f, dr], self.sems["yr"].at[f, dr], self.k.at_rep(dr),
        )

    def send_across(self, f):
        for dr in range(1, self.k.R):
            self.across(f, dr).start()

    def toward(self, f, p):
        b = 0 if self.only else p
        to = self.zr.at[rows_of(((0 if self.only else f) * self.k.S + self.k.z) * self.m, self.m)]
        return remote(
            self.zs.at[rows_of((f * self.B + b) * self.m, self.m)], to,
            self.sems["zs"].at[f, p], self.sems["zr"].at[f, self.k.z], self.k.at_z(p),
        )

    def owners(self, f, fn):
        if self.only:
            @pl.when(f != self.k.z)
            def _():
                fn(f)
        else:
            for dp in range(1, self.k.S):
                fn(lax.rem(self.k.z + dp, self.k.S))

    def if_owner(self, f, fn):
        if self.only:
            pl.when(f == self.k.z)(fn)
        else:
            fn()

    def sum_across(self, f):
        R, m = self.k.R, self.m
        for dr in range(1, R):
            self.across(f, dr).wait_recv()

        for b in range(self.B):
            at = rows_of((f * self.B + b) * m, m)
            total = self.keep[at, :]
            for dr in range(1, R):
                got = rows_of(((f * (R - 1) + dr - 1) * self.B + b) * m, m)
                total = total + self.yr[got, :].astype(f32)
            self.keep[at, :] = total
            self.zs[at, :] = total.astype(bf16)

        self.owners(f, lambda p: self.toward(f, p).start())

    def total(self, f):
        S, m = self.k.S, self.m

        def go():
            g = 0 if self.only else f
            at = rows_of((f * self.B + (0 if self.only else self.k.z)) * m, m)
            total = self.keep[at, :]
            for dp in range(1, S):
                p = lax.rem(self.k.z + dp, S)
                src = self.zr.at[rows_of((g * S + p) * m, m)]
                remote(src, src, self.sems["zs"].at[f, p], self.sems["zr"].at[f, p], self.k.at_z(p)).wait_recv()
                total = total + self.zr[rows_of((g * S + p) * m, m), :].astype(f32)
            fin = rows_of(g * m, m)
            self.fin[fin, :] = total.astype(bf16)
            src = self.fin.at[fin]
            local(src, self.piece(f, self.k.tx, self.k.core, self.k.rep), self.sems["gl"].at[f]).start()
            for c in self.spread(f, src, self.k.tx, self.k.rep, 0):
                c.start()

        self.if_owner(f, go)

    def spread(self, f, src, tx, r, stage):
        dst = self.piece(f, tx, self.k.core, r)
        src = dst if src is None else src
        out = []
        other = 1 if stage == 2 else 0
        out.append(
            remote(src, dst, self.sems["gcs"].at[f, other, r], self.sems["gcr"].at[f, other, r], self.k.at_core())
        )
        if stage < 2 and self.k.X > 1:
            out.append(remote(src, dst, self.sems["gxs"].at[f, r], self.sems["gxr"].at[f, r], self.k.at_tx()))
        if stage == 0:
            for dr in range(1, self.k.R):
                out.append(remote(src, dst, self.sems["gys"].at[f, dr], self.sems["gyr"].at[f, r], self.k.at_rep(dr)))
        return out

    def replicas(self, fn):
        for dr in range(1, self.k.R):
            fn(dr, lax.rem(self.k.rep + dr, self.k.R))

    def forward_rep(self, f):
        def go():
            def one(dr, r):
                b = self.piece(f, self.k.tx, self.k.core, r)
                remote(b, b, self.sems["gys"].at[f, dr], self.sems["gyr"].at[f, r], self.k.at_rep(dr)).wait_recv()
                for c in self.spread(f, None, self.k.tx, r, 1):
                    c.start()

            self.replicas(one)

        self.if_owner(f, go)

    def forward_tx(self, f):
        if self.k.X == 1:
            return

        def go():
            for r in range(self.k.R):
                b = self.piece(f, 1 - self.k.tx, self.k.core, r)
                remote(b, b, self.sems["gxs"].at[f, r], self.sems["gxr"].at[f, r], self.k.at_tx()).wait_recv()
                for c in self.spread(f, None, 1 - self.k.tx, r, 2):
                    c.start()

        self.if_owner(f, go)

    def finish(self, f):
        for dr in range(1, self.k.R):
            self.across(f, dr).wait_send()
        self.owners(f, lambda p: self.toward(f, p).wait_send())

        def go():
            src = self.fin.at[rows_of((0 if self.only else f) * self.m, self.m)]
            local(src, self.piece(f, self.k.tx, self.k.core, self.k.rep), self.sems["gl"].at[f]).wait()
            for c in self.spread(f, src, self.k.tx, self.k.rep, 0):
                c.wait_send()
            self.replicas(lambda dr, r: [c.wait_send() for c in self.spread(f, None, self.k.tx, r, 1)])
            for other in range(self.k.X):
                tx = self.k.tx if other == 0 else 1 - self.k.tx
                for r in range(self.k.R):
                    if other == 1:
                        for c in self.spread(f, None, tx, r, 2):
                            c.wait_send()
                    b = self.piece(f, tx, 1 - self.k.core, r)
                    remote(
                        b, b, self.sems["gcs"].at[f, other, r], self.sems["gcr"].at[f, other, r], self.k.at_core()
                    ).wait_recv()

        self.if_owner(f, go)


SEM_NAMES = ("ys", "yr", "zs", "zr", "gl", "gcs", "gcr", "gxs", "gxr", "gys", "gyr")


def grad_sems(count, R, X, S):
    dma = pltpu.SemaphoreType.DMA
    return [
        dma((count, R)), dma((count, R)), dma((count, S)), dma((count, S)), dma((count,)),
        dma((count, 2, R)), dma((count, 2, R)), dma((count, R)), dma((count, R)), dma((count, R)), dma((count, R)),
    ]


def feed_kernel(R, X, S, L, D, FT, *refs):
    (xg, dyg, wt_f, wo_f, we_f, ws_f, vec, ctx_i, gt_i, wtl, wth, wol, woh, tbg) = refs[:14]
    (out_o, ing_o, g_wt, g_wo, g_we, g_ws, v_o) = refs[14:21]
    rest = list(refs[21:])
    take = lambda count: [rest.pop(0) for _ in range(count)]
    (xb, dyb, n2b, actb, ghb, web, wsb, wob, ctb) = take(9)
    wt_bufs, wo_bufs, we_bufs, ws_bufs = take(5), take(5), take(6), take(6)
    (send_b, out_r, dx_r, xs_b, out_x, dx_x, vsum, vrecv) = take(8)
    sem_sets = [dict(zip(SEM_NAMES, take(len(SEM_NAMES)))) for _ in range(4)]
    (loc, tok, v_s, v_r, dxk) = take(5)
    T = 2 * X
    n = T * L
    rows = D // S
    DT = S * HEAD_DIM
    fs = FT // S
    k = Links(R, X, S)
    k.barrier(every_plane=True)
    rank = lambda tx, core: tx * 2 + core
    mt, mo, me, ms = rows // R, HEAD_DIM // R, rows // R, fs // R
    u_wt = GradSum(k, S, mt, [wtl] + wt_bufs, sem_sets[0],
                   lambda f, tx, c, r: g_wt.at[rows_of(rank(tx, c) * rows + r * mt, mt)])
    u_wo = GradSum(k, S, mo, [wol] + wo_bufs, sem_sets[1],
                   lambda f, tx, c, r: g_wo.at[rows_of(rank(tx, c) * HEAD_DIM + r * mo, mo)])
    u_we = GradSum(k, S, me, we_bufs, sem_sets[2],
                   lambda f, tx, c, r: g_we.at[rows_of(r * me, me), rows_of((f * T + rank(tx, c)) * fs, fs)])
    u_ws = GradSum(k, 1, ms, ws_bufs, sem_sets[3],
                   lambda f, tx, c, r: g_ws.at[rows_of(rank(tx, c) * fs + r * ms, ms)], only=True)
    first = (u_wt, u_wo)
    for u in first:
        u.send_across(0)

    def load_x(i, place):
        return local(xg.at[rows_of(i * L, L)], xb.at[pl.ds(place * L, L)], loc.at[place])

    load_x(0, 0).start()
    loads = [
        local(we_f, web, loc.at[2]), local(dyg, dyb, loc.at[3]), local(ws_f, wsb, loc.at[4]),
        local(wo_f, wob, loc.at[5]), local(ctx_i, ctb, loc.at[6]),
        local(wth, wt_bufs[0], loc.at[7]), local(woh, wo_bufs[0], loc.at[8]),
    ]
    for c in loads:
        c.start()

    gain1, gain2, shift2 = vec[0:1, 0:D], vec[2:3, 0:D], vec[3:4, 0:D]

    def norm_two(i, place):
        @pl.loop(0, L // 64)
        def _(b):
            n2b[rows_of(i * L + b * 64, 64), :] = (
                layer_norm_rows(xb[pl.ds(pl.multiple_of(place * L + b * 64, 64), 64), :]) * gain2 + shift2
            ).astype(bf16)

    for i in range(T):
        load_x(i, i % 2).wait()
        if i + 1 < T:
            load_x(i + 1, (i + 1) % 2).start()
        norm_two(i, i % 2)
    load_x(1, 0).start()
    for c in loads[:3]:
        c.wait()

    def hidden_body(it, carry):
        i, f = it // S, lax.rem(it, S)
        here, cols = rows_of(i * L, L), pl.ds(pl.multiple_of(f * fs, fs), fs)
        h = dot32(n2b[here, :], web[:, cols], ONE) + vec[8:9, cols]
        cdf = 0.5 * (1.0 + lax.erf(h * math.sqrt(0.5)))
        actb[here, cols] = (h * cdf).astype(bf16)
        slope = cdf + h * (jnp.exp(-0.5 * h * h) * (1.0 / math.sqrt(2.0 * math.pi)))
        ghb[here, cols] = (dot32(dyb[here, :], wsb[cols, :], NT) * slope).astype(bf16)
        return carry

    lax.fori_loop(0, T * S, hidden_body, 0)
    loads[3].wait()
    loads[4].wait()
    half = L // 2

    def feed_rows(i, b):
        at = i * L + b * half
        return dot32(actb[at : at + half, :], wsb[...], ONE) + dot32(ctb[:, at : at + half], wob[...], TN)

    def to_core(which, j):
        land = (out_r, dx_r)[which]
        return remote(
            send_b.at[pl.ds(j * L, L)], land.at[pl.ds(j * L, L)],
            tok.at[which, 0, j], tok.at[which, 1, j], k.at_core(),
        )

    def to_tx(which):
        return remote(
            xs_b.at[pl.ds(which * L, L)], (out_x, dx_x)[which], tok.at[which, 2, 0], tok.at[which, 2, 1], k.at_tx()
        )

    for j in range(X):
        for b in range(2):
            at = j * L + b * half
            send_b[at : at + half, :] = feed_rows(2 * j + 1, b).astype(bf16)
        to_core(0, j).start()
    if X > 1:
        to_core(0, 1).wait_recv()
        for b in range(2):
            got = out_r[L + b * half : L + (b + 1) * half, :].astype(f32)
            xs_b[b * half : (b + 1) * half, :] = (feed_rows(2, b) + got).astype(bf16)
        to_tx(0).start()

    for b in range(2):
        dxk[b * half : (b + 1) * half, :] = feed_rows(0, b)

    side = D // DT
    thirds = [wsb.at[pl.ds((j // side) * D, D), pl.ds((j % side) * DT, DT)] for j in range(3)]
    load_wt = [local(wt_f.at[:, pl.ds(j * DT, DT)], thirds[j], loc.at[(9, 11, 12)[j]]) for j in range(3)]
    for c in load_wt:
        c.start()

    def triple_back(at):
        total = None
        for j in range(0, 3, side):
            wide = min(side, 3 - j)
            part = dot32(
                actb[at, j * DT : (j + wide) * DT], wsb[(j // side) * D : (j // side + 1) * D, 0 : wide * DT], NT
            )
            total = part if total is None else total + part
        return total

    def store_grad(u, f, block, grad):
        for r in range(R):
            part = grad[r * u.m : (r + 1) * u.m]
            u.lo[rows_of(((f * R + r) * u.B + block) * u.m, u.m), :] = part.astype(bf16)

            @pl.when(k.rep == r)
            def _():
                u.keep[rows_of((f * u.B + block) * u.m, u.m), :] = part

    loads[5].wait()
    loads[6].wait()

    def chunk_body(f, carry):
        cols = pl.ds(pl.multiple_of(f * fs, fs), fs)
        store_grad(u_ws, f, 0, dot32(actb[:, cols], dyb[...], TN))
        u_ws.send_across(f)

        def block_body(p, c2):
            grad = dot32(n2b[:, pl.ds(pl.multiple_of(p * rows, rows), rows)], ghb[:, cols], TN)
            store_grad(u_we, f, p, grad)
            return c2

        lax.fori_loop(0, S, block_body, 0)
        u_we.send_across(f)

        @pl.when(f == 0)
        def _():
            for u in first:
                u.sum_across(0)

        return carry

    lax.fori_loop(0, S, chunk_body, 0)
    gtb = actb.at[:, pl.ds(0, 3 * DT)]
    load_gt = local(gt_i, gtb, loc.at[10])
    load_gt.start()
    for j in range(X):
        to_core(0, j).wait_send()
    load_gt.wait()
    for c in load_wt:
        c.wait()

    def pair(step, f):
        for u in (u_we, u_ws):
            getattr(u, step)(f)

    vsum[...] = jnp.zeros_like(vsum)

    def slot_grad(i, place, finish):
        for b in range(2):
            at = pl.ds(i * L + b * half, half)
            xhat = layer_norm_rows(xb[place * L + b * half : place * L + (b + 1) * half, :])
            g1 = triple_back(at)
            vsum[0:1, 0:D] += jnp.sum(g1 * xhat, 0, keepdims=True)
            vsum[1:2, 0:D] += jnp.sum(g1, 0, keepdims=True)
            g2 = dot32(ghb[at, :], web[...], NT)
            vsum[2:3, 0:D] += jnp.sum(g2 * xhat, 0, keepdims=True)
            vsum[3:4, 0:D] += jnp.sum(g2, 0, keepdims=True)
            finish(b, g1 * gain1 + g2 * gain2, xhat)

    order = [2 * j + 1 for j in range(X)] + ([2] if X > 1 else []) + [0]
    events = [("sum_across", f) for f in range(S)]
    for turn, i in enumerate(order):
        place = turn % 2
        load_x(i, place).wait()
        if turn + 1 < T:
            load_x(order[turn + 1], 1 - place).start()
        if i % 2 == 1:
            j = i // 2

            def finish(b, val, xhat):
                at = j * L + b * half
                send_b[at : at + half, :] = val.astype(bf16)

            slot_grad(i, place, finish)
            to_core(1, j).start()
        elif i == 2:
            to_core(1, 1).wait_recv()

            def finish(b, val, xhat):
                got = dx_r[L + b * half : L + (b + 1) * half, :].astype(f32)
                xs_b[L + b * half : L + (b + 1) * half, :] = (val + got).astype(bf16)

            slot_grad(2, place, finish)
            to_tx(1).start()
            pair("sum_across", 0)
            for u in first:
                u.total(0)
        else:
            to_core(0, 0).wait_recv()
            to_core(1, 0).wait_recv()
            if X > 1:
                to_tx(0).wait_recv()
            for j in range(X):
                to_core(1, j).wait_send()
            for b in range(2):
                rows_b = slice(b * half, (b + 1) * half)
                total = dxk[rows_b, :] + out_r[rows_b, :].astype(f32)
                if X > 1:
                    total = total + out_x[rows_b, :].astype(f32)
                total = total + xb[place * L + b * half : place * L + (b + 1) * half, :].astype(f32)
                send_b[rows_b, :] = (total + (vec[4:5, 0:D] + vec[5:6, 0:D])).astype(bf16)
            save_out = local(send_b.at[pl.ds(0, L)], out_o, loc.at[2])
            save_out.start()

            def finish(b, val, xhat):
                rows_b = slice(b * half, (b + 1) * half)
                dxk[rows_b, :] = val + dx_r[rows_b, :].astype(f32)

            slot_grad(0, place, finish)
            place0 = place
    ones = jnp.ones((8, L), bf16)
    vsum[4:5, 0:D] = dot32(ones, dyb[0:L, :], ONE)[0:1]
    mine = rank(k.tx, k.core)
    eb = dot32(jnp.ones((8, n), bf16), ghb[...], ONE)[0:1]
    for t in range(T):
        @pl.when(mine == t)
        def _():
            vsum[5 + t : 6 + t, 0 : 3 * DT] = tbg[0:1, :]
            vsum[5 + T + t : 6 + T + t, 0:FT] = eb

    def exchange(stage, copies):
        for c in copies:
            c.start()
        for c in copies:
            c.wait()
        for q in range(len(copies)):
            vsum[...] += vrecv[stage + q]

    at_stage = 0
    exchange(0, [remote(vsum, vrecv.at[0], v_s.at[0], v_r.at[0], k.at_core())])
    at_stage = 1
    if X > 1:
        exchange(1, [remote(vsum, vrecv.at[1], v_s.at[1], v_r.at[1], k.at_tx())])
        at_stage = 2
    rep_copies = [
        remote(vsum, vrecv.at[at_stage + dr - 1], v_s.at[at_stage + dr - 1], v_r.at[at_stage + dr - 1], k.at_rep(dr))
        for dr in range(1, R)
    ]
    exchange(at_stage, rep_copies)
    at_stage += R - 1
    pair("sum_across", 1)
    for u in first:
        u.forward_rep(0)
    z_copies = [
        remote(
            vsum, vrecv.at[at_stage + dz - 1], v_s.at[at_stage + dz - 1], v_r.at[at_stage + dz - 1],
            k.at_z(lax.rem(k.z + dz, S)),
        )
        for dz in range(1, S)
    ]
    for c in z_copies:
        c.start()
    pair("total", 0)
    for f in range(2, S):
        pair("sum_across", f)
        if f == 2:
            for u in first:
                u.forward_tx(0)
        pair("total", f - 1)
        pair("forward_rep", f - 2)
        if f > 2:
            pair("forward_tx", f - 3)
    for c in z_copies:
        c.wait()
    total = vsum[...]
    for q in range(S - 1):
        total = total + vrecv[at_stage + q]
    v_o[...] = total
    if X > 1:
        to_tx(1).wait_recv()
    for b in range(2):
        rows_b = slice(b * half, (b + 1) * half)
        dx = dxk[rows_b, :]
        if X > 1:
            dx = dx + dx_x[rows_b, :].astype(f32)
        xf = xb[place0 * L + b * half : place0 * L + (b + 1) * half, :].astype(f32)
        cen = xf - jnp.mean(xf, -1, keepdims=True)
        rstd = lax.rsqrt(jnp.mean(cen * cen, -1, keepdims=True) + eps_norm)
        xhat = cen * rstd
        back = dx - jnp.mean(dx, -1, keepdims=True) - xhat * jnp.mean(dx * xhat, -1, keepdims=True)
        send_b[L + b * half : L + (b + 1) * half, :] = (dyb[rows_b, :].astype(f32) + rstd * back).astype(bf16)
    save_ing = local(send_b.at[pl.ds(L, L)], ing_o, loc.at[3])
    save_ing.start()
    pair("total", S - 1)
    pair("forward_rep", S - 2)
    pair("forward_tx", S - 3)
    pair("forward_rep", S - 1)
    pair("forward_tx", S - 2)
    pair("forward_tx", S - 1)
    for u in first:
        u.finish(0)
    for f in range(S):
        pair("finish", f)
    if X > 1:
        to_tx(0).wait_send()
        to_tx(1).wait_send()
    save_out.wait()
    save_ing.wait()


def feed_phase(R, X, S, F, xg, dyg, wt_f, wo_f, we_f, ws_f, vecs, ctxT, gt, wtl, wth, wol, woh, tbg):
    T = 2 * X
    n, D = xg.shape
    L = n // T
    DT = S * HEAD_DIM
    FT = we_f.shape[1]
    fs = FT // S
    rows = D // S
    mt, mo, me, ms = rows // R, HEAD_DIM // R, rows // R, fs // R
    W = max(D, 3 * DT, FT)
    sds = jax.ShapeDtypeStruct
    vmem = pltpu.VMEM
    dma = pltpu.SemaphoreType.DMA
    outs = [
        sds((L, D), bf16), sds((L, D), bf16), sds((T * rows, 3 * DT), bf16), sds((rows, D), bf16),
        sds((rows, F), bf16), sds((F // S, D), bf16), sds((16, W), f32),
    ]

    def bufs(count, B, m, cols, lo, landing):
        made = [vmem((count * R * B * m, cols), bf16)] if lo else []
        return made + [
            vmem((count * B * m, cols), f32), vmem((count * (R - 1) * B * m, cols), bf16),
            vmem((count * B * m, cols), bf16), vmem((landing * S * m, cols), bf16), vmem((landing * m, cols), bf16),
        ]

    scratch = [
        vmem((2 * L, D), bf16), vmem((n, D), bf16), vmem((n, D), bf16), vmem((n, FT), bf16), vmem((n, FT), bf16),
        vmem((D, FT), bf16), vmem((FT, D), bf16), vmem((DT, D), bf16),
        vmem((DT, n), bf16),
    ]
    scratch += bufs(1, S, mt, 3 * DT, False, 1) + bufs(1, S, mo, D, False, 1)
    scratch += bufs(S, S, me, fs, True, S) + bufs(S, 1, ms, D, True, 1)
    scratch += [
        vmem((2 * L, D), bf16), vmem((X * L, D), bf16), vmem((X * L, D), bf16), vmem((2 * L, D), bf16),
        vmem((L, D), bf16), vmem((L, D), bf16), vmem((16, W), f32), vmem((2 + R - 1 + S - 1, 16, W), f32),
    ]
    for count in (1, 1, S, S):
        scratch += grad_sems(count, R, X, S)
    scratch += [dma((13,)), dma((2, 3, 2)), dma((2 + R - 1 + S - 1,)), dma((2 + R - 1 + S - 1,)), vmem((L, D), f32)]
    body = lambda *refs: feed_kernel(R, X, S, L, D, FT, *refs)
    return pl.pallas_call(
        body,
        name="feed_phase",
        out_shape=outs,
        in_specs=[ANY] * 6 + [VM] + [ANY] * 6 + [VM],
        out_specs=[ANY] * 6 + [VM],
        scratch_shapes=scratch,
        compiler_params=pltpu.CompilerParams(
            collective_id=2, has_side_effects=True, vmem_limit_bytes=67_000_000
        ),
    )(xg, dyg, wt_f, wo_f, we_f, ws_f, vecs, ctxT, gt, wtl, wth, wol, woh, tbg)


def adam_kernel(S, T, heads, *refs):
    g_ref, w_ref, m_ref, v_ref, g_o, w_o, m_o, v_o = refs

    def one(at, g):
        new_w, _, new_m, new_v = adam_step(w_ref[:, at], g, m_ref[:, at], v_ref[:, at], True)
        g_o[:, at] = g
        w_o[:, at] = new_w
        m_o[:, at] = new_m
        v_o[:, at] = new_v

    if not heads:
        one(slice(None), g_ref[...].astype(f32))
        return
    lane = lax.broadcasted_iota(jnp.int32, (1, 128), 1)
    DT = S * HEAD_DIM
    for j in range(3):
        for p in range(S):
            src = j * DT + (p // 2) * 128
            for u in range(T // 2):
                low = g_ref[2 * u, :, src : src + 128].astype(f32)
                high = g_ref[2 * u + 1, :, src : src + 128].astype(f32)
                if p % 2 == 1:
                    low = pltpu.roll(low, HEAD_DIM, 1)
                else:
                    high = pltpu.roll(high, HEAD_DIM, 1)
                to = ((j * S + p) * T + 2 * u) * HEAD_DIM
                one(slice(to, to + 128), jnp.where(lane < HEAD_DIM, low, high))


def adam_matrix(S, T, g, w, m, v, heads, rows_each):
    n, cols = w.shape
    spec = pl.BlockSpec((rows_each, cols), lambda i: (i, 0))
    g_spec = pl.BlockSpec((T, rows_each, g.shape[-1]), lambda i: (0, i, 0)) if heads else spec
    return pl.pallas_call(
        lambda *refs: adam_kernel(S, T, heads, *refs),
        name="adam_matrix",
        grid=(n // rows_each,),
        out_shape=[jax.ShapeDtypeStruct((n, cols), f32)] * 4,
        in_specs=[g_spec, spec, spec, spec],
        out_specs=[spec] * 4,
        compiler_params=pltpu.CompilerParams(vmem_limit_bytes=40 * 1024 * 1024),
    )(g, w, m, v)


TP = ("tx", "core")


def make_step(R, X, S):
    T = 2 * X

    def step(*args):
        x, dy = args[0], args[1]
        masters, momenta, variances = args[2:14], args[14:26], args[26:38]
        L, D = x.shape
        H = D // HEAD_DIM
        t = lax.axis_index(TP)
        z = lax.axis_index("shard")
        rep = lax.axis_index("rep")
        wt, wo, we, ws = masters[4], masters[6], masters[8], masters[10]
        rows = wt.shape[0]
        F = we.shape[1]
        fs = F // S // T
        HT = H // T

        eb_own = lax.dynamic_slice_in_dim(masters[9], t * fs, fs, 0)
        packed = [masters[i] for i in (0, 1, 2, 3, 7, 11)] + [eb_own, masters[5]]
        width = sum(v.shape[0] for v in packed)
        packed.append(jnp.zeros((SMALL_ROWS * 128 - width,), f32))
        small = lax.reduce_precision(jnp.concatenate(packed).reshape(SMALL_ROWS, 128), 8, 7)

        cosine, sine = rotary_tables(L)
        zero, one = jnp.zeros((L, 8), f32), jnp.ones((L, HEAD_DIM - 16), f32)
        pad = jnp.zeros((L, HEAD_DIM - 16), f32)
        tables = (
            jnp.tile(jnp.concatenate([cosine, cosine, one], 1), (1, S)),
            jnp.tile(jnp.concatenate([-sine, zero, pad], 1), (1, S)),
            jnp.tile(jnp.concatenate([zero, sine, pad], 1), (1, S)),
        )
        passed = attention_phase(R, X, S, x, dy, wt, wo, we, ws, small, tables)
        out, in_grad, wt_s, wo_s, we_s, ws_s, vec = feed_phase(R, X, S, F, *passed)
        wt_s = wt_s.reshape(T, rows, -1)
        DT, FT = S * HEAD_DIM, F // T
        tb_g = vec[5 : 5 + T, : 3 * DT].reshape(T, 3, S, HEAD_DIM).transpose(1, 2, 0, 3).reshape(-1)
        eb_g = vec[5 + T : 5 + 2 * T, :FT].reshape(T, S, fs).transpose(1, 0, 2).reshape(-1)

        def own(v):
            return lax.dynamic_slice_in_dim(v, z * (v.shape[0] // S), v.shape[0] // S, 0)

        vown = [own(vec[i, :D]) for i in range(5)] + [own(tb_g), own(eb_g)]
        done = {}
        for i, g, each in ((4, wt_s, 64), (6, wo_s, 128), (8, we_s, 64), (10, ws_s, 256)):
            each = min(each, g.shape[-2])
            done[i] = adam_matrix(S, T, g, masters[i], momenta[i], variances[i], i == 4, each)
        summed = [
            vown[0], vown[1], vown[2], vown[3], None, vown[5], None, vown[4], None, vown[6], None, vown[4],
        ]
        updated, ones, twos = [], [], []
        for i in range(12):
            if i in done:
                summed[i] = done[i][0]
                for kept, val in zip((updated, ones, twos), done[i][1:]):
                    kept.append(val)
                continue
            new_weight, delta, m_new, v_new = adam_step(
                masters[i], summed[i], momenta[i], variances[i], i in (4, 6, 8, 10)
            )
            updated.append(delta if i in (0, 2) else new_weight)
            ones.append(m_new)
            twos.append(v_new)
        return (out, in_grad, *summed, *updated, *ones, *twos)

    return step


def solution(mesh):
    G, S = mesh.shape["grp"], mesh.shape["shard"]
    X = 2 if S <= 4 else 1
    R = G // (2 * X)
    full = Mesh(mesh.devices.reshape(R, X, 2, S), ("rep", "tx", "core", "shard"))
    tok = P(("rep", "tx", "core", "shard"), None)
    vecs, mats = P("shard"), P("shard", None)
    group = tuple(mats if i in (4, 6, 8, 10) else vecs for i in range(12))
    return jax.shard_map(
        make_step(R, X, S),
        mesh=full,
        in_specs=(tok, tok) + group * 3,
        out_specs=(tok, tok) + group * 4,
        check_vma=False,
    )
```

```python
import math

import jax
import jax.numpy as jnp
import numpy as np
from jax import lax
from jax.experimental import pallas as pl
from jax.experimental.pallas import tpu as pltpu
from jax.sharding import Mesh, PartitionSpec as P

HEAD_DIM = 64
ROTARY = 16
STEP = 10
eps_norm = 1e-05
rope_base = 10000.0
beta_one = 0.9
beta_two = 0.95
learn_rate = 0.01
adam_eps = 1e-08
weight_decay = 0.01

bf16 = jnp.bfloat16
f32 = jnp.float32


def adam_step(weight, gradient, momentum, variance, decayed):
    momentum_new = beta_one * momentum + (1.0 - beta_one) * gradient
    variance_new = beta_two * variance + (1.0 - beta_two) * gradient * gradient
    mean_hat = momentum_new / (1.0 - beta_one**STEP)
    var_hat = variance_new / (1.0 - beta_two**STEP)
    change = mean_hat / (jnp.sqrt(var_hat) + adam_eps)
    if decayed:
        change = change + weight_decay * weight
    delta = -learn_rate * change
    return (weight + delta, delta, momentum_new, variance_new)


def rotary_tables(length):
    position = np.arange(length, dtype=np.float32)[:, None]
    half = ROTARY // 2
    inverse_freq = np.float32(rope_base) ** (-(np.arange(half, dtype=np.float32) * np.float32(2.0) / np.float32(ROTARY)))
    angles = position * inverse_freq[None, :].astype(np.float32)
    cosine, sine = np.cos(angles), np.sin(angles)
    rest = np.zeros((length, HEAD_DIM - 2 * ROTARY), np.float32)
    head = np.concatenate([cosine, cosine, -sine, sine, rest], 1)
    return np.concatenate([head[: length // 2], head[length // 2 :]], 1).astype(np.float32)


def dot32(a, b, dims):
    return lax.dot_general(a, b, (dims, ((), ())), preferred_element_type=f32)


MESH = pl.DeviceIdType.MESH
ANY = pl.BlockSpec(memory_space=pl.ANY)
VM = pl.BlockSpec(memory_space=pltpu.VMEM)
ONE = ((1,), (0,))
NT = ((1,), (1,))
TN = ((0,), (0,))


def rows_of(start, size):
    return pl.ds(pl.multiple_of(start, math.gcd(size, 512)), size)


class Links:
    def __init__(self, R, X, S):
        self.R, self.X, self.S = R, X, S
        self.rep = lax.axis_index("rep")
        self.tx = lax.axis_index("tx")
        self.core = lax.axis_index("core")
        self.z = lax.axis_index("shard")

    def at_core(self):
        return {"core": 1 - self.core}

    def at_tx(self):
        return {"tx": 1 - self.tx}

    def at_rep(self, dr):
        return {"rep": lax.rem(self.rep + dr, self.R)}

    def at_z(self, z):
        return {"shard": z}

    def barrier(self, every_plane=False):
        sem = pltpu.get_barrier_semaphore()

        def tell(where):
            pl.semaphore_signal(sem, inc=1, device_id=where, device_id_type=MESH)

        count = 1 + (self.X - 1) + (self.R - 1)
        tell(self.at_core())
        if self.X > 1:
            tell(self.at_tx())
        for dr in range(1, self.R):
            tell(self.at_rep(dr))

        if every_plane:
            for dz in range(1, self.S):
                tell(self.at_z(lax.rem(self.z + dz, self.S)))
            pl.semaphore_wait(sem, count + self.S - 1)
            return

        @pl.when(self.z > 0)
        def _():
            tell(self.at_z(self.z - 1))

        @pl.when(self.z < self.S - 1)
        def _():
            tell(self.at_z(self.z + 1))

        ends = (self.z > 0).astype(jnp.int32) + (self.z < self.S - 1).astype(jnp.int32)
        pl.semaphore_wait(sem, count + ends)


def remote(src, dst, send, recv, where):
    return pltpu.make_async_remote_copy(
        src_ref=src, dst_ref=dst, send_sem=send, recv_sem=recv, device_id=where, device_id_type=MESH
    )


def local(src, dst, sem):
    return pltpu.make_async_copy(src, dst, sem)


class LineGather:
    def __init__(self, links, own, buf, n, zs, zr, ys, yr, split):
        self.k = links
        self.own, self.buf, self.n = own, buf, n
        self.parts = links.R if split else 1
        self.m = n // self.parts
        self.zs, self.zr, self.ys, self.yr = zs, zr, ys, yr

    def block(self, p, r):
        return self.buf.at[rows_of(p * self.n + r * self.m, self.m)]

    def mine(self):
        return self.k.rep if self.parts > 1 else 0

    def hop(self, src, p, step, way):
        to = self.k.z + 1 if way == 0 else self.k.z - 1
        return remote(
            src, self.block(p, self.mine()), self.zs.at[step, way], self.zr.at[p], self.k.at_z(to)
        )

    def across(self, p, dr):
        b = self.block(p, self.k.rep)
        return remote(b, b, self.ys.at[p, dr], self.yr.at[p, self.k.rep], self.k.at_rep(dr))

    def each_way(self, step, fn):
        z, S = self.k.z, self.k.S
        for way in (0, 1):
            p = z - step if way == 0 else z + step
            here = (step <= z) if way == 0 else (z + step <= S - 1)
            on = (z < S - 1) if way == 0 else (z > 0)
            fn(way, p, here, on)

    def start(self):
        mine = self.mine()

        def go(way, p, here, on):
            @pl.when(on)
            def _():
                self.hop(self.own.at[rows_of(mine * self.m, self.m)], p, 0, way).start()

        self.each_way(0, go)

    def event(self, step):
        def go(way, p, here, on):
            @pl.when(here)
            def _():
                b = self.block(p, self.mine())
                self.hop(b, p, step, way).wait_recv()

                @pl.when(on)
                def _():
                    self.hop(b, p, step, way).start()

                if self.parts > 1:
                    for dr in range(1, self.k.R):
                        self.across(p, dr).start()

        self.each_way(step, go)

    def arrived(self):
        if self.parts == 1:
            return
        for p in range(self.k.S):
            @pl.when(p != self.k.z)
            def _():
                for dr in range(1, self.k.R):
                    r = lax.rem(self.k.rep + dr, self.k.R)
                    b = self.block(p, r)
                    remote(b, b, self.ys.at[p, dr], self.yr.at[p, r], self.k.at_rep(dr)).wait_recv()

    def drain(self):
        for step in range(self.k.S):
            def go(way, p, here, on):
                @pl.when(jnp.logical_and(here, on))
                def _():
                    self.hop(self.block(p, self.mine()), p, step, way).wait_send()

                if step > 0 and self.parts > 1:
                    @pl.when(here)
                    def _():
                        for dr in range(1, self.k.R):
                            self.across(p, dr).wait_send()

            self.each_way(step, go)


def layer_norm_rows(xb):
    xf = xb.astype(f32)
    cen = xf - jnp.mean(xf, -1, keepdims=True)
    return cen * lax.rsqrt(jnp.mean(cen * cen, -1, keepdims=True) + eps_norm)


SMALL_ROWS = 24


def small_row(sm, S, first, count):
    return jnp.concatenate(
        [sm[p * SMALL_ROWS + first + j : p * SMALL_ROWS + first + j + 1, :] for p in range(S) for j in range(count)],
        -1,
    )


def attention_kernel(R, X, S, L, D, FT, *refs):
    (x_ref, dy_ref, wt_m, wo_m, we_m, ws_m, sm_ref, turn_i) = refs[:8]
    (xg, dyg, wt_o, wo_o, we_o, ws_o, vec_o, ctx_o, gt_o, wtl_o, wth_o, wol_o, woh_o, tbg_o, n2_o) = refs[8:23]
    (
        xs, dys, n1, n2, gt, wtb, wob, smb, q_s, k_s, v_s, gc_s, kT, vT, ctxT, gqT, gk_a, gv_a, wtl, wth, wol, woh, wog,
        turn_s, turn_p, wt_w, wo_w, we_w, ws_w, wt_ref, wo_ref, we_ref, ws_ref,
        zs, zr, ys, yr, tok_s, tok_r, loc, cut,
    ) = refs[23:]
    T = 2 * X
    rows = D // S
    DT = S * HEAD_DIM
    links = Links(R, X, S)
    chunks = []
    for c, (own, buf) in enumerate(
        [(sm_ref, smb), (wt_ref, wtb), (wo_ref, wob), (we_ref, we_o), (ws_ref, ws_o)]
    ):
        chunks.append(
            LineGather(links, own, buf, own.shape[0], zs.at[c], zr.at[c], ys.at[c], yr.at[c], c > 0)
        )
    g_sm, g_wt, g_wo, g_we, g_ws = chunks
    lane = lax.broadcasted_iota(jnp.int32, (1, 128), 1)
    rank = links.tx * 2 + links.core
    fs = FT // S
    cuts = [[], [local(wo_m.at[rows_of(rank * HEAD_DIM, HEAD_DIM)], wo_w, cut.at[3 * S])], [],
            [local(ws_m.at[rows_of(rank * fs, fs)], ws_w, cut.at[3 * S + 1])]]
    for j in range(3):
        for p in range(S):
            block = ((j * S + p) * T + rank) // 2
            cuts[0].append(
                local(
                    wt_m.at[:, pl.ds(pl.multiple_of(block * 128, 128), 128)],
                    wt_w.at[:, pl.ds((j * S + p) * 128, 128)],
                    cut.at[j * S + p],
                )
            )
    for p in range(S):
        cuts[2].append(
            local(
                we_m.at[:, pl.ds(pl.multiple_of((p * T + rank) * fs, fs), fs)],
                we_w.at[:, pl.ds(p * fs, fs)],
                cut.at[3 * S + 2 + p],
            )
        )
    for group in cuts:
        for c in group:
            c.start()
    links.barrier()
    for c in cuts[0]:
        c.wait()

    def half_lanes(block, odd):
        val = wt_w[:, block * 128 : (block + 1) * 128]
        return jnp.where(lax.rem(rank, 2) == odd, val, pltpu.roll(val, HEAD_DIM, 1))

    for b in range(3 * S // 2):
        both = jnp.where(lane < HEAD_DIM, half_lanes(2 * b, 0), half_lanes(2 * b + 1, 1))
        wt_ref[:, b * 128 : (b + 1) * 128] = both.astype(bf16)
    cuts[1][0].wait()
    wo_ref[...] = wo_w[...].astype(bf16)

    own_copies = [
        local(x_ref, xs.at[pl.ds(0, L)], loc.at[0]),
        local(dy_ref, dys.at[pl.ds(0, L)], loc.at[1]),
    ]
    own_copies_late = []
    for c, g in enumerate(chunks):
        (own_copies if c < 3 else own_copies_late).append(local(g.own, g.buf.at[rows_of(links.z * g.n, g.n)], loc.at[2 + c]))

    def token_copy(a, slot):
        buf = (xs, dys)[a]
        src = (x_ref, dy_ref)[a]
        if slot == 1:
            return remote(src, buf.at[pl.ds(L, L)], tok_s.at[a, 1], tok_r.at[a, 1], links.at_core())
        if slot == 2:
            return remote(src, buf.at[pl.ds(2 * L, L)], tok_s.at[a, 2], tok_r.at[a, 2], links.at_tx())
        return remote(
            buf.at[pl.ds(2 * L, L)], buf.at[pl.ds(3 * L, L)], tok_s.at[a, 3], tok_r.at[a, 3], links.at_core()
        )

    g_sm.start()
    g_wt.start()
    g_wo.start()
    if X > 1:
        token_copy(0, 2).start()
        token_copy(1, 2).start()
    token_copy(0, 1).start()
    token_copy(1, 1).start()
    for c in own_copies:
        c.start()

    tables = [local(turn_i, turn_p, cut.at[4 * S + 2])]

    def table(q):
        return jnp.concatenate([turn_s[q * L : (q + 1) * L, :]] * (DT // 128), 1)

    for c in tables:
        c.start()
    for c in cuts[2] + cuts[3]:
        c.wait()
    we_ref[...] = we_w[...].astype(bf16)
    ws_ref[...] = ws_w[...].astype(bf16)
    for c in own_copies_late:
        c.start()
    own_copies[0].wait()
    own_copies[2].wait()
    for step in range(1, S):
        g_sm.event(step)
    per = rows // 128
    vec_o[...] = jnp.zeros_like(vec_o)
    sm = smb[...]
    for j in range(6):
        vec_o[j : j + 1, 0:D] = small_row(sm, S, j * per, per)
    fper = FT // S // 128
    vec_o[8 : 8 + 1, 0:FT] = small_row(sm, S, 6 * per, fper)
    def head_bias(j, p):
        block = j * (D // 128) + (T * p + rank) // 2
        at = (block // (3 * per)) * SMALL_ROWS + 6 * per + fper + lax.rem(block, 3 * per)
        row = smb[pl.ds(at, 1), :]
        return jnp.where(lax.rem(rank, 2) == p % 2, row, pltpu.roll(row, HEAD_DIM, 1))

    for j in range(3):
        for a in range(S // 2):
            both = jnp.where(lane < HEAD_DIM, head_bias(j, 2 * a), head_bias(j, 2 * a + 1))
            vec_o[9 + j : 10 + j, a * 128 : (a + 1) * 128] = both

    def norm_one(i):
        gain, shift = vec_o[0:1, 0:D], vec_o[1:2, 0:D]
        gain_b, shift_b = vec_o[2:3, 0:D], vec_o[3:4, 0:D]

        @pl.loop(0, L // 64)
        def _(b):
            at = rows_of(i * L + b * 64, 64)
            xhat = layer_norm_rows(xs[at, :])
            n1[at, :] = (xhat * gain + shift).astype(bf16)
            n2[at, :] = (xhat * gain_b + shift_b).astype(bf16)

    norm_one(0)
    g_wt.event(1)
    g_wo.event(1)
    g_we.start()
    for step in range(2, S):
        g_wt.event(step)
        g_wo.event(step)
    g_ws.start()
    own_copies[1].wait()
    own_copies[3].wait()
    own_copies[4].wait()
    for c in tables:
        c.wait()
    packed_turn = turn_p[...]
    other_turn = pltpu.roll(packed_turn, HEAD_DIM, 1)
    entry = lax.rem(lane, HEAD_DIM)
    for b in range(2):
        near, far = (packed_turn, other_turn) if b == 0 else (other_turn, packed_turn)
        full = jnp.where(lane < HEAD_DIM, near, far)
        moved = pltpu.roll(full, 128 - ROTARY, 1)
        at = b * (L // 2)
        turn_s[at : at + L // 2, :] = jnp.where(entry < ROTARY, full, 1.0)
        turn_s[L + at : L + at + L // 2, :] = jnp.where(entry < ROTARY // 2, moved, 0.0)
        upper = jnp.logical_and(entry >= ROTARY // 2, entry < ROTARY)
        turn_s[2 * L + at : 2 * L + at + L // 2, :] = jnp.where(upper, moved, 0.0)
    g_wt.arrived()
    g_wo.arrived()
    late = [(g, step) for step in range(1, S) for g in (g_we, g_ws)]

    def pump(i, turn):
        for index in range(T):
            at = 2 * (2 * index + turn) - 2
            todo = late[max(at, 0) : at + 2]
            if todo:
                @pl.when(i == index)
                def _():
                    for g, step in todo:
                        g.event(step)

    half = L // 2
    lane_head = lax.broadcasted_iota(jnp.int32, (1, DT), 1) // HEAD_DIM
    key_at = lax.broadcasted_iota(jnp.int32, (half, half), 0)
    query_at = lax.broadcasted_iota(jnp.int32, (half, half), 1)
    causal = key_at <= query_at

    def slot_body(i, carry):
        here = rows_of(i * L, L)
        for j, dst in enumerate((q_s, k_s, v_s)):
            val = dot32(n1[here, :], wtb[:, j * DT : (j + 1) * DT], ONE) + vec_o[9 + j : 10 + j, 0:DT]
            if j < 2:
                val = (
                    val * table(0)
                    + pltpu.roll(val, DT - 8, 1) * table(1)
                    + pltpu.roll(val, 8, 1) * table(2)
                )
            vb = val.astype(bf16)
            if j == 0:
                q_s[...] = vb * bf16(0.125)
            else:
                dst[...] = vb
                (kT if j == 1 else vT)[...] = vb.T
        gc_s[...] = dot32(dys[here, :], wob[...], NT).astype(bf16)
        gk_a[...] = jnp.zeros_like(gk_a)
        gv_a[...] = jnp.zeros_like(gv_a)
        pump(i, 0)

        def head_body(h, c2):
            mine = (lane_head == h).astype(f32).astype(bf16)
            hrows = rows_of(h * HEAD_DIM, HEAD_DIM)
            for b in range(2):
                qs = pl.ds(b * half, half)
                kl = (b + 1) * half
                km = k_s[0:kl, :] * mine
                sT = dot32(km, q_s[qs, :], NT)
                diag = jnp.where(causal, sT[kl - half :], -1e30)
                sT = diag if b == 0 else jnp.concatenate([sT[: kl - half], diag], 0)
                e = jnp.exp(sT - jnp.max(sT, 0, keepdims=True))
                p = e * (1.0 / jnp.sum(e, 0, keepdims=True))
                pb = p.astype(bf16)
                ctxT[hrows, qs] = dot32(vT[hrows, 0:kl], pb, ONE).astype(bf16)
                gv_a[0:kl, :] += dot32(pb, gc_s[qs, :] * mine, ONE)
                gp = dot32(v_s[0:kl, :] * mine, gc_s[qs, :], NT)
                gs = (p * (gp - jnp.sum(p * gp, 0, keepdims=True))).astype(bf16)
                gk_a[0:kl, :] += dot32(gs, q_s[qs, :] * mine, ONE)
                gqT[hrows, qs] = dot32(kT[hrows, 0:kl], gs, ONE) * 0.125
            return c2

        lax.fori_loop(0, S, head_body, 0)
        pump(i, 1)
        for j in range(3):
            if j == 2:
                val = gv_a[...]
            else:
                val = gqT[...].T if j == 0 else gk_a[...]
                val = (
                    val * table(0)
                    - pltpu.roll(val, DT - 8, 1) * table(1)
                    - pltpu.roll(val, 8, 1) * table(2)
                )
            gt[here, j * DT : (j + 1) * DT] = val.astype(bf16)
        ctx_o[:, rows_of(i * L, L)] = ctxT[...]
        grad = dot32(ctxT[...], dys[here, :], ONE)

        @pl.when(i == 0)
        def _():
            wog[...] = grad

        @pl.when(i > 0)
        def _():
            wog[...] += grad

        if X > 1:
            @pl.when(i == 1)
            def _():
                for a in (0, 1):
                    token_copy(a, 2).wait_recv()
                    token_copy(a, 3).start()

        for nxt in range(1, T):
            @pl.when(i + 1 == nxt)
            def _():
                for a in (0, 1):
                    if nxt != 2:
                        token_copy(a, nxt).wait_recv()

        @pl.when(i + 1 < T)
        def _():
            norm_one(i + 1)

        return carry

    lax.fori_loop(0, T, slot_body, 0)
    outs = [
        local(xs, xg, loc.at[0]),
        local(dys, dyg, loc.at[1]),
        local(wtb, wt_o, loc.at[3]),
        local(wob, wo_o, loc.at[4]),
        local(gt, gt_o, loc.at[7]),
        local(n2, n2_o, loc.at[12]),
    ]
    for o in outs:
        o.start()
    for g, step in late[4 * T - 2 :]:
        g.event(step)
    ones = jnp.ones((8, T * L), bf16)
    tbg_o[...] = dot32(ones, gt[...], ONE)

    m = rows // R

    @pl.loop(0, S)
    def _(p):
        grad = dot32(n1[:, pl.ds(pl.multiple_of(p * rows, rows), rows)], gt[...], TN)
        for r in range(R):
            part = grad[r * m : (r + 1) * m]
            wtl[rows_of((r * S + p) * m, m), :] = part.astype(bf16)

            @pl.when(links.rep == r)
            def _():
                wth[rows_of(p * m, m), :] = part

    mo = HEAD_DIM // R
    for p in range(S):
        for r in range(R):
            part = wog[p * HEAD_DIM + r * mo : p * HEAD_DIM + (r + 1) * mo, :]
            wol[(r * S + p) * mo : (r * S + p + 1) * mo, :] = part.astype(bf16)

            @pl.when(links.rep == r)
            def _():
                woh[p * mo : (p + 1) * mo, :] = part

    last = [
        local(wtl, wtl_o, loc.at[8]),
        local(wth, wth_o, loc.at[9]),
        local(wol, wol_o, loc.at[10]),
        local(woh, woh_o, loc.at[11]),
    ]
    for o in last:
        o.start()
    for c in own_copies_late:
        c.wait()
    g_we.arrived()
    g_ws.arrived()
    for g in chunks:
        g.drain()
    for a in (0, 1):
        for slot in range(1, T):
            token_copy(a, slot).wait_send()
    for o in outs + last:
        o.wait()


def attention_phase(R, X, S, x, dy, wt, wo, we, ws, small, tables):
    L, D = x.shape
    T = 2 * X
    DT = S * HEAD_DIM
    FT = we.shape[1] // T
    fs = FT // S
    rows = D // S
    n = T * L
    sds = jax.ShapeDtypeStruct
    dma = pltpu.SemaphoreType.DMA
    outs = [
        sds((n, D), bf16), sds((n, D), bf16), sds((D, 3 * DT), bf16), sds((DT, D), bf16),
        sds((D, FT), bf16), sds((FT, D), bf16), sds((16, max(D, FT)), f32), sds((DT, n), bf16),
        sds((n, 3 * DT), bf16), sds((D, 3 * DT), bf16), sds((D // R, 3 * DT), f32),
        sds((DT, D), bf16), sds((DT // R, D), f32), sds((8, 3 * DT), f32), sds((n, D), bf16),
    ]
    specs = [ANY] * 6 + [VM, VM] + [ANY] * 5 + [VM, ANY]
    vmem = pltpu.VMEM
    scratch = [
        vmem((n, D), bf16), vmem((n, D), bf16), vmem((n, D), bf16), vmem((n, D), bf16), vmem((n, 3 * DT), bf16),
        vmem((D, 3 * DT), bf16), vmem((DT, D), bf16), vmem((S * SMALL_ROWS, 128), f32),
        vmem((L, DT), bf16), vmem((L, DT), bf16), vmem((L, DT), bf16), vmem((L, DT), bf16),
        vmem((DT, L), bf16), vmem((DT, L), bf16), vmem((DT, L), bf16), vmem((DT, L), f32),
        vmem((L, DT), f32), vmem((L, DT), f32), vmem((D, 3 * DT), bf16), vmem((D // R, 3 * DT), f32),
        vmem((DT, D), bf16), vmem((DT // R, D), f32), vmem((DT, D), f32),
        vmem((3 * L, 128), f32), vmem((L // 2, 128), f32),
        vmem((rows, 3 * S * 128), f32), vmem((HEAD_DIM, D), f32), vmem((rows, FT), f32), vmem((fs, D), f32),
        vmem((rows, 3 * DT), bf16), vmem((HEAD_DIM, D), bf16), vmem((rows, FT), bf16), vmem((fs, D), bf16),
        dma((5, S, 2)), dma((5, S)), dma((5, S, R)), dma((5, S, R)), dma((2, 4)), dma((2, 4)), dma((13,)), dma((4 * S + 5,)),
    ]
    body = lambda *refs: attention_kernel(R, X, S, L, D, FT, *refs)
    return pl.pallas_call(
        body,
        name="attention_phase",
        out_shape=outs,
        in_specs=[ANY] * 8,
        out_specs=specs,
        scratch_shapes=scratch,
        compiler_params=pltpu.CompilerParams(
            collective_id=1, has_side_effects=True, vmem_limit_bytes=60 * 1024 * 1024
        ),
    )(x, dy, wt, wo, we, ws, small, tables)


class GradSum:
    def __init__(self, links, blocks, m, bufs, sems, piece, only=None):
        self.k, self.B, self.m = links, blocks, m
        self.lo, self.keep, self.yr, self.zs, self.zr, self.fin = bufs
        self.sems, self.piece, self.only = sems, piece, only

    def across(self, f, dr):
        size = self.B * self.m
        r = lax.rem(self.k.rep + dr, self.k.R)
        return remote(
            self.lo.at[rows_of((f * self.k.R + r) * size, size)],
            self.yr.at[rows_of((f * (self.k.R - 1) + dr - 1) * size, size)],
            self.sems["ys"].at[f, dr], self.sems["yr"].at[f, dr], self.k.at_rep(dr),
        )

    def send_across(self, f):
        for dr in range(1, self.k.R):
            self.across(f, dr).start()

    def toward(self, f, p):
        b = 0 if self.only else p
        to = self.zr.at[rows_of(((0 if self.only else f) * self.k.S + self.k.z) * self.m, self.m)]
        return remote(
            self.zs.at[rows_of((f * self.B + b) * self.m, self.m)], to,
            self.sems["zs"].at[f, p], self.sems["zr"].at[f, self.k.z], self.k.at_z(p),
        )

    def owners(self, f, fn):
        if self.only:
            @pl.when(f != self.k.z)
            def _():
                fn(f)
        else:
            for dp in range(1, self.k.S):
                fn(lax.rem(self.k.z + dp, self.k.S))

    def if_owner(self, f, fn):
        if self.only:
            pl.when(f == self.k.z)(fn)
        else:
            fn()

    def sum_across(self, f):
        R, m = self.k.R, self.m
        for dr in range(1, R):
            self.across(f, dr).wait_recv()

        for b in range(self.B):
            at = rows_of((f * self.B + b) * m, m)
            total = self.keep[at, :]
            for dr in range(1, R):
                got = rows_of(((f * (R - 1) + dr - 1) * self.B + b) * m, m)
                total = total + self.yr[got, :].astype(f32)
            self.keep[at, :] = total
            self.zs[at, :] = total.astype(bf16)

        self.owners(f, lambda p: self.toward(f, p).start())

    def total(self, f):
        S, m = self.k.S, self.m

        def go():
            g = 0 if self.only else f
            at = rows_of((f * self.B + (0 if self.only else self.k.z)) * m, m)
            total = self.keep[at, :]
            for dp in range(1, S):
                p = lax.rem(self.k.z + dp, S)
                src = self.zr.at[rows_of((g * S + p) * m, m)]
                remote(src, src, self.sems["zs"].at[f, p], self.sems["zr"].at[f, p], self.k.at_z(p)).wait_recv()
                total = total + self.zr[rows_of((g * S + p) * m, m), :].astype(f32)
            fin = rows_of(g * m, m)
            self.fin[fin, :] = total.astype(bf16)
            src = self.fin.at[fin]
            local(src, self.piece(f, self.k.tx, self.k.core, self.k.rep), self.sems["gl"].at[f]).start()
            for c in self.spread(f, src, self.k.tx, self.k.rep, 0):
                c.start()

        self.if_owner(f, go)

    def spread(self, f, src, tx, r, stage):
        dst = self.piece(f, tx, self.k.core, r)
        src = dst if src is None else src
        out = []
        other = 1 if stage == 2 else 0
        out.append(
            remote(src, dst, self.sems["gcs"].at[f, other, r], self.sems["gcr"].at[f, other, r], self.k.at_core())
        )
        if stage < 2 and self.k.X > 1:
            out.append(remote(src, dst, self.sems["gxs"].at[f, r], self.sems["gxr"].at[f, r], self.k.at_tx()))
        if stage == 0:
            for dr in range(1, self.k.R):
                out.append(remote(src, dst, self.sems["gys"].at[f, dr], self.sems["gyr"].at[f, r], self.k.at_rep(dr)))
        return out

    def replicas(self, fn):
        for dr in range(1, self.k.R):
            fn(dr, lax.rem(self.k.rep + dr, self.k.R))

    def forward_rep(self, f):
        def go():
            def one(dr, r):
                b = self.piece(f, self.k.tx, self.k.core, r)
                remote(b, b, self.sems["gys"].at[f, dr], self.sems["gyr"].at[f, r], self.k.at_rep(dr)).wait_recv()
                for c in self.spread(f, None, self.k.tx, r, 1):
                    c.start()

            self.replicas(one)

        self.if_owner(f, go)

    def forward_tx(self, f):
        if self.k.X == 1:
            return

        def go():
            for r in range(self.k.R):
                b = self.piece(f, 1 - self.k.tx, self.k.core, r)
                remote(b, b, self.sems["gxs"].at[f, r], self.sems["gxr"].at[f, r], self.k.at_tx()).wait_recv()
                for c in self.spread(f, None, 1 - self.k.tx, r, 2):
                    c.start()

        self.if_owner(f, go)

    def finish(self, f):
        for dr in range(1, self.k.R):
            self.across(f, dr).wait_send()
        self.owners(f, lambda p: self.toward(f, p).wait_send())

        def go():
            src = self.fin.at[rows_of((0 if self.only else f) * self.m, self.m)]
            local(src, self.piece(f, self.k.tx, self.k.core, self.k.rep), self.sems["gl"].at[f]).wait()
            for c in self.spread(f, src, self.k.tx, self.k.rep, 0):
                c.wait_send()
            self.replicas(lambda dr, r: [c.wait_send() for c in self.spread(f, None, self.k.tx, r, 1)])
            for other in range(self.k.X):
                tx = self.k.tx if other == 0 else 1 - self.k.tx
                for r in range(self.k.R):
                    if other == 1:
                        for c in self.spread(f, None, tx, r, 2):
                            c.wait_send()
                    b = self.piece(f, tx, 1 - self.k.core, r)
                    remote(
                        b, b, self.sems["gcs"].at[f, other, r], self.sems["gcr"].at[f, other, r], self.k.at_core()
                    ).wait_recv()

        self.if_owner(f, go)


SEM_NAMES = ("ys", "yr", "zs", "zr", "gl", "gcs", "gcr", "gxs", "gxr", "gys", "gyr")


def grad_sems(count, R, X, S):
    dma = pltpu.SemaphoreType.DMA
    return [
        dma((count, R)), dma((count, R)), dma((count, S)), dma((count, S)), dma((count,)),
        dma((count, 2, R)), dma((count, 2, R)), dma((count, R)), dma((count, R)), dma((count, R)), dma((count, R)),
    ]


def feed_kernel(R, X, S, L, D, FT, *refs):
    (xg, dyg, wt_f, wo_f, we_f, ws_f, vec, ctx_i, gt_i, wtl, wth, wol, woh, tbg, n2_i) = refs[:15]
    (out_o, ing_o, g_wt, g_wo, g_we, g_ws, v_o) = refs[15:22]
    rest = list(refs[22:])
    take = lambda count: [rest.pop(0) for _ in range(count)]
    (xb, dyb, n2b, actb, ghb, web, wsb, wob, ctb) = take(9)
    wt_bufs, wt2_bufs, wo_bufs, we_bufs, ws_bufs = take(5), take(5), take(5), take(6), take(6)
    (send_b, out_r, dx_r, xs_b, out_x, dx_x, vsum, vrecv) = take(8)
    sem_sets = [dict(zip(SEM_NAMES, take(len(SEM_NAMES)))) for _ in range(5)]
    (loc, tok, v_s, v_r, dxk) = take(5)
    T = 2 * X
    n = T * L
    rows = D // S
    DT = S * HEAD_DIM
    fs = FT // S
    k = Links(R, X, S)
    k.barrier(every_plane=True)
    rank = lambda tx, core: tx * 2 + core
    mt, mo, me, ms = rows // R, HEAD_DIM // R, rows // R, fs // R
    wide = 3 * DT // 2

    def triple_half(c, bufs, sems):
        cols = pl.ds(c * wide, wide)
        return GradSum(k, S, mt, [wtl.at[:, cols]] + bufs, sems,
                       lambda f, tx, core, r: g_wt.at[rows_of(rank(tx, core) * rows + r * mt, mt), cols])

    u_wt, u_wt2 = triple_half(0, wt_bufs, sem_sets[0]), triple_half(1, wt2_bufs, sem_sets[4])
    u_wo = GradSum(k, S, mo, [wol] + wo_bufs, sem_sets[1],
                   lambda f, tx, c, r: g_wo.at[rows_of(rank(tx, c) * HEAD_DIM + r * mo, mo)])
    u_we = GradSum(k, S, me, we_bufs, sem_sets[2],
                   lambda f, tx, c, r: g_we.at[rows_of(r * me, me), rows_of((f * T + rank(tx, c)) * fs, fs)])
    u_ws = GradSum(k, 1, ms, ws_bufs, sem_sets[3],
                   lambda f, tx, c, r: g_ws.at[rows_of(rank(tx, c) * fs + r * ms, ms)], only=True)
    first = (u_wo, u_wt, u_wt2)
    for u in first:
        u.send_across(0)

    def load_x(i, place):
        return local(xg.at[rows_of(i * L, L)], xb.at[pl.ds(place * L, L)], loc.at[place])

    load_x(1, 0).start()
    loads = [
        local(we_f, web, loc.at[2]), local(n2_i, n2b, loc.at[1 + 12]), local(dyg, dyb, loc.at[3]), local(ws_f, wsb, loc.at[4]),
        local(wo_f, wob, loc.at[5]), local(ctx_i, ctb, loc.at[6]),
        local(woh, wo_bufs[0], loc.at[8]),
        local(wth.at[:, pl.ds(0, wide)], wt_bufs[0], loc.at[7]),
        local(wth.at[:, pl.ds(wide, wide)], wt2_bufs[0], loc.at[14]),
    ]
    for c in loads:
        c.start()

    gain1, gain2 = vec[0:1, 0:D], vec[2:3, 0:D]
    for c in loads[:4]:
        c.wait()
    for c in loads[6:9]:
        c.wait()
    early = {T * S // 4: u_wo, T * S // 2: u_wt, T * S - 1: u_wt2}

    def hidden_body(it, carry):
        i, f = it // S, lax.rem(it, S)
        here, cols = rows_of(i * L, L), pl.ds(pl.multiple_of(f * fs, fs), fs)
        h = dot32(n2b[here, :], web[:, cols], ONE) + vec[8:9, cols]
        cdf = 0.5 * (1.0 + lax.erf(h * math.sqrt(0.5)))
        actb[here, cols] = (h * cdf).astype(bf16)
        slope = cdf + h * (jnp.exp(-0.5 * h * h) * (1.0 / math.sqrt(2.0 * math.pi)))
        ghb[here, cols] = (dot32(dyb[here, :], wsb[cols, :], NT) * slope).astype(bf16)
        for turn, u in early.items():
            @pl.when(it == turn)
            def _():
                u.sum_across(0)
        return carry

    lax.fori_loop(0, T * S, hidden_body, 0)
    loads[4].wait()
    loads[5].wait()
    half = L // 2

    def feed_rows(i, b):
        at = i * L + b * half
        return dot32(actb[at : at + half, :], wsb[...], ONE) + dot32(ctb[:, at : at + half], wob[...], TN)

    def to_core(which, j):
        land = (out_r, dx_r)[which]
        return remote(
            send_b.at[pl.ds(j * L, L)], land.at[pl.ds(j * L, L)],
            tok.at[which, 0, j], tok.at[which, 1, j], k.at_core(),
        )

    def to_tx(which):
        return remote(
            xs_b.at[pl.ds(which * L, L)], (out_x, dx_x)[which], tok.at[which, 2, 0], tok.at[which, 2, 1], k.at_tx()
        )

    for j in range(X):
        for b in range(2):
            at = j * L + b * half
            send_b[at : at + half, :] = feed_rows(2 * j + 1, b).astype(bf16)
        to_core(0, j).start()
    if X > 1:
        to_core(0, 1).wait_recv()
        for b in range(2):
            got = out_r[L + b * half : L + (b + 1) * half, :].astype(f32)
            xs_b[b * half : (b + 1) * half, :] = (feed_rows(2, b) + got).astype(bf16)
        to_tx(0).start()

    side = D // DT

    def triple_back(at):
        total = None
        for j in range(0, 3, side):
            wide = min(side, 3 - j)
            part = dot32(
                actb[at, j * DT : (j + wide) * DT], wsb[(j // side) * D : (j // side + 1) * D, 0 : wide * DT], NT
            )
            total = part if total is None else total + part
        return total

    def store_grad(u, f, block, grad):
        for r in range(R):
            part = grad[r * u.m : (r + 1) * u.m]
            u.lo[rows_of(((f * R + r) * u.B + block) * u.m, u.m), :] = part.astype(bf16)

            @pl.when(k.rep == r)
            def _():
                u.keep[rows_of((f * u.B + block) * u.m, u.m), :] = part

    def chunk_body(f, carry):
        cols = pl.ds(pl.multiple_of(f * fs, fs), fs)
        store_grad(u_ws, f, 0, dot32(actb[:, cols], dyb[...], TN))
        u_ws.send_across(f)

        def block_body(p, c2):
            grad = dot32(n2b[:, pl.ds(pl.multiple_of(p * rows, rows), rows)], ghb[:, cols], TN)
            store_grad(u_we, f, p, grad)
            return c2

        lax.fori_loop(0, S, block_body, 0)
        u_we.send_across(f)
        return carry

    lax.fori_loop(0, S, chunk_body, 0)
    for b in range(2):
        dxk[b * half : (b + 1) * half, :] = feed_rows(0, b)

    thirds = [wsb.at[pl.ds((j // side) * D, D), pl.ds((j % side) * DT, DT)] for j in range(3)]
    load_wt = [local(wt_f.at[:, pl.ds(j * DT, DT)], thirds[j], loc.at[(9, 11, 12)[j]]) for j in range(3)]
    for c in load_wt:
        c.start()

    gtb = actb.at[:, pl.ds(0, 3 * DT)]
    load_gt = local(gt_i, gtb, loc.at[10])
    load_gt.start()
    for j in range(X):
        to_core(0, j).wait_send()
    load_gt.wait()
    for c in load_wt:
        c.wait()

    def pair(step, f):
        for u in (u_we, u_ws):
            getattr(u, step)(f)

    vsum[...] = jnp.zeros_like(vsum)
    for u in first:
        u.total(0)
    pair("sum_across", 0)

    def slot_grad(i, place, finish):
        for b in range(2):
            at = pl.ds(i * L + b * half, half)
            xhat = layer_norm_rows(xb[place * L + b * half : place * L + (b + 1) * half, :])
            g1 = triple_back(at)
            vsum[0:1, 0:D] += jnp.sum(g1 * xhat, 0, keepdims=True)
            vsum[1:2, 0:D] += jnp.sum(g1, 0, keepdims=True)
            g2 = dot32(ghb[at, :], web[...], NT)
            vsum[2:3, 0:D] += jnp.sum(g2 * xhat, 0, keepdims=True)
            vsum[3:4, 0:D] += jnp.sum(g2, 0, keepdims=True)
            finish(b, g1 * gain1 + g2 * gain2, xhat)

    order = [2 * j + 1 for j in range(X)] + ([2] if X > 1 else []) + [0]
    events = [("sum_across", f) for f in range(S)]
    for turn, i in enumerate(order):
        place = turn % 2
        load_x(i, place).wait()
        if turn + 1 < T:
            load_x(order[turn + 1], 1 - place).start()
        if i % 2 == 1:
            j = i // 2

            def finish(b, val, xhat):
                at = j * L + b * half
                send_b[at : at + half, :] = val.astype(bf16)

            slot_grad(i, place, finish)
            to_core(1, j).start()
            if turn == 0:
                for u in first:
                    u.forward_rep(0)
            else:
                pair("sum_across", 1)
                pair("total", 0)
                for u in first:
                    u.forward_tx(0)
        elif i == 2:
            to_core(1, 1).wait_recv()

            def finish(b, val, xhat):
                got = dx_r[L + b * half : L + (b + 1) * half, :].astype(f32)
                xs_b[L + b * half : L + (b + 1) * half, :] = (val + got).astype(bf16)

            slot_grad(2, place, finish)
            to_tx(1).start()
            pair("sum_across", 2)
            pair("total", 1)
            pair("forward_rep", 0)
        else:
            to_core(0, 0).wait_recv()
            to_core(1, 0).wait_recv()
            if X > 1:
                to_tx(0).wait_recv()
            for j in range(X):
                to_core(1, j).wait_send()
            for b in range(2):
                rows_b = slice(b * half, (b + 1) * half)
                total = dxk[rows_b, :] + out_r[rows_b, :].astype(f32)
                if X > 1:
                    total = total + out_x[rows_b, :].astype(f32)
                total = total + xb[place * L + b * half : place * L + (b + 1) * half, :].astype(f32)
                send_b[rows_b, :] = (total + (vec[4:5, 0:D] + vec[5:6, 0:D])).astype(bf16)
            save_out = local(send_b.at[pl.ds(0, L)], out_o, loc.at[2])
            save_out.start()

            def finish(b, val, xhat):
                rows_b = slice(b * half, (b + 1) * half)
                dxk[rows_b, :] = val + dx_r[rows_b, :].astype(f32)

            slot_grad(0, place, finish)
            place0 = place
    ones = jnp.ones((8, L), bf16)
    vsum[4:5, 0:D] = dot32(ones, dyb[0:L, :], ONE)[0:1]
    mine = rank(k.tx, k.core)
    eb = dot32(jnp.ones((8, n), bf16), ghb[...], ONE)[0:1]
    for t in range(T):
        @pl.when(mine == t)
        def _():
            vsum[5 + t : 6 + t, 0 : 3 * DT] = tbg[0:1, :]
            vsum[5 + T + t : 6 + T + t, 0:FT] = eb

    def exchange(stage, copies):
        for c in copies:
            c.start()
        for c in copies:
            c.wait()
        for q in range(len(copies)):
            vsum[...] += vrecv[stage + q]

    at_stage = 0
    exchange(0, [remote(vsum, vrecv.at[0], v_s.at[0], v_r.at[0], k.at_core())])
    at_stage = 1
    if X > 1:
        exchange(1, [remote(vsum, vrecv.at[1], v_s.at[1], v_r.at[1], k.at_tx())])
        at_stage = 2
    rep_copies = [
        remote(vsum, vrecv.at[at_stage + dr - 1], v_s.at[at_stage + dr - 1], v_r.at[at_stage + dr - 1], k.at_rep(dr))
        for dr in range(1, R)
    ]
    exchange(at_stage, rep_copies)
    at_stage += R - 1
    z_copies = [
        remote(
            vsum, vrecv.at[at_stage + dz - 1], v_s.at[at_stage + dz - 1], v_r.at[at_stage + dz - 1],
            k.at_z(lax.rem(k.z + dz, S)),
        )
        for dz in range(1, S)
    ]
    for c in z_copies:
        c.start()
    if X == 1:
        for u in first:
            u.forward_tx(0)
        pair("sum_across", 1)
        pair("sum_across", 2)
        pair("total", 0)
        pair("total", 1)
        pair("forward_rep", 0)
    for f in range(3, S):
        pair("sum_across", f)
        pair("total", f - 1)
        pair("forward_rep", f - 2)
        pair("forward_tx", f - 3)
    for c in z_copies:
        c.wait()
    total = vsum[...]
    for q in range(S - 1):
        total = total + vrecv[at_stage + q]
    v_o[...] = total
    if X > 1:
        to_tx(1).wait_recv()
    for b in range(2):
        rows_b = slice(b * half, (b + 1) * half)
        dx = dxk[rows_b, :]
        if X > 1:
            dx = dx + dx_x[rows_b, :].astype(f32)
        xf = xb[place0 * L + b * half : place0 * L + (b + 1) * half, :].astype(f32)
        cen = xf - jnp.mean(xf, -1, keepdims=True)
        rstd = lax.rsqrt(jnp.mean(cen * cen, -1, keepdims=True) + eps_norm)
        xhat = cen * rstd
        back = dx - jnp.mean(dx, -1, keepdims=True) - xhat * jnp.mean(dx * xhat, -1, keepdims=True)
        send_b[L + b * half : L + (b + 1) * half, :] = (dyb[rows_b, :].astype(f32) + rstd * back).astype(bf16)
    save_ing = local(send_b.at[pl.ds(L, L)], ing_o, loc.at[3])
    save_ing.start()
    pair("total", S - 1)
    pair("forward_rep", S - 2)
    pair("forward_tx", S - 3)
    pair("forward_rep", S - 1)
    pair("forward_tx", S - 2)
    pair("forward_tx", S - 1)
    for u in first:
        u.finish(0)
    for f in range(S):
        pair("finish", f)
    if X > 1:
        to_tx(0).wait_send()
        to_tx(1).wait_send()
    save_out.wait()
    save_ing.wait()


def feed_phase(R, X, S, F, xg, dyg, wt_f, wo_f, we_f, ws_f, vecs, ctxT, gt, wtl, wth, wol, woh, tbg, n2):
    T = 2 * X
    n, D = xg.shape
    L = n // T
    DT = S * HEAD_DIM
    FT = we_f.shape[1]
    fs = FT // S
    rows = D // S
    mt, mo, me, ms = rows // R, HEAD_DIM // R, rows // R, fs // R
    W = max(D, 3 * DT, FT)
    sds = jax.ShapeDtypeStruct
    vmem = pltpu.VMEM
    dma = pltpu.SemaphoreType.DMA
    outs = [
        sds((L, D), bf16), sds((L, D), bf16), sds((T * rows, 3 * DT), bf16), sds((rows, D), bf16),
        sds((rows, F), bf16), sds((F // S, D), bf16), sds((16, W), f32),
    ]

    def bufs(count, B, m, cols, lo, landing):
        made = [vmem((count * R * B * m, cols), bf16)] if lo else []
        return made + [
            vmem((count * B * m, cols), f32), vmem((count * (R - 1) * B * m, cols), bf16),
            vmem((count * B * m, cols), bf16), vmem((landing * S * m, cols), bf16), vmem((landing * m, cols), bf16),
        ]

    scratch = [
        vmem((2 * L, D), bf16), vmem((n, D), bf16), vmem((n, D), bf16), vmem((n, FT), bf16), vmem((n, FT), bf16),
        vmem((D, FT), bf16), vmem((FT, D), bf16), vmem((DT, D), bf16),
        vmem((DT, n), bf16),
    ]
    scratch += bufs(1, S, mt, 3 * DT // 2, False, 1) * 2 + bufs(1, S, mo, D, False, 1)
    scratch += bufs(S, S, me, fs, True, S) + bufs(S, 1, ms, D, True, 1)
    scratch += [
        vmem((2 * L, D), bf16), vmem((X * L, D), bf16), vmem((X * L, D), bf16), vmem((2 * L, D), bf16),
        vmem((L, D), bf16), vmem((L, D), bf16), vmem((16, W), f32), vmem((2 + R - 1 + S - 1, 16, W), f32),
    ]
    for count in (1, 1, S, S, 1):
        scratch += grad_sems(count, R, X, S)
    scratch += [dma((15,)), dma((2, 3, 2)), dma((2 + R - 1 + S - 1,)), dma((2 + R - 1 + S - 1,)), vmem((L, D), f32)]
    body = lambda *refs: feed_kernel(R, X, S, L, D, FT, *refs)
    return pl.pallas_call(
        body,
        name="feed_phase",
        out_shape=outs,
        in_specs=[ANY] * 6 + [VM] + [ANY] * 6 + [VM, ANY],
        out_specs=[ANY] * 6 + [VM],
        scratch_shapes=scratch,
        compiler_params=pltpu.CompilerParams(
            collective_id=2, has_side_effects=True, vmem_limit_bytes=67_000_000
        ),
    )(xg, dyg, wt_f, wo_f, we_f, ws_f, vecs, ctxT, gt, wtl, wth, wol, woh, tbg, n2)


def adam_kernel(S, T, heads, *refs):
    g_ref, w_ref, m_ref, v_ref, g_o, w_o, m_o, v_o = refs

    def one(at, g):
        new_w, _, new_m, new_v = adam_step(w_ref[:, at], g, m_ref[:, at], v_ref[:, at], True)
        g_o[:, at] = g
        w_o[:, at] = new_w
        m_o[:, at] = new_m
        v_o[:, at] = new_v

    if not heads:
        one(slice(None), g_ref[...].astype(f32))
        return
    lane = lax.broadcasted_iota(jnp.int32, (1, 128), 1)
    DT = S * HEAD_DIM
    for j in range(3):
        for p in range(S):
            src = j * DT + (p // 2) * 128
            for u in range(T // 2):
                low = g_ref[2 * u, :, src : src + 128].astype(f32)
                high = g_ref[2 * u + 1, :, src : src + 128].astype(f32)
                if p % 2 == 1:
                    low = pltpu.roll(low, HEAD_DIM, 1)
                else:
                    high = pltpu.roll(high, HEAD_DIM, 1)
                to = ((j * S + p) * T + 2 * u) * HEAD_DIM
                one(slice(to, to + 128), jnp.where(lane < HEAD_DIM, low, high))


def adam_matrix(S, T, g, w, m, v, heads, rows_each):
    n, cols = w.shape
    spec = pl.BlockSpec((rows_each, cols), lambda i: (i, 0))
    g_spec = pl.BlockSpec((T, rows_each, g.shape[-1]), lambda i: (0, i, 0)) if heads else spec
    return pl.pallas_call(
        lambda *refs: adam_kernel(S, T, heads, *refs),
        name="adam_matrix",
        grid=(n // rows_each,),
        out_shape=[jax.ShapeDtypeStruct((n, cols), f32)] * 4,
        in_specs=[g_spec, spec, spec, spec],
        out_specs=[spec] * 4,
        compiler_params=pltpu.CompilerParams(vmem_limit_bytes=40 * 1024 * 1024),
    )(g, w, m, v)


TP = ("tx", "core")


def make_step(R, X, S):
    T = 2 * X

    def step(*args):
        x, dy = args[0], args[1]
        masters, momenta, variances = args[2:14], args[14:26], args[26:38]
        L, D = x.shape
        H = D // HEAD_DIM
        t = lax.axis_index(TP)
        z = lax.axis_index("shard")
        rep = lax.axis_index("rep")
        wt, wo, we, ws = masters[4], masters[6], masters[8], masters[10]
        rows = wt.shape[0]
        F = we.shape[1]
        fs = F // S // T
        HT = H // T

        eb_own = lax.dynamic_slice_in_dim(masters[9], t * fs, fs, 0)
        packed = [masters[i] for i in (0, 1, 2, 3, 7, 11)] + [eb_own, masters[5]]
        wide, at, flat = SMALL_ROWS * 128, 0, 0.0
        for v in packed:
            flat = flat + lax.pad(v, jnp.float32(0), [(at, wide - at - v.shape[0], 0)])
            at += v.shape[0]
        small = lax.reduce_precision(flat, 8, 7).reshape(SMALL_ROWS, 128)

        passed = attention_phase(R, X, S, x, dy, wt, wo, we, ws, small, jnp.asarray(rotary_tables(L)))
        out, in_grad, wt_s, wo_s, we_s, ws_s, vec = feed_phase(R, X, S, F, *passed)
        wt_s = wt_s.reshape(T, rows, -1)
        DT, FT = S * HEAD_DIM, F // T
        tb_g = vec[5 : 5 + T, : 3 * DT].reshape(T, 3, S, HEAD_DIM).transpose(1, 2, 0, 3).reshape(-1)
        eb_g = vec[5 + T : 5 + 2 * T, :FT].reshape(T, S, fs).transpose(1, 0, 2).reshape(-1)

        def own(v):
            return lax.dynamic_slice_in_dim(v, z * (v.shape[0] // S), v.shape[0] // S, 0)

        vown = [own(vec[i, :D]) for i in range(5)] + [own(tb_g), own(eb_g)]
        done = {}
        for i, g, each in ((4, wt_s, 64), (6, wo_s, 128), (8, we_s, 64), (10, ws_s, 256)):
            each = min(each, g.shape[-2])
            done[i] = adam_matrix(S, T, g, masters[i], momenta[i], variances[i], i == 4, each)
        summed = [
            vown[0], vown[1], vown[2], vown[3], None, vown[5], None, vown[4], None, vown[6], None, vown[4],
        ]
        updated, ones, twos = [], [], []
        for i in range(12):
            if i in done:
                summed[i] = done[i][0]
                for kept, val in zip((updated, ones, twos), done[i][1:]):
                    kept.append(val)
                continue
            new_weight, delta, m_new, v_new = adam_step(
                masters[i], summed[i], momenta[i], variances[i], i in (4, 6, 8, 10)
            )
            updated.append(delta if i in (0, 2) else new_weight)
            ones.append(m_new)
            twos.append(v_new)
        return (out, in_grad, *summed, *updated, *ones, *twos)

    return step


def solution(mesh):
    G, S = mesh.shape["grp"], mesh.shape["shard"]
    X = 2 if S <= 4 else 1
    R = G // (2 * X)
    full = Mesh(mesh.devices.reshape(R, X, 2, S), ("rep", "tx", "core", "shard"))
    tok = P(("rep", "tx", "core", "shard"), None)
    vecs, mats = P("shard"), P("shard", None)
    group = tuple(mats if i in (4, 6, 8, 10) else vecs for i in range(12))
    return jax.shard_map(
        make_step(R, X, S),
        mesh=full,
        in_specs=(tok, tok) + group * 3,
        out_specs=(tok, tok) + group * 4,
        check_vma=False,
    )
```

```python
import math

import jax
import jax.numpy as jnp
import numpy as np
from jax import lax
from jax.experimental import pallas as pl
from jax.experimental.pallas import tpu as pltpu
from jax.sharding import Mesh, PartitionSpec as P

HEAD_DIM = 64
ROTARY = 16
STEP = 10
eps_norm = 1e-05
rope_base = 10000.0
beta_one = 0.9
beta_two = 0.95
learn_rate = 0.01
adam_eps = 1e-08
weight_decay = 0.01

bf16 = jnp.bfloat16
f32 = jnp.float32


def adam_step(weight, gradient, momentum, variance, decayed):
    momentum_new = beta_one * momentum + (1.0 - beta_one) * gradient
    variance_new = beta_two * variance + (1.0 - beta_two) * gradient * gradient
    mean_hat = momentum_new / (1.0 - beta_one**STEP)
    var_hat = variance_new / (1.0 - beta_two**STEP)
    change = mean_hat / (jnp.sqrt(var_hat) + adam_eps)
    if decayed:
        change = change + weight_decay * weight
    delta = -learn_rate * change
    return (weight + delta, delta, momentum_new, variance_new)


def rotary_tables(length):
    position = np.arange(length, dtype=np.float32)[:, None]
    half = ROTARY // 2
    inverse_freq = np.float32(rope_base) ** (-(np.arange(half, dtype=np.float32) * np.float32(2.0) / np.float32(ROTARY)))
    angles = position * inverse_freq[None, :].astype(np.float32)
    cosine, sine = np.cos(angles), np.sin(angles)
    rest = np.zeros((length, HEAD_DIM - 2 * ROTARY), np.float32)
    head = np.concatenate([cosine, cosine, -sine, sine, rest], 1)
    return np.concatenate([head[: length // 2], head[length // 2 :]], 1).astype(np.float32)


def dot32(a, b, dims):
    return lax.dot_general(a, b, (dims, ((), ())), preferred_element_type=f32)


MESH = pl.DeviceIdType.MESH
ANY = pl.BlockSpec(memory_space=pl.ANY)
VM = pl.BlockSpec(memory_space=pltpu.VMEM)
ONE = ((1,), (0,))
NT = ((1,), (1,))
TN = ((0,), (0,))


def rows_of(start, size):
    return pl.ds(pl.multiple_of(start, math.gcd(size, 512)), size)


class Links:
    def __init__(self, R, X, S):
        self.R, self.X, self.S = R, X, S
        self.rep = lax.axis_index("rep")
        self.tx = lax.axis_index("tx")
        self.core = lax.axis_index("core")
        self.z = lax.axis_index("shard")

    def at_core(self):
        return {"core": 1 - self.core}

    def at_tx(self):
        return {"tx": 1 - self.tx}

    def at_rep(self, dr):
        return {"rep": lax.rem(self.rep + dr, self.R)}

    def at_z(self, z):
        return {"shard": z}

    def barrier(self, every_plane=False):
        sem = pltpu.get_barrier_semaphore()

        def tell(where):
            pl.semaphore_signal(sem, inc=1, device_id=where, device_id_type=MESH)

        count = 1 + (self.X - 1) + (self.R - 1)
        tell(self.at_core())
        if self.X > 1:
            tell(self.at_tx())
        for dr in range(1, self.R):
            tell(self.at_rep(dr))

        if every_plane:
            for dz in range(1, self.S):
                tell(self.at_z(lax.rem(self.z + dz, self.S)))
            pl.semaphore_wait(sem, count + self.S - 1)
            return

        @pl.when(self.z > 0)
        def _():
            tell(self.at_z(self.z - 1))

        @pl.when(self.z < self.S - 1)
        def _():
            tell(self.at_z(self.z + 1))

        ends = (self.z > 0).astype(jnp.int32) + (self.z < self.S - 1).astype(jnp.int32)
        pl.semaphore_wait(sem, count + ends)


def remote(src, dst, send, recv, where):
    return pltpu.make_async_remote_copy(
        src_ref=src, dst_ref=dst, send_sem=send, recv_sem=recv, device_id=where, device_id_type=MESH
    )


def local(src, dst, sem):
    return pltpu.make_async_copy(src, dst, sem)


class LineGather:
    def __init__(self, links, own, buf, n, zs, zr, ys, yr, split):
        self.k = links
        self.own, self.buf, self.n = own, buf, n
        self.parts = links.R if split else 1
        self.m = n // self.parts
        self.zs, self.zr, self.ys, self.yr = zs, zr, ys, yr

    def block(self, p, r):
        return self.buf.at[rows_of(p * self.n + r * self.m, self.m)]

    def mine(self):
        return self.k.rep if self.parts > 1 else 0

    def hop(self, src, p, step, way):
        to = self.k.z + 1 if way == 0 else self.k.z - 1
        return remote(
            src, self.block(p, self.mine()), self.zs.at[step, way], self.zr.at[p], self.k.at_z(to)
        )

    def across(self, p, dr):
        b = self.block(p, self.k.rep)
        return remote(b, b, self.ys.at[p, dr], self.yr.at[p, self.k.rep], self.k.at_rep(dr))

    def each_way(self, step, fn):
        z, S = self.k.z, self.k.S
        for way in (0, 1):
            p = z - step if way == 0 else z + step
            here = (step <= z) if way == 0 else (z + step <= S - 1)
            on = (z < S - 1) if way == 0 else (z > 0)
            fn(way, p, here, on)

    def start(self):
        mine = self.mine()

        def go(way, p, here, on):
            @pl.when(on)
            def _():
                self.hop(self.own.at[rows_of(mine * self.m, self.m)], p, 0, way).start()

        self.each_way(0, go)

    def event(self, step):
        def go(way, p, here, on):
            @pl.when(here)
            def _():
                b = self.block(p, self.mine())
                self.hop(b, p, step, way).wait_recv()

                @pl.when(on)
                def _():
                    self.hop(b, p, step, way).start()

                if self.parts > 1:
                    for dr in range(1, self.k.R):
                        self.across(p, dr).start()

        self.each_way(step, go)

    def arrived(self):
        if self.parts == 1:
            return
        for p in range(self.k.S):
            @pl.when(p != self.k.z)
            def _():
                for dr in range(1, self.k.R):
                    r = lax.rem(self.k.rep + dr, self.k.R)
                    b = self.block(p, r)
                    remote(b, b, self.ys.at[p, dr], self.yr.at[p, r], self.k.at_rep(dr)).wait_recv()

    def drain(self):
        for step in range(self.k.S):
            def go(way, p, here, on):
                @pl.when(jnp.logical_and(here, on))
                def _():
                    self.hop(self.block(p, self.mine()), p, step, way).wait_send()

                if step > 0 and self.parts > 1:
                    @pl.when(here)
                    def _():
                        for dr in range(1, self.k.R):
                            self.across(p, dr).wait_send()

            self.each_way(step, go)


def layer_norm_rows(xb):
    xf = xb.astype(f32)
    cen = xf - jnp.mean(xf, -1, keepdims=True)
    return cen * lax.rsqrt(jnp.mean(cen * cen, -1, keepdims=True) + eps_norm)


SMALL_ROWS = 24


def small_row(sm, S, first, count):
    return jnp.concatenate(
        [sm[p * SMALL_ROWS + first + j : p * SMALL_ROWS + first + j + 1, :] for p in range(S) for j in range(count)],
        -1,
    )


def attention_kernel(R, X, S, L, D, FT, *refs):
    (x_ref, dy_ref, wt_m, wo_m, we_m, ws_m, sm_ref, turn_i) = refs[:8]
    (xg, dyg, wt_o, wo_o, we_o, ws_o, vec_o, ctx_o, gt_o, wtl_o, wth_o, wol_o, woh_o, tbg_o, n2_o) = refs[8:23]
    (
        xs, dys, n1, n2, gt, wtb, wob, smb, q_s, k_s, v_s, gc_s, kT, vT, ctxT, gqT, gk_a, gv_a, wtl, wth, wol, woh, wog,
        turn_s, turn_p, wt_w, wo_w, we_w, ws_w, wt_ref, wo_ref, we_ref, ws_ref,
        zs, zr, ys, yr, tok_s, tok_r, loc, cut,
    ) = refs[23:]
    T = 2 * X
    rows = D // S
    DT = S * HEAD_DIM
    links = Links(R, X, S)
    chunks = []
    for c, (own, buf) in enumerate(
        [(sm_ref, smb), (wt_ref, wtb), (wo_ref, wob), (we_ref, we_o), (ws_ref, ws_o)]
    ):
        chunks.append(
            LineGather(links, own, buf, own.shape[0], zs.at[c], zr.at[c], ys.at[c], yr.at[c], c > 0)
        )
    g_sm, g_wt, g_wo, g_we, g_ws = chunks
    lane = lax.broadcasted_iota(jnp.int32, (1, 128), 1)
    rank = links.tx * 2 + links.core
    fs = FT // S
    cuts = [[], [local(wo_m.at[rows_of(rank * HEAD_DIM, HEAD_DIM)], wo_w, cut.at[3 * S])], [],
            [local(ws_m.at[rows_of(rank * fs, fs)], ws_w, cut.at[3 * S + 1])]]
    for j in range(3):
        for p in range(S):
            block = ((j * S + p) * T + rank) // 2
            cuts[0].append(
                local(
                    wt_m.at[:, pl.ds(pl.multiple_of(block * 128, 128), 128)],
                    wt_w.at[:, pl.ds((j * S + p) * 128, 128)],
                    cut.at[j * S + p],
                )
            )
    for p in range(S):
        cuts[2].append(
            local(
                we_m.at[:, pl.ds(pl.multiple_of((p * T + rank) * fs, fs), fs)],
                we_w.at[:, pl.ds(p * fs, fs)],
                cut.at[3 * S + 2 + p],
            )
        )
    for group in cuts:
        for c in group:
            c.start()
    links.barrier()
    for c in cuts[0]:
        c.wait()

    def half_lanes(block, odd):
        val = wt_w[:, block * 128 : (block + 1) * 128]
        return jnp.where(lax.rem(rank, 2) == odd, val, pltpu.roll(val, HEAD_DIM, 1))

    for b in range(3 * S // 2):
        both = jnp.where(lane < HEAD_DIM, half_lanes(2 * b, 0), half_lanes(2 * b + 1, 1))
        wt_ref[:, b * 128 : (b + 1) * 128] = both.astype(bf16)
    cuts[1][0].wait()
    wo_ref[...] = wo_w[...].astype(bf16)

    own_copies = [
        local(x_ref, xs.at[pl.ds(0, L)], loc.at[0]),
        local(dy_ref, dys.at[pl.ds(0, L)], loc.at[1]),
    ]
    own_copies_late = []
    for c, g in enumerate(chunks):
        (own_copies if c < 3 else own_copies_late).append(local(g.own, g.buf.at[rows_of(links.z * g.n, g.n)], loc.at[2 + c]))

    def token_copy(a, slot):
        buf = (xs, dys)[a]
        src = (x_ref, dy_ref)[a]
        if slot == 1:
            return remote(src, buf.at[pl.ds(L, L)], tok_s.at[a, 1], tok_r.at[a, 1], links.at_core())
        if slot == 2:
            return remote(src, buf.at[pl.ds(2 * L, L)], tok_s.at[a, 2], tok_r.at[a, 2], links.at_tx())
        return remote(
            buf.at[pl.ds(2 * L, L)], buf.at[pl.ds(3 * L, L)], tok_s.at[a, 3], tok_r.at[a, 3], links.at_core()
        )

    g_sm.start()
    g_wt.start()
    g_wo.start()
    if X > 1:
        token_copy(0, 2).start()
        token_copy(1, 2).start()
    token_copy(0, 1).start()
    token_copy(1, 1).start()
    for c in own_copies:
        c.start()

    tables = [local(turn_i, turn_p, cut.at[4 * S + 2])]

    def table(q):
        return jnp.concatenate([turn_s[q * L : (q + 1) * L, :]] * (DT // 128), 1)

    for c in tables:
        c.start()
    for c in cuts[2] + cuts[3]:
        c.wait()
    we_ref[...] = we_w[...].astype(bf16)
    ws_ref[...] = ws_w[...].astype(bf16)
    for c in own_copies_late:
        c.start()
    own_copies[0].wait()
    own_copies[2].wait()
    for step in range(1, S):
        g_sm.event(step)
    per = rows // 128
    vec_o[...] = jnp.zeros_like(vec_o)
    sm = smb[...]
    for j in range(6):
        vec_o[j : j + 1, 0:D] = small_row(sm, S, j * per, per)
    fper = FT // S // 128
    vec_o[8 : 8 + 1, 0:FT] = small_row(sm, S, 6 * per, fper)
    def head_bias(j, p):
        block = j * (D // 128) + (T * p + rank) // 2
        at = (block // (3 * per)) * SMALL_ROWS + 6 * per + fper + lax.rem(block, 3 * per)
        row = smb[pl.ds(at, 1), :]
        return jnp.where(lax.rem(rank, 2) == p % 2, row, pltpu.roll(row, HEAD_DIM, 1))

    for j in range(3):
        for a in range(S // 2):
            both = jnp.where(lane < HEAD_DIM, head_bias(j, 2 * a), head_bias(j, 2 * a + 1))
            vec_o[9 + j : 10 + j, a * 128 : (a + 1) * 128] = both

    def norm_one(i):
        gain, shift = vec_o[0:1, 0:D], vec_o[1:2, 0:D]
        gain_b, shift_b = vec_o[2:3, 0:D], vec_o[3:4, 0:D]

        @pl.loop(0, L // 64)
        def _(b):
            at = rows_of(i * L + b * 64, 64)
            xhat = layer_norm_rows(xs[at, :])
            n1[at, :] = (xhat * gain + shift).astype(bf16)
            n2[at, :] = (xhat * gain_b + shift_b).astype(bf16)

    norm_one(0)
    g_wt.event(1)
    g_wo.event(1)
    g_we.start()
    for step in range(2, S):
        g_wt.event(step)
        g_wo.event(step)
    g_ws.start()
    own_copies[1].wait()
    own_copies[3].wait()
    own_copies[4].wait()
    for c in tables:
        c.wait()
    packed_turn = turn_p[...]
    other_turn = pltpu.roll(packed_turn, HEAD_DIM, 1)
    entry = lax.rem(lane, HEAD_DIM)
    for b in range(2):
        near, far = (packed_turn, other_turn) if b == 0 else (other_turn, packed_turn)
        full = jnp.where(lane < HEAD_DIM, near, far)
        moved = pltpu.roll(full, 128 - ROTARY, 1)
        at = b * (L // 2)
        turn_s[at : at + L // 2, :] = jnp.where(entry < ROTARY, full, 1.0)
        turn_s[L + at : L + at + L // 2, :] = jnp.where(entry < ROTARY // 2, moved, 0.0)
        upper = jnp.logical_and(entry >= ROTARY // 2, entry < ROTARY)
        turn_s[2 * L + at : 2 * L + at + L // 2, :] = jnp.where(upper, moved, 0.0)
    g_wt.arrived()
    g_wo.arrived()
    late = [(g, step) for step in range(1, S) for g in (g_we, g_ws)]

    def pump(i, turn):
        for index in range(T):
            at = 2 * (2 * index + turn) - 2
            todo = late[max(at, 0) : at + 2]
            if todo:
                @pl.when(i == index)
                def _():
                    for g, step in todo:
                        g.event(step)

    half = L // 2
    lane_head = lax.broadcasted_iota(jnp.int32, (1, DT), 1) // HEAD_DIM
    key_at = lax.broadcasted_iota(jnp.int32, (half, half), 0)
    query_at = lax.broadcasted_iota(jnp.int32, (half, half), 1)
    causal = key_at <= query_at

    def slot_body(i, carry):
        here = rows_of(i * L, L)
        for j, dst in enumerate((q_s, k_s, v_s)):
            val = dot32(n1[here, :], wtb[:, j * DT : (j + 1) * DT], ONE) + vec_o[9 + j : 10 + j, 0:DT]
            if j < 2:
                val = (
                    val * table(0)
                    + pltpu.roll(val, DT - 8, 1) * table(1)
                    + pltpu.roll(val, 8, 1) * table(2)
                )
            vb = val.astype(bf16)
            if j == 0:
                q_s[...] = vb * bf16(0.125)
            else:
                dst[...] = vb
                (kT if j == 1 else vT)[...] = vb.T
        gc_s[...] = dot32(dys[here, :], wob[...], NT).astype(bf16)
        gk_a[...] = jnp.zeros_like(gk_a)
        gv_a[...] = jnp.zeros_like(gv_a)
        pump(i, 0)

        def head_body(h, c2):
            mine = (lane_head == h).astype(f32).astype(bf16)
            hrows = rows_of(h * HEAD_DIM, HEAD_DIM)
            for b in range(2):
                qs = pl.ds(b * half, half)
                kl = (b + 1) * half
                km = k_s[0:kl, :] * mine
                sT = dot32(km, q_s[qs, :], NT)
                diag = jnp.where(causal, sT[kl - half :], -1e30)
                sT = diag if b == 0 else jnp.concatenate([sT[: kl - half], diag], 0)
                e = jnp.exp(sT - jnp.max(sT, 0, keepdims=True))
                p = e * (1.0 / jnp.sum(e, 0, keepdims=True))
                pb = p.astype(bf16)
                ctxT[hrows, qs] = dot32(vT[hrows, 0:kl], pb, ONE).astype(bf16)
                gv_a[0:kl, :] += dot32(pb, gc_s[qs, :] * mine, ONE)
                gp = dot32(v_s[0:kl, :] * mine, gc_s[qs, :], NT)
                gs = (p * (gp - jnp.sum(p * gp, 0, keepdims=True))).astype(bf16)
                gk_a[0:kl, :] += dot32(gs, q_s[qs, :] * mine, ONE)
                gqT[hrows, qs] = dot32(kT[hrows, 0:kl], gs, ONE) * 0.125
            return c2

        lax.fori_loop(0, S, head_body, 0)
        pump(i, 1)
        for j in range(3):
            if j == 2:
                val = gv_a[...]
            else:
                val = gqT[...].T if j == 0 else gk_a[...]
                val = (
                    val * table(0)
                    - pltpu.roll(val, DT - 8, 1) * table(1)
                    - pltpu.roll(val, 8, 1) * table(2)
                )
            gt[here, j * DT : (j + 1) * DT] = val.astype(bf16)
        ctx_o[:, rows_of(i * L, L)] = ctxT[...]
        grad = dot32(ctxT[...], dys[here, :], ONE)

        @pl.when(i == 0)
        def _():
            wog[...] = grad

        @pl.when(i > 0)
        def _():
            wog[...] += grad

        if X > 1:
            @pl.when(i == 1)
            def _():
                for a in (0, 1):
                    token_copy(a, 2).wait_recv()
                    token_copy(a, 3).start()

        for nxt in range(1, T):
            @pl.when(i + 1 == nxt)
            def _():
                for a in (0, 1):
                    if nxt != 2:
                        token_copy(a, nxt).wait_recv()

        @pl.when(i + 1 < T)
        def _():
            norm_one(i + 1)

        return carry

    lax.fori_loop(0, T, slot_body, 0)
    outs = [
        local(xs, xg, loc.at[0]),
        local(dys, dyg, loc.at[1]),
        local(wtb, wt_o, loc.at[3]),
        local(wob, wo_o, loc.at[4]),
        local(gt, gt_o, loc.at[7]),
        local(n2, n2_o, loc.at[12]),
    ]
    for o in outs:
        o.start()
    for g, step in late[4 * T - 2 :]:
        g.event(step)
    ones = jnp.ones((8, T * L), bf16)
    tbg_o[...] = dot32(ones, gt[...], ONE)

    m = rows // R

    @pl.loop(0, S)
    def _(p):
        grad = dot32(n1[:, pl.ds(pl.multiple_of(p * rows, rows), rows)], gt[...], TN)
        for r in range(R):
            part = grad[r * m : (r + 1) * m]
            wtl[rows_of((r * S + p) * m, m), :] = part.astype(bf16)

            @pl.when(links.rep == r)
            def _():
                wth[rows_of(p * m, m), :] = part

    mo = HEAD_DIM // R
    for p in range(S):
        for r in range(R):
            part = wog[p * HEAD_DIM + r * mo : p * HEAD_DIM + (r + 1) * mo, :]
            wol[(r * S + p) * mo : (r * S + p + 1) * mo, :] = part.astype(bf16)

            @pl.when(links.rep == r)
            def _():
                woh[p * mo : (p + 1) * mo, :] = part

    last = [
        local(wtl, wtl_o, loc.at[8]),
        local(wth, wth_o, loc.at[9]),
        local(wol, wol_o, loc.at[10]),
        local(woh, woh_o, loc.at[11]),
    ]
    for o in last:
        o.start()
    for c in own_copies_late:
        c.wait()
    g_we.arrived()
    g_ws.arrived()
    for g in chunks:
        g.drain()
    for a in (0, 1):
        for slot in range(1, T):
            token_copy(a, slot).wait_send()
    for o in outs + last:
        o.wait()


def attention_phase(R, X, S, x, dy, wt, wo, we, ws, small, tables):
    L, D = x.shape
    T = 2 * X
    DT = S * HEAD_DIM
    FT = we.shape[1] // T
    fs = FT // S
    rows = D // S
    n = T * L
    sds = jax.ShapeDtypeStruct
    dma = pltpu.SemaphoreType.DMA
    outs = [
        sds((n, D), bf16), sds((n, D), bf16), sds((D, 3 * DT), bf16), sds((DT, D), bf16),
        sds((D, FT), bf16), sds((FT, D), bf16), sds((16, max(D, FT)), f32), sds((DT, n), bf16),
        sds((n, 3 * DT), bf16), sds((D, 3 * DT), bf16), sds((D // R, 3 * DT), f32),
        sds((DT, D), bf16), sds((DT // R, D), f32), sds((8, 3 * DT), f32), sds((n, D), bf16),
    ]
    specs = [ANY] * 6 + [VM, VM] + [ANY] * 5 + [VM, ANY]
    vmem = pltpu.VMEM
    scratch = [
        vmem((n, D), bf16), vmem((n, D), bf16), vmem((n, D), bf16), vmem((n, D), bf16), vmem((n, 3 * DT), bf16),
        vmem((D, 3 * DT), bf16), vmem((DT, D), bf16), vmem((S * SMALL_ROWS, 128), f32),
        vmem((L, DT), bf16), vmem((L, DT), bf16), vmem((L, DT), bf16), vmem((L, DT), bf16),
        vmem((DT, L), bf16), vmem((DT, L), bf16), vmem((DT, L), bf16), vmem((DT, L), f32),
        vmem((L, DT), f32), vmem((L, DT), f32), vmem((D, 3 * DT), bf16), vmem((D // R, 3 * DT), f32),
        vmem((DT, D), bf16), vmem((DT // R, D), f32), vmem((DT, D), f32),
        vmem((3 * L, 128), f32), vmem((L // 2, 128), f32),
        vmem((rows, 3 * S * 128), f32), vmem((HEAD_DIM, D), f32), vmem((rows, FT), f32), vmem((fs, D), f32),
        vmem((rows, 3 * DT), bf16), vmem((HEAD_DIM, D), bf16), vmem((rows, FT), bf16), vmem((fs, D), bf16),
        dma((5, S, 2)), dma((5, S)), dma((5, S, R)), dma((5, S, R)), dma((2, 4)), dma((2, 4)), dma((13,)), dma((4 * S + 5,)),
    ]
    body = lambda *refs: attention_kernel(R, X, S, L, D, FT, *refs)
    return pl.pallas_call(
        body,
        name="attention_phase",
        out_shape=outs,
        in_specs=[ANY] * 8,
        out_specs=specs,
        scratch_shapes=scratch,
        compiler_params=pltpu.CompilerParams(
            collective_id=1, has_side_effects=True, vmem_limit_bytes=60 * 1024 * 1024
        ),
    )(x, dy, wt, wo, we, ws, small, tables)


class GradSum:
    def __init__(self, links, blocks, m, bufs, sems, piece, only=None):
        self.k, self.B, self.m = links, blocks, m
        self.lo, self.keep, self.yr, self.zs, self.zr, self.fin = bufs
        self.sems, self.piece, self.only = sems, piece, only

    def across(self, f, dr):
        size = self.B * self.m
        r = lax.rem(self.k.rep + dr, self.k.R)
        return remote(
            self.lo.at[rows_of((f * self.k.R + r) * size, size)],
            self.yr.at[rows_of((f * (self.k.R - 1) + dr - 1) * size, size)],
            self.sems["ys"].at[f, dr], self.sems["yr"].at[f, dr], self.k.at_rep(dr),
        )

    def send_across(self, f):
        for dr in range(1, self.k.R):
            self.across(f, dr).start()

    def toward(self, f, p):
        b = 0 if self.only else p
        to = self.zr.at[rows_of(((0 if self.only else f) * self.k.S + self.k.z) * self.m, self.m)]
        return remote(
            self.zs.at[rows_of((f * self.B + b) * self.m, self.m)], to,
            self.sems["zs"].at[f, p], self.sems["zr"].at[f, self.k.z], self.k.at_z(p),
        )

    def owners(self, f, fn):
        if self.only:
            @pl.when(f != self.k.z)
            def _():
                fn(f)
        else:
            for dp in range(1, self.k.S):
                fn(lax.rem(self.k.z + dp, self.k.S))

    def if_owner(self, f, fn):
        if self.only:
            pl.when(f == self.k.z)(fn)
        else:
            fn()

    def sum_across(self, f):
        R, m = self.k.R, self.m
        for dr in range(1, R):
            self.across(f, dr).wait_recv()

        for b in range(self.B):
            at = rows_of((f * self.B + b) * m, m)
            total = self.keep[at, :]
            for dr in range(1, R):
                got = rows_of(((f * (R - 1) + dr - 1) * self.B + b) * m, m)
                total = total + self.yr[got, :].astype(f32)
            self.keep[at, :] = total
            self.zs[at, :] = total.astype(bf16)

        self.owners(f, lambda p: self.toward(f, p).start())

    def total(self, f):
        S, m = self.k.S, self.m

        def go():
            g = 0 if self.only else f
            at = rows_of((f * self.B + (0 if self.only else self.k.z)) * m, m)
            total = self.keep[at, :]
            for dp in range(1, S):
                p = lax.rem(self.k.z + dp, S)
                src = self.zr.at[rows_of((g * S + p) * m, m)]
                remote(src, src, self.sems["zs"].at[f, p], self.sems["zr"].at[f, p], self.k.at_z(p)).wait_recv()
                total = total + self.zr[rows_of((g * S + p) * m, m), :].astype(f32)
            fin = rows_of(g * m, m)
            self.fin[fin, :] = total.astype(bf16)
            src = self.fin.at[fin]
            local(src, self.piece(f, self.k.tx, self.k.core, self.k.rep), self.sems["gl"].at[f]).start()
            for c in self.spread(f, src, self.k.tx, self.k.rep, 0):
                c.start()

        self.if_owner(f, go)

    def spread(self, f, src, tx, r, stage):
        dst = self.piece(f, tx, self.k.core, r)
        src = dst if src is None else src
        out = []
        other = 1 if stage == 2 else 0
        out.append(
            remote(src, dst, self.sems["gcs"].at[f, other, r], self.sems["gcr"].at[f, other, r], self.k.at_core())
        )
        if stage < 2 and self.k.X > 1:
            out.append(remote(src, dst, self.sems["gxs"].at[f, r], self.sems["gxr"].at[f, r], self.k.at_tx()))
        if stage == 0:
            for dr in range(1, self.k.R):
                out.append(remote(src, dst, self.sems["gys"].at[f, dr], self.sems["gyr"].at[f, r], self.k.at_rep(dr)))
        return out

    def replicas(self, fn):
        for dr in range(1, self.k.R):
            fn(dr, lax.rem(self.k.rep + dr, self.k.R))

    def forward_rep(self, f):
        def go():
            def one(dr, r):
                b = self.piece(f, self.k.tx, self.k.core, r)
                remote(b, b, self.sems["gys"].at[f, dr], self.sems["gyr"].at[f, r], self.k.at_rep(dr)).wait_recv()
                for c in self.spread(f, None, self.k.tx, r, 1):
                    c.start()

            self.replicas(one)

        self.if_owner(f, go)

    def forward_tx(self, f):
        if self.k.X == 1:
            return

        def go():
            for r in range(self.k.R):
                b = self.piece(f, 1 - self.k.tx, self.k.core, r)
                remote(b, b, self.sems["gxs"].at[f, r], self.sems["gxr"].at[f, r], self.k.at_tx()).wait_recv()
                for c in self.spread(f, None, 1 - self.k.tx, r, 2):
                    c.start()

        self.if_owner(f, go)

    def finish(self, f):
        for dr in range(1, self.k.R):
            self.across(f, dr).wait_send()
        self.owners(f, lambda p: self.toward(f, p).wait_send())

        def go():
            src = self.fin.at[rows_of((0 if self.only else f) * self.m, self.m)]
            local(src, self.piece(f, self.k.tx, self.k.core, self.k.rep), self.sems["gl"].at[f]).wait()
            for c in self.spread(f, src, self.k.tx, self.k.rep, 0):
                c.wait_send()
            self.replicas(lambda dr, r: [c.wait_send() for c in self.spread(f, None, self.k.tx, r, 1)])
            for other in range(self.k.X):
                tx = self.k.tx if other == 0 else 1 - self.k.tx
                for r in range(self.k.R):
                    if other == 1:
                        for c in self.spread(f, None, tx, r, 2):
                            c.wait_send()
                    b = self.piece(f, tx, 1 - self.k.core, r)
                    remote(
                        b, b, self.sems["gcs"].at[f, other, r], self.sems["gcr"].at[f, other, r], self.k.at_core()
                    ).wait_recv()

        self.if_owner(f, go)


SEM_NAMES = ("ys", "yr", "zs", "zr", "gl", "gcs", "gcr", "gxs", "gxr", "gys", "gyr")


def grad_sems(count, R, X, S):
    dma = pltpu.SemaphoreType.DMA
    return [
        dma((count, R)), dma((count, R)), dma((count, S)), dma((count, S)), dma((count,)),
        dma((count, 2, R)), dma((count, 2, R)), dma((count, R)), dma((count, R)), dma((count, R)), dma((count, R)),
    ]


def feed_kernel(R, X, S, L, D, FT, *refs):
    (xg, dyg, wt_f, wo_f, we_f, ws_f, vec, ctx_i, gt_i, wtl, wth, wol, woh, tbg, n2_i) = refs[:15]
    (out_o, ing_o, g_wt, g_wo, g_we, g_ws, v_o) = refs[15:22]
    rest = list(refs[22:])
    take = lambda count: [rest.pop(0) for _ in range(count)]
    (xb, dyb, n2b, actb, ghb, web, wsb, wob, ctb) = take(9)
    wt_bufs, wt2_bufs, wo_bufs, we_bufs, ws_bufs = take(5), take(5), take(5), take(6), take(6)
    (send_b, out_r, dx_r, xs_b, out_x, dx_x, vsum, vrecv) = take(8)
    sem_sets = [dict(zip(SEM_NAMES, take(len(SEM_NAMES)))) for _ in range(5)]
    (loc, tok, v_s, v_r, dxk) = take(5)
    T = 2 * X
    n = T * L
    rows = D // S
    DT = S * HEAD_DIM
    fs = FT // S
    k = Links(R, X, S)
    k.barrier(every_plane=True)
    rank = lambda tx, core: tx * 2 + core
    mt, mo, me, ms = rows // R, HEAD_DIM // R, rows // R, fs // R
    wide = 3 * DT // 2

    def triple_half(c, bufs, sems):
        cols = pl.ds(c * wide, wide)
        return GradSum(k, S, mt, [wtl.at[:, cols]] + bufs, sems,
                       lambda f, tx, core, r: g_wt.at[rows_of(rank(tx, core) * rows + r * mt, mt), cols])

    u_wt, u_wt2 = triple_half(0, wt_bufs, sem_sets[0]), triple_half(1, wt2_bufs, sem_sets[4])
    u_wo = GradSum(k, S, mo, [wol] + wo_bufs, sem_sets[1],
                   lambda f, tx, c, r: g_wo.at[rows_of(rank(tx, c) * HEAD_DIM + r * mo, mo)])
    u_we = GradSum(k, S, me, we_bufs, sem_sets[2],
                   lambda f, tx, c, r: g_we.at[rows_of(r * me, me), rows_of((f * T + rank(tx, c)) * fs, fs)])
    u_ws = GradSum(k, 1, ms, ws_bufs, sem_sets[3],
                   lambda f, tx, c, r: g_ws.at[rows_of(rank(tx, c) * fs + r * ms, ms)], only=True)
    first = (u_wo, u_wt, u_wt2)
    for u in first:
        u.send_across(0)

    def load_x(i, place):
        return local(xg.at[rows_of(i * L, L)], xb.at[pl.ds(place * L, L)], loc.at[place])

    load_x(1, 0).start()
    loads = [
        local(we_f, web, loc.at[2]), local(n2_i, n2b, loc.at[1 + 12]), local(dyg, dyb, loc.at[3]), local(ws_f, wsb, loc.at[4]),
        local(wo_f, wob, loc.at[5]), local(ctx_i, ctb, loc.at[6]),
        local(woh, wo_bufs[0], loc.at[8]),
        local(wth.at[:, pl.ds(0, wide)], wt_bufs[0], loc.at[7]),
        local(wth.at[:, pl.ds(wide, wide)], wt2_bufs[0], loc.at[14]),
    ]
    for c in loads:
        c.start()

    gain1, gain2 = vec[0:1, 0:D], vec[2:3, 0:D]
    for c in loads[:4]:
        c.wait()
    for c in loads[6:9]:
        c.wait()
    early = {T * S // 4: u_wo, T * S // 2: u_wt, T * S - 1: u_wt2}

    def hidden_body(it, carry):
        i, f = it // S, lax.rem(it, S)
        here, cols = rows_of(i * L, L), pl.ds(pl.multiple_of(f * fs, fs), fs)
        h = dot32(n2b[here, :], web[:, cols], ONE) + vec[8:9, cols]
        cdf = 0.5 * (1.0 + lax.erf(h * math.sqrt(0.5)))
        actb[here, cols] = (h * cdf).astype(bf16)
        slope = cdf + h * (jnp.exp(-0.5 * h * h) * (1.0 / math.sqrt(2.0 * math.pi)))
        ghb[here, cols] = (dot32(dyb[here, :], wsb[cols, :], NT) * slope).astype(bf16)
        for turn, u in early.items():
            @pl.when(it == turn)
            def _():
                u.sum_across(0)
        return carry

    lax.fori_loop(0, T * S, hidden_body, 0)
    loads[4].wait()
    loads[5].wait()
    half = L // 2

    def feed_rows(i, b):
        at = i * L + b * half
        return dot32(actb[at : at + half, :], wsb[...], ONE) + dot32(ctb[:, at : at + half], wob[...], TN)

    def to_core(which, j):
        land = (out_r, dx_r)[which]
        return remote(
            send_b.at[pl.ds(j * L, L)], land.at[pl.ds(j * L, L)],
            tok.at[which, 0, j], tok.at[which, 1, j], k.at_core(),
        )

    def to_tx(which):
        return remote(
            xs_b.at[pl.ds(which * L, L)], (out_x, dx_x)[which], tok.at[which, 2, 0], tok.at[which, 2, 1], k.at_tx()
        )

    for j in range(X):
        for b in range(2):
            at = j * L + b * half
            send_b[at : at + half, :] = feed_rows(2 * j + 1, b).astype(bf16)
        to_core(0, j).start()
    if X > 1:
        to_core(0, 1).wait_recv()
        for b in range(2):
            got = out_r[L + b * half : L + (b + 1) * half, :].astype(f32)
            xs_b[b * half : (b + 1) * half, :] = (feed_rows(2, b) + got).astype(bf16)
        to_tx(0).start()

    side = D // DT

    def triple_back(at):
        total = None
        for j in range(0, 3, side):
            wide = min(side, 3 - j)
            part = dot32(
                actb[at, j * DT : (j + wide) * DT], wsb[(j // side) * D : (j // side + 1) * D, 0 : wide * DT], NT
            )
            total = part if total is None else total + part
        return total

    def store_grad(u, f, block, grad):
        for r in range(R):
            part = grad[r * u.m : (r + 1) * u.m]
            u.lo[rows_of(((f * R + r) * u.B + block) * u.m, u.m), :] = part.astype(bf16)

            @pl.when(k.rep == r)
            def _():
                u.keep[rows_of((f * u.B + block) * u.m, u.m), :] = part

    def chunk_body(f, carry):
        cols = pl.ds(pl.multiple_of(f * fs, fs), fs)
        store_grad(u_ws, f, 0, dot32(actb[:, cols], dyb[...], TN))
        u_ws.send_across(f)

        def block_body(p, c2):
            grad = dot32(n2b[:, pl.ds(pl.multiple_of(p * rows, rows), rows)], ghb[:, cols], TN)
            store_grad(u_we, f, p, grad)
            return c2

        lax.fori_loop(0, S, block_body, 0)
        u_we.send_across(f)
        return carry

    lax.fori_loop(0, S, chunk_body, 0)
    for b in range(2):
        dxk[b * half : (b + 1) * half, :] = feed_rows(0, b)

    thirds = [wsb.at[pl.ds((j // side) * D, D), pl.ds((j % side) * DT, DT)] for j in range(3)]
    load_wt = [local(wt_f.at[:, pl.ds(j * DT, DT)], thirds[j], loc.at[(9, 11, 12)[j]]) for j in range(3)]
    for c in load_wt:
        c.start()

    gtb = actb.at[:, pl.ds(0, 3 * DT)]
    load_gt = local(gt_i, gtb, loc.at[10])
    load_gt.start()
    for j in range(X):
        to_core(0, j).wait_send()
    load_gt.wait()
    for c in load_wt:
        c.wait()

    def pair(step, f):
        for u in (u_we, u_ws):
            getattr(u, step)(f)

    vsum[...] = jnp.zeros_like(vsum)
    for u in first:
        u.total(0)
    pair("sum_across", 0)

    def slot_grad(i, place, finish):
        for b in range(2):
            at = pl.ds(i * L + b * half, half)
            xhat = layer_norm_rows(xb[place * L + b * half : place * L + (b + 1) * half, :])
            g1 = triple_back(at)
            vsum[0:1, 0:D] += jnp.sum(g1 * xhat, 0, keepdims=True)
            vsum[1:2, 0:D] += jnp.sum(g1, 0, keepdims=True)
            g2 = dot32(ghb[at, :], web[...], NT)
            vsum[2:3, 0:D] += jnp.sum(g2 * xhat, 0, keepdims=True)
            vsum[3:4, 0:D] += jnp.sum(g2, 0, keepdims=True)
            finish(b, g1 * gain1 + g2 * gain2, xhat)

    order = [2 * j + 1 for j in range(X)] + ([2] if X > 1 else []) + [0]
    events = [("sum_across", f) for f in range(S)]
    for turn, i in enumerate(order):
        place = turn % 2
        load_x(i, place).wait()
        if turn + 1 < T:
            load_x(order[turn + 1], 1 - place).start()
        if i % 2 == 1:
            j = i // 2

            def finish(b, val, xhat):
                at = j * L + b * half
                send_b[at : at + half, :] = val.astype(bf16)

            slot_grad(i, place, finish)
            to_core(1, j).start()
            if turn == 0:
                for u in first:
                    u.forward_rep(0)
        elif i == 2:
            to_core(1, 1).wait_recv()

            def finish(b, val, xhat):
                got = dx_r[L + b * half : L + (b + 1) * half, :].astype(f32)
                xs_b[L + b * half : L + (b + 1) * half, :] = (val + got).astype(bf16)

            slot_grad(2, place, finish)
            to_tx(1).start()
            pair("sum_across", 1)
            pair("total", 0)
            for u in first:
                u.forward_tx(0)
            pair("sum_across", 2)
            pair("total", 1)
            pair("forward_rep", 0)
        else:
            to_core(0, 0).wait_recv()
            to_core(1, 0).wait_recv()
            if X > 1:
                to_tx(0).wait_recv()
            for j in range(X):
                to_core(1, j).wait_send()
            for b in range(2):
                rows_b = slice(b * half, (b + 1) * half)
                total = dxk[rows_b, :] + out_r[rows_b, :].astype(f32)
                if X > 1:
                    total = total + out_x[rows_b, :].astype(f32)
                total = total + xb[place * L + b * half : place * L + (b + 1) * half, :].astype(f32)
                send_b[rows_b, :] = (total + (vec[4:5, 0:D] + vec[5:6, 0:D])).astype(bf16)
            save_out = local(send_b.at[pl.ds(0, L)], out_o, loc.at[2])
            save_out.start()

            def finish(b, val, xhat):
                rows_b = slice(b * half, (b + 1) * half)
                dxk[rows_b, :] = val + dx_r[rows_b, :].astype(f32)

            slot_grad(0, place, finish)
            place0 = place
    ones = jnp.ones((8, L), bf16)
    vsum[4:5, 0:D] = dot32(ones, dyb[0:L, :], ONE)[0:1]
    mine = rank(k.tx, k.core)
    eb = dot32(jnp.ones((8, n), bf16), ghb[...], ONE)[0:1]
    for t in range(T):
        @pl.when(mine == t)
        def _():
            vsum[5 + t : 6 + t, 0 : 3 * DT] = tbg[0:1, :]
            vsum[5 + T + t : 6 + T + t, 0:FT] = eb

    def exchange(stage, copies):
        for c in copies:
            c.start()
        for c in copies:
            c.wait()
        for q in range(len(copies)):
            vsum[...] += vrecv[stage + q]

    at_stage = 0
    exchange(0, [remote(vsum, vrecv.at[0], v_s.at[0], v_r.at[0], k.at_core())])
    at_stage = 1
    if X > 1:
        exchange(1, [remote(vsum, vrecv.at[1], v_s.at[1], v_r.at[1], k.at_tx())])
        at_stage = 2
    rep_copies = [
        remote(vsum, vrecv.at[at_stage + dr - 1], v_s.at[at_stage + dr - 1], v_r.at[at_stage + dr - 1], k.at_rep(dr))
        for dr in range(1, R)
    ]
    exchange(at_stage, rep_copies)
    at_stage += R - 1
    z_copies = [
        remote(
            vsum, vrecv.at[at_stage + dz - 1], v_s.at[at_stage + dz - 1], v_r.at[at_stage + dz - 1],
            k.at_z(lax.rem(k.z + dz, S)),
        )
        for dz in range(1, S)
    ]
    for c in z_copies:
        c.start()
    if X == 1:
        for u in first:
            u.forward_tx(0)
        pair("sum_across", 1)
        pair("sum_across", 2)
        pair("total", 0)
        pair("total", 1)
        pair("forward_rep", 0)
    for f in range(3, S):
        pair("sum_across", f)
        pair("total", f - 1)
        pair("forward_rep", f - 2)
        pair("forward_tx", f - 3)
    for c in z_copies:
        c.wait()
    total = vsum[...]
    for q in range(S - 1):
        total = total + vrecv[at_stage + q]
    v_o[...] = total
    if X > 1:
        to_tx(1).wait_recv()
    for b in range(2):
        rows_b = slice(b * half, (b + 1) * half)
        dx = dxk[rows_b, :]
        if X > 1:
            dx = dx + dx_x[rows_b, :].astype(f32)
        xf = xb[place0 * L + b * half : place0 * L + (b + 1) * half, :].astype(f32)
        cen = xf - jnp.mean(xf, -1, keepdims=True)
        rstd = lax.rsqrt(jnp.mean(cen * cen, -1, keepdims=True) + eps_norm)
        xhat = cen * rstd
        back = dx - jnp.mean(dx, -1, keepdims=True) - xhat * jnp.mean(dx * xhat, -1, keepdims=True)
        send_b[L + b * half : L + (b + 1) * half, :] = (dyb[rows_b, :].astype(f32) + rstd * back).astype(bf16)
    save_ing = local(send_b.at[pl.ds(L, L)], ing_o, loc.at[3])
    save_ing.start()
    pair("total", S - 1)
    pair("forward_rep", S - 2)
    pair("forward_tx", S - 3)
    pair("forward_rep", S - 1)
    pair("forward_tx", S - 2)
    pair("forward_tx", S - 1)
    for u in first:
        u.finish(0)
    for f in range(S):
        pair("finish", f)
    if X > 1:
        to_tx(0).wait_send()
        to_tx(1).wait_send()
    save_out.wait()
    save_ing.wait()


def feed_phase(R, X, S, F, xg, dyg, wt_f, wo_f, we_f, ws_f, vecs, ctxT, gt, wtl, wth, wol, woh, tbg, n2):
    T = 2 * X
    n, D = xg.shape
    L = n // T
    DT = S * HEAD_DIM
    FT = we_f.shape[1]
    fs = FT // S
    rows = D // S
    mt, mo, me, ms = rows // R, HEAD_DIM // R, rows // R, fs // R
    W = max(D, 3 * DT, FT)
    sds = jax.ShapeDtypeStruct
    vmem = pltpu.VMEM
    dma = pltpu.SemaphoreType.DMA
    outs = [
        sds((L, D), bf16), sds((L, D), bf16), sds((T * rows, 3 * DT), bf16), sds((rows, D), bf16),
        sds((rows, F), bf16), sds((F // S, D), bf16), sds((16, W), f32),
    ]

    def bufs(count, B, m, cols, lo, landing):
        made = [vmem((count * R * B * m, cols), bf16)] if lo else []
        return made + [
            vmem((count * B * m, cols), f32), vmem((count * (R - 1) * B * m, cols), bf16),
            vmem((count * B * m, cols), bf16), vmem((landing * S * m, cols), bf16), vmem((landing * m, cols), bf16),
        ]

    scratch = [
        vmem((2 * L, D), bf16), vmem((n, D), bf16), vmem((n, D), bf16), vmem((n, FT), bf16), vmem((n, FT), bf16),
        vmem((D, FT), bf16), vmem((FT, D), bf16), vmem((DT, D), bf16),
        vmem((DT, n), bf16),
    ]
    scratch += bufs(1, S, mt, 3 * DT // 2, False, 1) * 2 + bufs(1, S, mo, D, False, 1)
    scratch += bufs(S, S, me, fs, True, S) + bufs(S, 1, ms, D, True, 1)
    scratch += [
        vmem((2 * L, D), bf16), vmem((X * L, D), bf16), vmem((X * L, D), bf16), vmem((2 * L, D), bf16),
        vmem((L, D), bf16), vmem((L, D), bf16), vmem((16, W), f32), vmem((2 + R - 1 + S - 1, 16, W), f32),
    ]
    for count in (1, 1, S, S, 1):
        scratch += grad_sems(count, R, X, S)
    scratch += [dma((15,)), dma((2, 3, 2)), dma((2 + R - 1 + S - 1,)), dma((2 + R - 1 + S - 1,)), vmem((L, D), f32)]
    body = lambda *refs: feed_kernel(R, X, S, L, D, FT, *refs)
    return pl.pallas_call(
        body,
        name="feed_phase",
        out_shape=outs,
        in_specs=[ANY] * 6 + [VM] + [ANY] * 6 + [VM, ANY],
        out_specs=[ANY] * 6 + [VM],
        scratch_shapes=scratch,
        compiler_params=pltpu.CompilerParams(
            collective_id=2, has_side_effects=True, vmem_limit_bytes=67_000_000
        ),
    )(xg, dyg, wt_f, wo_f, we_f, ws_f, vecs, ctxT, gt, wtl, wth, wol, woh, tbg, n2)


def adam_kernel(S, T, heads, *refs):
    g_ref, w_ref, m_ref, v_ref, g_o, w_o, m_o, v_o = refs

    def one(at, g):
        new_w, _, new_m, new_v = adam_step(w_ref[:, at], g, m_ref[:, at], v_ref[:, at], True)
        g_o[:, at] = g
        w_o[:, at] = new_w
        m_o[:, at] = new_m
        v_o[:, at] = new_v

    if not heads:
        one(slice(None), g_ref[...].astype(f32))
        return
    lane = lax.broadcasted_iota(jnp.int32, (1, 128), 1)
    DT = S * HEAD_DIM
    for j in range(3):
        for p in range(S):
            src = j * DT + (p // 2) * 128
            for u in range(T // 2):
                low = g_ref[2 * u, :, src : src + 128].astype(f32)
                high = g_ref[2 * u + 1, :, src : src + 128].astype(f32)
                if p % 2 == 1:
                    low = pltpu.roll(low, HEAD_DIM, 1)
                else:
                    high = pltpu.roll(high, HEAD_DIM, 1)
                to = ((j * S + p) * T + 2 * u) * HEAD_DIM
                one(slice(to, to + 128), jnp.where(lane < HEAD_DIM, low, high))


def adam_matrix(S, T, g, w, m, v, heads, rows_each):
    n, cols = w.shape
    spec = pl.BlockSpec((rows_each, cols), lambda i: (i, 0))
    g_spec = pl.BlockSpec((T, rows_each, g.shape[-1]), lambda i: (0, i, 0)) if heads else spec
    return pl.pallas_call(
        lambda *refs: adam_kernel(S, T, heads, *refs),
        name="adam_matrix",
        grid=(n // rows_each,),
        out_shape=[jax.ShapeDtypeStruct((n, cols), f32)] * 4,
        in_specs=[g_spec, spec, spec, spec],
        out_specs=[spec] * 4,
        compiler_params=pltpu.CompilerParams(vmem_limit_bytes=40 * 1024 * 1024),
    )(g, w, m, v)


TP = ("tx", "core")


def make_step(R, X, S):
    T = 2 * X

    def step(*args):
        x, dy = args[0], args[1]
        masters, momenta, variances = args[2:14], args[14:26], args[26:38]
        L, D = x.shape
        H = D // HEAD_DIM
        t = lax.axis_index(TP)
        z = lax.axis_index("shard")
        rep = lax.axis_index("rep")
        wt, wo, we, ws = masters[4], masters[6], masters[8], masters[10]
        rows = wt.shape[0]
        F = we.shape[1]
        fs = F // S // T
        HT = H // T

        eb_own = lax.dynamic_slice_in_dim(masters[9], t * fs, fs, 0)
        packed = [masters[i] for i in (0, 1, 2, 3, 7, 11)] + [eb_own, masters[5]]
        wide, at, flat = SMALL_ROWS * 128, 0, 0.0
        for v in packed:
            flat = flat + lax.pad(v, jnp.float32(0), [(at, wide - at - v.shape[0], 0)])
            at += v.shape[0]
        small = lax.reduce_precision(flat, 8, 7).reshape(SMALL_ROWS, 128)

        passed = attention_phase(R, X, S, x, dy, wt, wo, we, ws, small, jnp.asarray(rotary_tables(L)))
        out, in_grad, wt_s, wo_s, we_s, ws_s, vec = feed_phase(R, X, S, F, *passed)
        wt_s = wt_s.reshape(T, rows, -1)
        DT, FT = S * HEAD_DIM, F // T
        tb_g = vec[5 : 5 + T, : 3 * DT].reshape(T, 3, S, HEAD_DIM).transpose(1, 2, 0, 3).reshape(-1)
        eb_g = vec[5 + T : 5 + 2 * T, :FT].reshape(T, S, fs).transpose(1, 0, 2).reshape(-1)

        def own(v):
            return lax.dynamic_slice_in_dim(v, z * (v.shape[0] // S), v.shape[0] // S, 0)

        vown = [own(vec[i, :D]) for i in range(5)] + [own(tb_g), own(eb_g)]
        done = {}
        for i, g, each in ((4, wt_s, 64), (6, wo_s, 128), (8, we_s, 64), (10, ws_s, 256)):
            each = min(each, g.shape[-2])
            done[i] = adam_matrix(S, T, g, masters[i], momenta[i], variances[i], i == 4, each)
        summed = [
            vown[0], vown[1], vown[2], vown[3], None, vown[5], None, vown[4], None, vown[6], None, vown[4],
        ]
        updated, ones, twos = [], [], []
        for i in range(12):
            if i in done:
                summed[i] = done[i][0]
                for kept, val in zip((updated, ones, twos), done[i][1:]):
                    kept.append(val)
                continue
            new_weight, delta, m_new, v_new = adam_step(
                masters[i], summed[i], momenta[i], variances[i], i in (4, 6, 8, 10)
            )
            updated.append(delta if i in (0, 2) else new_weight)
            ones.append(m_new)
            twos.append(v_new)
        return (out, in_grad, *summed, *updated, *ones, *twos)

    return step


def solution(mesh):
    G, S = mesh.shape["grp"], mesh.shape["shard"]
    X = 2 if S <= 4 else 1
    R = G // (2 * X)
    full = Mesh(mesh.devices.reshape(R, X, 2, S), ("rep", "tx", "core", "shard"))
    tok = P(("rep", "tx", "core", "shard"), None)
    vecs, mats = P("shard"), P("shard", None)
    group = tuple(mats if i in (4, 6, 8, 10) else vecs for i in range(12))
    return jax.shard_map(
        make_step(R, X, S),
        mesh=full,
        in_specs=(tok, tok) + group * 3,
        out_specs=(tok, tok) + group * 4,
        check_vma=False,
    )
```

```python
import math

import jax
import jax.numpy as jnp
import numpy as np
from jax import lax
from jax.experimental import pallas as pl
from jax.experimental.pallas import tpu as pltpu
from jax.sharding import Mesh, PartitionSpec as P

HEAD_DIM = 64
ROTARY = 16
STEP = 10
eps_norm = 1e-05
rope_base = 10000.0
beta_one = 0.9
beta_two = 0.95
learn_rate = 0.01
adam_eps = 1e-08
weight_decay = 0.01

bf16 = jnp.bfloat16
f32 = jnp.float32


def adam_step(weight, gradient, momentum, variance, decayed):
    momentum_new = beta_one * momentum + (1.0 - beta_one) * gradient
    variance_new = beta_two * variance + (1.0 - beta_two) * gradient * gradient
    mean_hat = momentum_new / (1.0 - beta_one**STEP)
    var_hat = variance_new / (1.0 - beta_two**STEP)
    change = mean_hat / (jnp.sqrt(var_hat) + adam_eps)
    if decayed:
        change = change + weight_decay * weight
    delta = -learn_rate * change
    return (weight + delta, delta, momentum_new, variance_new)


def rotary_tables(length):
    position = np.arange(length, dtype=np.float32)[:, None]
    half = ROTARY // 2
    inverse_freq = np.float32(rope_base) ** (-(np.arange(half, dtype=np.float32) * np.float32(2.0) / np.float32(ROTARY)))
    angles = position * inverse_freq[None, :].astype(np.float32)
    cosine, sine = np.cos(angles), np.sin(angles)
    rest = np.zeros((length, HEAD_DIM - 2 * ROTARY), np.float32)
    head = np.concatenate([cosine, cosine, -sine, sine, rest], 1)
    return np.concatenate([head[: length // 2], head[length // 2 :]], 1).astype(np.float32)


def dot32(a, b, dims):
    return lax.dot_general(a, b, (dims, ((), ())), preferred_element_type=f32)


MESH = pl.DeviceIdType.MESH
ANY = pl.BlockSpec(memory_space=pl.ANY)
VM = pl.BlockSpec(memory_space=pltpu.VMEM)
ONE = ((1,), (0,))
NT = ((1,), (1,))
TN = ((0,), (0,))


def rows_of(start, size):
    return pl.ds(pl.multiple_of(start, math.gcd(size, 512)), size)


class Links:
    def __init__(self, R, X, S):
        self.R, self.X, self.S = R, X, S
        self.rep = lax.axis_index("rep")
        self.tx = lax.axis_index("tx")
        self.core = lax.axis_index("core")
        self.z = lax.axis_index("shard")

    def at_core(self):
        return {"core": 1 - self.core}

    def at_tx(self):
        return {"tx": 1 - self.tx}

    def at_rep(self, dr):
        return {"rep": lax.rem(self.rep + dr, self.R)}

    def at_z(self, z):
        return {"shard": z}

    def barrier(self, every_plane=False):
        sem = pltpu.get_barrier_semaphore()

        def tell(where):
            pl.semaphore_signal(sem, inc=1, device_id=where, device_id_type=MESH)

        count = 1 + (self.X - 1) + (self.R - 1)
        tell(self.at_core())
        if self.X > 1:
            tell(self.at_tx())
        for dr in range(1, self.R):
            tell(self.at_rep(dr))

        if every_plane:
            for dz in range(1, self.S):
                tell(self.at_z(lax.rem(self.z + dz, self.S)))
            pl.semaphore_wait(sem, count + self.S - 1)
            return

        @pl.when(self.z > 0)
        def _():
            tell(self.at_z(self.z - 1))

        @pl.when(self.z < self.S - 1)
        def _():
            tell(self.at_z(self.z + 1))

        ends = (self.z > 0).astype(jnp.int32) + (self.z < self.S - 1).astype(jnp.int32)
        pl.semaphore_wait(sem, count + ends)


def remote(src, dst, send, recv, where):
    return pltpu.make_async_remote_copy(
        src_ref=src, dst_ref=dst, send_sem=send, recv_sem=recv, device_id=where, device_id_type=MESH
    )


def local(src, dst, sem):
    return pltpu.make_async_copy(src, dst, sem)


class LineGather:
    def __init__(self, links, own, buf, n, zs, zr, ys, yr, split):
        self.k = links
        self.own, self.buf, self.n = own, buf, n
        self.parts = links.R if split else 1
        self.m = n // self.parts
        self.zs, self.zr, self.ys, self.yr = zs, zr, ys, yr

    def block(self, p, r):
        return self.buf.at[rows_of(p * self.n + r * self.m, self.m)]

    def mine(self):
        return self.k.rep if self.parts > 1 else 0

    def hop(self, src, p, step, way):
        to = self.k.z + 1 if way == 0 else self.k.z - 1
        return remote(
            src, self.block(p, self.mine()), self.zs.at[step, way], self.zr.at[p], self.k.at_z(to)
        )

    def across(self, p, dr):
        b = self.block(p, self.k.rep)
        return remote(b, b, self.ys.at[p, dr], self.yr.at[p, self.k.rep], self.k.at_rep(dr))

    def each_way(self, step, fn):
        z, S = self.k.z, self.k.S
        for way in (0, 1):
            p = z - step if way == 0 else z + step
            here = (step <= z) if way == 0 else (z + step <= S - 1)
            on = (z < S - 1) if way == 0 else (z > 0)
            fn(way, p, here, on)

    def start(self):
        mine = self.mine()

        def go(way, p, here, on):
            @pl.when(on)
            def _():
                self.hop(self.own.at[rows_of(mine * self.m, self.m)], p, 0, way).start()

        self.each_way(0, go)

    def event(self, step):
        def go(way, p, here, on):
            @pl.when(here)
            def _():
                b = self.block(p, self.mine())
                self.hop(b, p, step, way).wait_recv()

                @pl.when(on)
                def _():
                    self.hop(b, p, step, way).start()

                if self.parts > 1:
                    for dr in range(1, self.k.R):
                        self.across(p, dr).start()

        self.each_way(step, go)

    def arrived(self):
        if self.parts == 1:
            return
        for p in range(self.k.S):
            @pl.when(p != self.k.z)
            def _():
                for dr in range(1, self.k.R):
                    r = lax.rem(self.k.rep + dr, self.k.R)
                    b = self.block(p, r)
                    remote(b, b, self.ys.at[p, dr], self.yr.at[p, r], self.k.at_rep(dr)).wait_recv()

    def drain(self):
        for step in range(self.k.S):
            def go(way, p, here, on):
                @pl.when(jnp.logical_and(here, on))
                def _():
                    self.hop(self.block(p, self.mine()), p, step, way).wait_send()

                if step > 0 and self.parts > 1:
                    @pl.when(here)
                    def _():
                        for dr in range(1, self.k.R):
                            self.across(p, dr).wait_send()

            self.each_way(step, go)


def layer_norm_rows(xb):
    xf = xb.astype(f32)
    cen = xf - jnp.mean(xf, -1, keepdims=True)
    return cen * lax.rsqrt(jnp.mean(cen * cen, -1, keepdims=True) + eps_norm)


SMALL_ROWS = 24


def small_row(sm, S, first, count):
    return jnp.concatenate(
        [sm[p * SMALL_ROWS + first + j : p * SMALL_ROWS + first + j + 1, :] for p in range(S) for j in range(count)],
        -1,
    )


def attention_kernel(R, X, S, L, D, FT, *refs):
    (x_ref, dy_ref, wt_m, wo_m, we_m, ws_m, sm_ref, turn_i) = refs[:8]
    (xg, dyg, wt_o, wo_o, we_o, ws_o, vec_o, ctx_o, gt_o, wtl_o, wth_o, wol_o, woh_o, tbg_o, n2_o) = refs[8:23]
    (
        xs, dys, n1, n2, gt, wtb, wob, smb, q_s, k_s, v_s, gc_s, kT, vT, ctxT, gqT, gk_a, gv_a, wtl, wth, wol, woh, wog,
        turn_s, turn_p, wt_w, wo_w, we_w, ws_w, wt_ref, wo_ref, we_ref, ws_ref,
        zs, zr, ys, yr, tok_s, tok_r, loc, cut,
    ) = refs[23:]
    T = 2 * X
    rows = D // S
    DT = S * HEAD_DIM
    links = Links(R, X, S)
    chunks = []
    for c, (own, buf) in enumerate(
        [(sm_ref, smb), (wt_ref, wtb), (wo_ref, wob), (we_ref, we_o), (ws_ref, ws_o)]
    ):
        chunks.append(
            LineGather(links, own, buf, own.shape[0], zs.at[c], zr.at[c], ys.at[c], yr.at[c], c > 0)
        )
    g_sm, g_wt, g_wo, g_we, g_ws = chunks
    lane = lax.broadcasted_iota(jnp.int32, (1, 128), 1)
    rank = links.tx * 2 + links.core
    fs = FT // S
    cuts = [[], [local(wo_m.at[rows_of(rank * HEAD_DIM, HEAD_DIM)], wo_w, cut.at[3 * S])], [],
            [local(ws_m.at[rows_of(rank * fs, fs)], ws_w, cut.at[3 * S + 1])]]
    for j in range(3):
        for p in range(S):
            block = ((j * S + p) * T + rank) // 2
            cuts[0].append(
                local(
                    wt_m.at[:, pl.ds(pl.multiple_of(block * 128, 128), 128)],
                    wt_w.at[:, pl.ds((j * S + p) * 128, 128)],
                    cut.at[j * S + p],
                )
            )
    for p in range(S):
        cuts[2].append(
            local(
                we_m.at[:, pl.ds(pl.multiple_of((p * T + rank) * fs, fs), fs)],
                we_w.at[:, pl.ds(p * fs, fs)],
                cut.at[3 * S + 2 + p],
            )
        )
    for group in cuts:
        for c in group:
            c.start()
    links.barrier()
    for c in cuts[0]:
        c.wait()

    def half_lanes(block, odd):
        val = wt_w[:, block * 128 : (block + 1) * 128]
        return jnp.where(lax.rem(rank, 2) == odd, val, pltpu.roll(val, HEAD_DIM, 1))

    for b in range(3 * S // 2):
        both = jnp.where(lane < HEAD_DIM, half_lanes(2 * b, 0), half_lanes(2 * b + 1, 1))
        wt_ref[:, b * 128 : (b + 1) * 128] = both.astype(bf16)
    cuts[1][0].wait()
    wo_ref[...] = wo_w[...].astype(bf16)

    own_copies = [
        local(x_ref, xs.at[pl.ds(0, L)], loc.at[0]),
        local(dy_ref, dys.at[pl.ds(0, L)], loc.at[1]),
    ]
    own_copies_late = []
    for c, g in enumerate(chunks):
        (own_copies if c < 3 else own_copies_late).append(local(g.own, g.buf.at[rows_of(links.z * g.n, g.n)], loc.at[2 + c]))

    def token_copy(a, slot):
        buf = (xs, dys)[a]
        src = (x_ref, dy_ref)[a]
        if slot == 1:
            return remote(src, buf.at[pl.ds(L, L)], tok_s.at[a, 1], tok_r.at[a, 1], links.at_core())
        if slot == 2:
            return remote(src, buf.at[pl.ds(2 * L, L)], tok_s.at[a, 2], tok_r.at[a, 2], links.at_tx())
        return remote(
            buf.at[pl.ds(2 * L, L)], buf.at[pl.ds(3 * L, L)], tok_s.at[a, 3], tok_r.at[a, 3], links.at_core()
        )

    g_sm.start()
    g_wt.start()
    g_wo.start()
    if X > 1:
        token_copy(0, 2).start()
        token_copy(1, 2).start()
    token_copy(0, 1).start()
    token_copy(1, 1).start()
    for c in own_copies:
        c.start()

    tables = [local(turn_i, turn_p, cut.at[4 * S + 2])]

    def table(q):
        return jnp.concatenate([turn_s[q * L : (q + 1) * L, :]] * (DT // 128), 1)

    for c in tables:
        c.start()
    for c in cuts[2] + cuts[3]:
        c.wait()
    we_ref[...] = we_w[...].astype(bf16)
    ws_ref[...] = ws_w[...].astype(bf16)
    for c in own_copies_late:
        c.start()
    own_copies[0].wait()
    own_copies[2].wait()
    for step in range(1, S):
        g_sm.event(step)
    per = rows // 128
    vec_o[...] = jnp.zeros_like(vec_o)
    sm = smb[...]
    for j in range(6):
        vec_o[j : j + 1, 0:D] = small_row(sm, S, j * per, per)
    fper = FT // S // 128
    vec_o[8 : 8 + 1, 0:FT] = small_row(sm, S, 6 * per, fper)
    def head_bias(j, p):
        block = j * (D // 128) + (T * p + rank) // 2
        at = (block // (3 * per)) * SMALL_ROWS + 6 * per + fper + lax.rem(block, 3 * per)
        row = smb[pl.ds(at, 1), :]
        return jnp.where(lax.rem(rank, 2) == p % 2, row, pltpu.roll(row, HEAD_DIM, 1))

    for j in range(3):
        for a in range(S // 2):
            both = jnp.where(lane < HEAD_DIM, head_bias(j, 2 * a), head_bias(j, 2 * a + 1))
            vec_o[9 + j : 10 + j, a * 128 : (a + 1) * 128] = both

    def norm_one(i):
        gain, shift = vec_o[0:1, 0:D], vec_o[1:2, 0:D]
        gain_b, shift_b = vec_o[2:3, 0:D], vec_o[3:4, 0:D]

        @pl.loop(0, L // 64)
        def _(b):
            at = rows_of(i * L + b * 64, 64)
            xhat = layer_norm_rows(xs[at, :])
            n1[at, :] = (xhat * gain + shift).astype(bf16)
            n2[at, :] = (xhat * gain_b + shift_b).astype(bf16)

    norm_one(0)
    g_wt.event(1)
    g_wo.event(1)
    g_we.start()
    for step in range(2, S):
        g_wt.event(step)
        g_wo.event(step)
    g_ws.start()
    own_copies[1].wait()
    own_copies[3].wait()
    own_copies[4].wait()
    for c in tables:
        c.wait()
    packed_turn = turn_p[...]
    other_turn = pltpu.roll(packed_turn, HEAD_DIM, 1)
    entry = lax.rem(lane, HEAD_DIM)
    for b in range(2):
        near, far = (packed_turn, other_turn) if b == 0 else (other_turn, packed_turn)
        full = jnp.where(lane < HEAD_DIM, near, far)
        moved = pltpu.roll(full, 128 - ROTARY, 1)
        at = b * (L // 2)
        turn_s[at : at + L // 2, :] = jnp.where(entry < ROTARY, full, 1.0)
        turn_s[L + at : L + at + L // 2, :] = jnp.where(entry < ROTARY // 2, moved, 0.0)
        upper = jnp.logical_and(entry >= ROTARY // 2, entry < ROTARY)
        turn_s[2 * L + at : 2 * L + at + L // 2, :] = jnp.where(upper, moved, 0.0)
    g_wt.arrived()
    g_wo.arrived()
    late = [(g, step) for step in range(1, S) for g in (g_we, g_ws)]

    def pump(i, turn):
        for index in range(T):
            at = 2 * (2 * index + turn) - 2
            todo = late[max(at, 0) : at + 2]
            if todo:
                @pl.when(i == index)
                def _():
                    for g, step in todo:
                        g.event(step)

    half = L // 2
    lane_head = lax.broadcasted_iota(jnp.int32, (1, DT), 1) // HEAD_DIM
    key_at = lax.broadcasted_iota(jnp.int32, (half, half), 0)
    query_at = lax.broadcasted_iota(jnp.int32, (half, half), 1)
    causal = key_at <= query_at

    def slot_body(i, carry):
        here = rows_of(i * L, L)
        for j, dst in enumerate((q_s, k_s, v_s)):
            val = dot32(n1[here, :], wtb[:, j * DT : (j + 1) * DT], ONE) + vec_o[9 + j : 10 + j, 0:DT]
            if j < 2:
                val = (
                    val * table(0)
                    + pltpu.roll(val, DT - 8, 1) * table(1)
                    + pltpu.roll(val, 8, 1) * table(2)
                )
            vb = val.astype(bf16)
            if j == 0:
                q_s[...] = vb * bf16(0.125)
            else:
                dst[...] = vb
                (kT if j == 1 else vT)[...] = vb.T
        gc_s[...] = dot32(dys[here, :], wob[...], NT).astype(bf16)
        gk_a[...] = jnp.zeros_like(gk_a)
        gv_a[...] = jnp.zeros_like(gv_a)
        pump(i, 0)

        def head_body(h, c2):
            mine = (lane_head == h).astype(f32).astype(bf16)
            hrows = rows_of(h * HEAD_DIM, HEAD_DIM)
            for b in range(2):
                qs = pl.ds(b * half, half)
                kl = (b + 1) * half
                km = k_s[0:kl, :] * mine
                sT = dot32(km, q_s[qs, :], NT)
                diag = jnp.where(causal, sT[kl - half :], -1e30)
                sT = diag if b == 0 else jnp.concatenate([sT[: kl - half], diag], 0)
                e = jnp.exp(sT - jnp.max(sT, 0, keepdims=True))
                p = e * (1.0 / jnp.sum(e, 0, keepdims=True))
                pb = p.astype(bf16)
                ctxT[hrows, qs] = dot32(vT[hrows, 0:kl], pb, ONE).astype(bf16)
                gv_a[0:kl, :] += dot32(pb, gc_s[qs, :] * mine, ONE)
                gp = dot32(v_s[0:kl, :] * mine, gc_s[qs, :], NT)
                gs = (p * (gp - jnp.sum(p * gp, 0, keepdims=True))).astype(bf16)
                gk_a[0:kl, :] += dot32(gs, q_s[qs, :] * mine, ONE)
                gqT[hrows, qs] = dot32(kT[hrows, 0:kl], gs, ONE) * 0.125
            return c2

        lax.fori_loop(0, S, head_body, 0)
        pump(i, 1)
        for j in range(3):
            if j == 2:
                val = gv_a[...]
            else:
                val = gqT[...].T if j == 0 else gk_a[...]
                val = (
                    val * table(0)
                    - pltpu.roll(val, DT - 8, 1) * table(1)
                    - pltpu.roll(val, 8, 1) * table(2)
                )
            gt[here, j * DT : (j + 1) * DT] = val.astype(bf16)
        ctx_o[:, rows_of(i * L, L)] = ctxT[...]
        grad = dot32(ctxT[...], dys[here, :], ONE)

        @pl.when(i == 0)
        def _():
            wog[...] = grad

        @pl.when(i > 0)
        def _():
            wog[...] += grad

        if X > 1:
            @pl.when(i == 1)
            def _():
                for a in (0, 1):
                    token_copy(a, 2).wait_recv()
                    token_copy(a, 3).start()

        for nxt in range(1, T):
            @pl.when(i + 1 == nxt)
            def _():
                for a in (0, 1):
                    if nxt != 2:
                        token_copy(a, nxt).wait_recv()

        @pl.when(i + 1 < T)
        def _():
            norm_one(i + 1)

        return carry

    lax.fori_loop(0, T, slot_body, 0)
    outs = [
        local(xs, xg, loc.at[0]),
        local(dys, dyg, loc.at[1]),
        local(wtb, wt_o, loc.at[3]),
        local(wob, wo_o, loc.at[4]),
        local(gt, gt_o, loc.at[7]),
        local(n2, n2_o, loc.at[12]),
    ]
    for o in outs:
        o.start()
    for g, step in late[4 * T - 2 :]:
        g.event(step)
    ones = jnp.ones((8, T * L), bf16)
    tbg_o[...] = dot32(ones, gt[...], ONE)

    m = rows // R

    @pl.loop(0, S)
    def _(p):
        grad = dot32(n1[:, pl.ds(pl.multiple_of(p * rows, rows), rows)], gt[...], TN)
        for r in range(R):
            part = grad[r * m : (r + 1) * m]
            wtl[rows_of((r * S + p) * m, m), :] = part.astype(bf16)

            @pl.when(links.rep == r)
            def _():
                wth[rows_of(p * m, m), :] = part

    mo = HEAD_DIM // R
    for p in range(S):
        for r in range(R):
            part = wog[p * HEAD_DIM + r * mo : p * HEAD_DIM + (r + 1) * mo, :]
            wol[(r * S + p) * mo : (r * S + p + 1) * mo, :] = part.astype(bf16)

            @pl.when(links.rep == r)
            def _():
                woh[p * mo : (p + 1) * mo, :] = part

    last = [
        local(wtl, wtl_o, loc.at[8]),
        local(wth, wth_o, loc.at[9]),
        local(wol, wol_o, loc.at[10]),
        local(woh, woh_o, loc.at[11]),
    ]
    for o in last:
        o.start()
    for c in own_copies_late:
        c.wait()
    g_we.arrived()
    g_ws.arrived()
    for g in chunks:
        g.drain()
    for a in (0, 1):
        for slot in range(1, T):
            token_copy(a, slot).wait_send()
    for o in outs + last:
        o.wait()


def attention_phase(R, X, S, x, dy, wt, wo, we, ws, small, tables):
    L, D = x.shape
    T = 2 * X
    DT = S * HEAD_DIM
    FT = we.shape[1] // T
    fs = FT // S
    rows = D // S
    n = T * L
    sds = jax.ShapeDtypeStruct
    dma = pltpu.SemaphoreType.DMA
    outs = [
        sds((n, D), bf16), sds((n, D), bf16), sds((D, 3 * DT), bf16), sds((DT, D), bf16),
        sds((D, FT), bf16), sds((FT, D), bf16), sds((16, max(D, FT)), f32), sds((DT, n), bf16),
        sds((n, 3 * DT), bf16), sds((D, 3 * DT), bf16), sds((D // R, 3 * DT), f32),
        sds((DT, D), bf16), sds((DT // R, D), f32), sds((8, 3 * DT), f32), sds((n, D), bf16),
    ]
    specs = [ANY] * 6 + [VM, VM] + [ANY] * 5 + [VM, ANY]
    vmem = pltpu.VMEM
    scratch = [
        vmem((n, D), bf16), vmem((n, D), bf16), vmem((n, D), bf16), vmem((n, D), bf16), vmem((n, 3 * DT), bf16),
        vmem((D, 3 * DT), bf16), vmem((DT, D), bf16), vmem((S * SMALL_ROWS, 128), f32),
        vmem((L, DT), bf16), vmem((L, DT), bf16), vmem((L, DT), bf16), vmem((L, DT), bf16),
        vmem((DT, L), bf16), vmem((DT, L), bf16), vmem((DT, L), bf16), vmem((DT, L), f32),
        vmem((L, DT), f32), vmem((L, DT), f32), vmem((D, 3 * DT), bf16), vmem((D // R, 3 * DT), f32),
        vmem((DT, D), bf16), vmem((DT // R, D), f32), vmem((DT, D), f32),
        vmem((3 * L, 128), f32), vmem((L // 2, 128), f32),
        vmem((rows, 3 * S * 128), f32), vmem((HEAD_DIM, D), f32), vmem((rows, FT), f32), vmem((fs, D), f32),
        vmem((rows, 3 * DT), bf16), vmem((HEAD_DIM, D), bf16), vmem((rows, FT), bf16), vmem((fs, D), bf16),
        dma((5, S, 2)), dma((5, S)), dma((5, S, R)), dma((5, S, R)), dma((2, 4)), dma((2, 4)), dma((13,)), dma((4 * S + 5,)),
    ]
    body = lambda *refs: attention_kernel(R, X, S, L, D, FT, *refs)
    return pl.pallas_call(
        body,
        name="attention_phase",
        out_shape=outs,
        in_specs=[ANY] * 8,
        out_specs=specs,
        scratch_shapes=scratch,
        compiler_params=pltpu.CompilerParams(
            collective_id=1, has_side_effects=True, vmem_limit_bytes=60 * 1024 * 1024
        ),
    )(x, dy, wt, wo, we, ws, small, tables)


class GradSum:
    def __init__(self, links, blocks, m, bufs, sems, piece, only=None):
        self.k, self.B, self.m = links, blocks, m
        self.lo, self.keep, self.yr, self.zs, self.zr, self.fin = bufs
        self.sems, self.piece, self.only = sems, piece, only

    def across(self, f, dr):
        size = self.B * self.m
        r = lax.rem(self.k.rep + dr, self.k.R)
        return remote(
            self.lo.at[rows_of((f * self.k.R + r) * size, size)],
            self.yr.at[rows_of((f * (self.k.R - 1) + dr - 1) * size, size)],
            self.sems["ys"].at[f, dr], self.sems["yr"].at[f, dr], self.k.at_rep(dr),
        )

    def send_across(self, f):
        for dr in range(1, self.k.R):
            self.across(f, dr).start()

    def toward(self, f, p):
        b = 0 if self.only else p
        to = self.zr.at[rows_of(((0 if self.only else f) * self.k.S + self.k.z) * self.m, self.m)]
        return remote(
            self.zs.at[rows_of((f * self.B + b) * self.m, self.m)], to,
            self.sems["zs"].at[f, p], self.sems["zr"].at[f, self.k.z], self.k.at_z(p),
        )

    def owners(self, f, fn):
        if self.only:
            @pl.when(f != self.k.z)
            def _():
                fn(f)
        else:
            for dp in range(1, self.k.S):
                fn(lax.rem(self.k.z + dp, self.k.S))

    def if_owner(self, f, fn):
        if self.only:
            pl.when(f == self.k.z)(fn)
        else:
            fn()

    def sum_across(self, f):
        R, m = self.k.R, self.m
        for dr in range(1, R):
            self.across(f, dr).wait_recv()

        for b in range(self.B):
            at = rows_of((f * self.B + b) * m, m)
            total = self.keep[at, :]
            for dr in range(1, R):
                got = rows_of(((f * (R - 1) + dr - 1) * self.B + b) * m, m)
                total = total + self.yr[got, :].astype(f32)
            self.keep[at, :] = total
            self.zs[at, :] = total.astype(bf16)

        self.owners(f, lambda p: self.toward(f, p).start())

    def total(self, f):
        S, m = self.k.S, self.m

        def go():
            g = 0 if self.only else f
            at = rows_of((f * self.B + (0 if self.only else self.k.z)) * m, m)
            total = self.keep[at, :]
            for dp in range(1, S):
                p = lax.rem(self.k.z + dp, S)
                src = self.zr.at[rows_of((g * S + p) * m, m)]
                remote(src, src, self.sems["zs"].at[f, p], self.sems["zr"].at[f, p], self.k.at_z(p)).wait_recv()
                total = total + self.zr[rows_of((g * S + p) * m, m), :].astype(f32)
            fin = rows_of(g * m, m)
            self.fin[fin, :] = total.astype(bf16)
            src = self.fin.at[fin]
            local(src, self.piece(f, self.k.tx, self.k.core, self.k.rep), self.sems["gl"].at[f]).start()
            for c in self.spread(f, src, self.k.tx, self.k.rep, 0):
                c.start()

        self.if_owner(f, go)

    def spread(self, f, src, tx, r, stage):
        dst = self.piece(f, tx, self.k.core, r)
        src = dst if src is None else src
        out = []
        other = 1 if stage == 2 else 0
        out.append(
            remote(src, dst, self.sems["gcs"].at[f, other, r], self.sems["gcr"].at[f, other, r], self.k.at_core())
        )
        if stage < 2 and self.k.X > 1:
            out.append(remote(src, dst, self.sems["gxs"].at[f, r], self.sems["gxr"].at[f, r], self.k.at_tx()))
        if stage == 0:
            for dr in range(1, self.k.R):
                out.append(remote(src, dst, self.sems["gys"].at[f, dr], self.sems["gyr"].at[f, r], self.k.at_rep(dr)))
        return out

    def replicas(self, fn):
        for dr in range(1, self.k.R):
            fn(dr, lax.rem(self.k.rep + dr, self.k.R))

    def forward_rep(self, f):
        def go():
            def one(dr, r):
                b = self.piece(f, self.k.tx, self.k.core, r)
                remote(b, b, self.sems["gys"].at[f, dr], self.sems["gyr"].at[f, r], self.k.at_rep(dr)).wait_recv()
                for c in self.spread(f, None, self.k.tx, r, 1):
                    c.start()

            self.replicas(one)

        self.if_owner(f, go)

    def forward_tx(self, f):
        if self.k.X == 1:
            return

        def go():
            for r in range(self.k.R):
                b = self.piece(f, 1 - self.k.tx, self.k.core, r)
                remote(b, b, self.sems["gxs"].at[f, r], self.sems["gxr"].at[f, r], self.k.at_tx()).wait_recv()
                for c in self.spread(f, None, 1 - self.k.tx, r, 2):
                    c.start()

        self.if_owner(f, go)

    def finish(self, f):
        for dr in range(1, self.k.R):
            self.across(f, dr).wait_send()
        self.owners(f, lambda p: self.toward(f, p).wait_send())

        def go():
            src = self.fin.at[rows_of((0 if self.only else f) * self.m, self.m)]
            local(src, self.piece(f, self.k.tx, self.k.core, self.k.rep), self.sems["gl"].at[f]).wait()
            for c in self.spread(f, src, self.k.tx, self.k.rep, 0):
                c.wait_send()
            self.replicas(lambda dr, r: [c.wait_send() for c in self.spread(f, None, self.k.tx, r, 1)])
            for other in range(self.k.X):
                tx = self.k.tx if other == 0 else 1 - self.k.tx
                for r in range(self.k.R):
                    if other == 1:
                        for c in self.spread(f, None, tx, r, 2):
                            c.wait_send()
                    b = self.piece(f, tx, 1 - self.k.core, r)
                    remote(
                        b, b, self.sems["gcs"].at[f, other, r], self.sems["gcr"].at[f, other, r], self.k.at_core()
                    ).wait_recv()

        self.if_owner(f, go)


SEM_NAMES = ("ys", "yr", "zs", "zr", "gl", "gcs", "gcr", "gxs", "gxr", "gys", "gyr")


def grad_sems(count, R, X, S):
    dma = pltpu.SemaphoreType.DMA
    return [
        dma((count, R)), dma((count, R)), dma((count, S)), dma((count, S)), dma((count,)),
        dma((count, 2, R)), dma((count, 2, R)), dma((count, R)), dma((count, R)), dma((count, R)), dma((count, R)),
    ]


def feed_kernel(R, X, S, L, D, FT, *refs):
    (xg, dyg, wt_f, wo_f, we_f, ws_f, vec, ctx_i, gt_i, wtl, wth, wol, woh, tbg, n2_i) = refs[:15]
    (out_o, ing_o, g_wt, g_wo, g_we, g_ws, v_o) = refs[15:22]
    rest = list(refs[22:])
    take = lambda count: [rest.pop(0) for _ in range(count)]
    (xb, dyb, n2b, actb, ghb, web, wsb, wob, ctb) = take(9)
    wt_bufs, wt2_bufs, wo_bufs, we_bufs, ws_bufs = take(5), take(5), take(5), take(6), take(6)
    (send_b, out_r, dx_r, xs_b, out_x, dx_x, vsum, vrecv) = take(8)
    sem_sets = [dict(zip(SEM_NAMES, take(len(SEM_NAMES)))) for _ in range(5)]
    (loc, tok, v_s, v_r, dxk) = take(5)
    T = 2 * X
    n = T * L
    rows = D // S
    DT = S * HEAD_DIM
    fs = FT // S
    k = Links(R, X, S)
    k.barrier(every_plane=True)
    rank = lambda tx, core: tx * 2 + core
    mt, mo, me, ms = rows // R, HEAD_DIM // R, rows // R, fs // R
    wide = 3 * DT // 2

    def triple_half(c, bufs, sems):
        cols = pl.ds(c * wide, wide)
        return GradSum(k, S, mt, [wtl.at[:, cols]] + bufs, sems,
                       lambda f, tx, core, r: g_wt.at[rows_of(rank(tx, core) * rows + r * mt, mt), cols])

    u_wt, u_wt2 = triple_half(0, wt_bufs, sem_sets[0]), triple_half(1, wt2_bufs, sem_sets[4])
    u_wo = GradSum(k, S, mo, [wol] + wo_bufs, sem_sets[1],
                   lambda f, tx, c, r: g_wo.at[rows_of(rank(tx, c) * HEAD_DIM + r * mo, mo)])
    u_we = GradSum(k, S, me, we_bufs, sem_sets[2],
                   lambda f, tx, c, r: g_we.at[rows_of(r * me, me), rows_of((f * T + rank(tx, c)) * fs, fs)])
    u_ws = GradSum(k, 1, ms, ws_bufs, sem_sets[3],
                   lambda f, tx, c, r: g_ws.at[rows_of(rank(tx, c) * fs + r * ms, ms)], only=True)
    first = (u_wo, u_wt, u_wt2)
    for u in first:
        u.send_across(0)

    def load_x(i, place):
        return local(xg.at[rows_of(i * L, L)], xb.at[pl.ds(place * L, L)], loc.at[place])

    load_x(1, 0).start()
    loads = [
        local(we_f, web, loc.at[2]), local(n2_i, n2b, loc.at[1 + 12]), local(dyg, dyb, loc.at[3]), local(ws_f, wsb, loc.at[4]),
        local(wo_f, wob, loc.at[5]), local(ctx_i, ctb, loc.at[6]),
        local(woh, wo_bufs[0], loc.at[8]),
        local(wth.at[:, pl.ds(0, wide)], wt_bufs[0], loc.at[7]),
        local(wth.at[:, pl.ds(wide, wide)], wt2_bufs[0], loc.at[14]),
    ]
    for c in loads:
        c.start()

    gain1, gain2 = vec[0:1, 0:D], vec[2:3, 0:D]
    for c in loads[:4]:
        c.wait()
    for c in loads[6:9]:
        c.wait()
    early = {T * S // 4: u_wo, T * S // 2: u_wt, T * S - 1: u_wt2}

    def hidden_body(it, carry):
        i, f = it // S, lax.rem(it, S)
        here, cols = rows_of(i * L, L), pl.ds(pl.multiple_of(f * fs, fs), fs)
        h = dot32(n2b[here, :], web[:, cols], ONE) + vec[8:9, cols]
        cdf = 0.5 * (1.0 + lax.erf(h * math.sqrt(0.5)))
        actb[here, cols] = (h * cdf).astype(bf16)
        slope = cdf + h * (jnp.exp(-0.5 * h * h) * (1.0 / math.sqrt(2.0 * math.pi)))
        ghb[here, cols] = (dot32(dyb[here, :], wsb[cols, :], NT) * slope).astype(bf16)
        for turn, u in early.items():
            @pl.when(it == turn)
            def _():
                u.sum_across(0)
        return carry

    lax.fori_loop(0, T * S, hidden_body, 0)
    loads[4].wait()
    loads[5].wait()
    half = L // 2

    def feed_rows(i, b):
        at = i * L + b * half
        return dot32(actb[at : at + half, :], wsb[...], ONE) + dot32(ctb[:, at : at + half], wob[...], TN)

    def to_core(which, j):
        land = (out_r, dx_r)[which]
        return remote(
            send_b.at[pl.ds(j * L, L)], land.at[pl.ds(j * L, L)],
            tok.at[which, 0, j], tok.at[which, 1, j], k.at_core(),
        )

    def to_tx(which):
        return remote(
            xs_b.at[pl.ds(which * L, L)], (out_x, dx_x)[which], tok.at[which, 2, 0], tok.at[which, 2, 1], k.at_tx()
        )

    for j in range(X):
        for b in range(2):
            at = j * L + b * half
            send_b[at : at + half, :] = feed_rows(2 * j + 1, b).astype(bf16)
        to_core(0, j).start()
    if X > 1:
        to_core(0, 1).wait_recv()
        for b in range(2):
            got = out_r[L + b * half : L + (b + 1) * half, :].astype(f32)
            xs_b[b * half : (b + 1) * half, :] = (feed_rows(2, b) + got).astype(bf16)
        to_tx(0).start()

    side = D // DT

    def triple_back(at):
        total = None
        for j in range(0, 3, side):
            wide = min(side, 3 - j)
            part = dot32(
                actb[at, j * DT : (j + wide) * DT], wsb[(j // side) * D : (j // side + 1) * D, 0 : wide * DT], NT
            )
            total = part if total is None else total + part
        return total

    def store_grad(u, f, block, grad):
        for r in range(R):
            part = grad[r * u.m : (r + 1) * u.m]
            u.lo[rows_of(((f * R + r) * u.B + block) * u.m, u.m), :] = part.astype(bf16)

            @pl.when(k.rep == r)
            def _():
                u.keep[rows_of((f * u.B + block) * u.m, u.m), :] = part

    def chunk_body(f, carry):
        cols = pl.ds(pl.multiple_of(f * fs, fs), fs)
        store_grad(u_ws, f, 0, dot32(actb[:, cols], dyb[...], TN))
        u_ws.send_across(f)
        return carry

    def expand_body(f, carry):
        cols = pl.ds(pl.multiple_of(f * fs, fs), fs)

        def block_body(p, c2):
            grad = dot32(n2b[:, pl.ds(pl.multiple_of(p * rows, rows), rows)], ghb[:, cols], TN)
            store_grad(u_we, f, p, grad)
            return c2

        lax.fori_loop(0, S, block_body, 0)
        u_we.send_across(f)
        return carry

    lax.fori_loop(0, S, chunk_body, 0)
    lax.fori_loop(0, S, expand_body, 0)
    for b in range(2):
        dxk[b * half : (b + 1) * half, :] = feed_rows(0, b)

    thirds = [wsb.at[pl.ds((j // side) * D, D), pl.ds((j % side) * DT, DT)] for j in range(3)]
    load_wt = [local(wt_f.at[:, pl.ds(j * DT, DT)], thirds[j], loc.at[(9, 11, 12)[j]]) for j in range(3)]
    for c in load_wt:
        c.start()

    gtb = actb.at[:, pl.ds(0, 3 * DT)]
    load_gt = local(gt_i, gtb, loc.at[10])
    load_gt.start()
    for j in range(X):
        to_core(0, j).wait_send()
    load_gt.wait()
    for c in load_wt:
        c.wait()

    queue = [(u_ws, f) for f in range(S)] + [(u_we, f) for f in range(S)]

    def pair(step, stage):
        for u, f in queue[2 * stage : 2 * stage + 2]:
            getattr(u, step)(f)

    vsum[...] = jnp.zeros_like(vsum)
    for u in first:
        u.total(0)
    pair("sum_across", 0)

    def slot_grad(i, place, finish):
        for b in range(2):
            at = pl.ds(i * L + b * half, half)
            xhat = layer_norm_rows(xb[place * L + b * half : place * L + (b + 1) * half, :])
            g1 = triple_back(at)
            vsum[0:1, 0:D] += jnp.sum(g1 * xhat, 0, keepdims=True)
            vsum[1:2, 0:D] += jnp.sum(g1, 0, keepdims=True)
            g2 = dot32(ghb[at, :], web[...], NT)
            vsum[2:3, 0:D] += jnp.sum(g2 * xhat, 0, keepdims=True)
            vsum[3:4, 0:D] += jnp.sum(g2, 0, keepdims=True)
            finish(b, g1 * gain1 + g2 * gain2, xhat)

    order = [2 * j + 1 for j in range(X)] + ([2] if X > 1 else []) + [0]
    events = [("sum_across", f) for f in range(S)]
    for turn, i in enumerate(order):
        place = turn % 2
        load_x(i, place).wait()
        if turn + 1 < T:
            load_x(order[turn + 1], 1 - place).start()
        if i % 2 == 1:
            j = i // 2

            def finish(b, val, xhat):
                at = j * L + b * half
                send_b[at : at + half, :] = val.astype(bf16)

            slot_grad(i, place, finish)
            to_core(1, j).start()
            if turn == 0:
                for u in first:
                    u.forward_rep(0)
        elif i == 2:
            to_core(1, 1).wait_recv()

            def finish(b, val, xhat):
                got = dx_r[L + b * half : L + (b + 1) * half, :].astype(f32)
                xs_b[L + b * half : L + (b + 1) * half, :] = (val + got).astype(bf16)

            slot_grad(2, place, finish)
            to_tx(1).start()
            pair("sum_across", 1)
            pair("total", 0)
            for u in first:
                u.forward_tx(0)
            pair("sum_across", 2)
            pair("total", 1)
            pair("forward_rep", 0)
        else:
            to_core(0, 0).wait_recv()
            to_core(1, 0).wait_recv()
            if X > 1:
                to_tx(0).wait_recv()
            for j in range(X):
                to_core(1, j).wait_send()
            for b in range(2):
                rows_b = slice(b * half, (b + 1) * half)
                total = dxk[rows_b, :] + out_r[rows_b, :].astype(f32)
                if X > 1:
                    total = total + out_x[rows_b, :].astype(f32)
                total = total + xb[place * L + b * half : place * L + (b + 1) * half, :].astype(f32)
                send_b[rows_b, :] = (total + (vec[4:5, 0:D] + vec[5:6, 0:D])).astype(bf16)
            save_out = local(send_b.at[pl.ds(0, L)], out_o, loc.at[2])
            save_out.start()

            def finish(b, val, xhat):
                rows_b = slice(b * half, (b + 1) * half)
                dxk[rows_b, :] = val + dx_r[rows_b, :].astype(f32)

            slot_grad(0, place, finish)
            place0 = place
    ones = jnp.ones((8, L), bf16)
    vsum[4:5, 0:D] = dot32(ones, dyb[0:L, :], ONE)[0:1]
    mine = rank(k.tx, k.core)
    eb = dot32(jnp.ones((8, n), bf16), ghb[...], ONE)[0:1]
    for t in range(T):
        @pl.when(mine == t)
        def _():
            vsum[5 + t : 6 + t, 0 : 3 * DT] = tbg[0:1, :]
            vsum[5 + T + t : 6 + T + t, 0:FT] = eb

    def exchange(stage, copies):
        for c in copies:
            c.start()
        for c in copies:
            c.wait()
        for q in range(len(copies)):
            vsum[...] += vrecv[stage + q]

    at_stage = 0
    exchange(0, [remote(vsum, vrecv.at[0], v_s.at[0], v_r.at[0], k.at_core())])
    at_stage = 1
    if X > 1:
        exchange(1, [remote(vsum, vrecv.at[1], v_s.at[1], v_r.at[1], k.at_tx())])
        at_stage = 2
    rep_copies = [
        remote(vsum, vrecv.at[at_stage + dr - 1], v_s.at[at_stage + dr - 1], v_r.at[at_stage + dr - 1], k.at_rep(dr))
        for dr in range(1, R)
    ]
    exchange(at_stage, rep_copies)
    at_stage += R - 1
    z_copies = [
        remote(
            vsum, vrecv.at[at_stage + dz - 1], v_s.at[at_stage + dz - 1], v_r.at[at_stage + dz - 1],
            k.at_z(lax.rem(k.z + dz, S)),
        )
        for dz in range(1, S)
    ]
    for c in z_copies:
        c.start()
    if X == 1:
        for u in first:
            u.forward_tx(0)
        pair("sum_across", 1)
        pair("sum_across", 2)
        pair("total", 0)
        pair("total", 1)
        pair("forward_rep", 0)
    for f in range(3, S):
        pair("sum_across", f)
        pair("total", f - 1)
        pair("forward_rep", f - 2)
        pair("forward_tx", f - 3)
    for c in z_copies:
        c.wait()
    total = vsum[...]
    for q in range(S - 1):
        total = total + vrecv[at_stage + q]
    v_o[...] = total
    if X > 1:
        to_tx(1).wait_recv()
    for b in range(2):
        rows_b = slice(b * half, (b + 1) * half)
        dx = dxk[rows_b, :]
        if X > 1:
            dx = dx + dx_x[rows_b, :].astype(f32)
        xf = xb[place0 * L + b * half : place0 * L + (b + 1) * half, :].astype(f32)
        cen = xf - jnp.mean(xf, -1, keepdims=True)
        rstd = lax.rsqrt(jnp.mean(cen * cen, -1, keepdims=True) + eps_norm)
        xhat = cen * rstd
        back = dx - jnp.mean(dx, -1, keepdims=True) - xhat * jnp.mean(dx * xhat, -1, keepdims=True)
        send_b[L + b * half : L + (b + 1) * half, :] = (dyb[rows_b, :].astype(f32) + rstd * back).astype(bf16)
    save_ing = local(send_b.at[pl.ds(L, L)], ing_o, loc.at[3])
    save_ing.start()
    pair("total", S - 1)
    pair("forward_rep", S - 2)
    pair("forward_tx", S - 3)
    pair("forward_rep", S - 1)
    pair("forward_tx", S - 2)
    pair("forward_tx", S - 1)
    for u in first:
        u.finish(0)
    for f in range(S):
        pair("finish", f)
    if X > 1:
        to_tx(0).wait_send()
        to_tx(1).wait_send()
    save_out.wait()
    save_ing.wait()


def feed_phase(R, X, S, F, xg, dyg, wt_f, wo_f, we_f, ws_f, vecs, ctxT, gt, wtl, wth, wol, woh, tbg, n2):
    T = 2 * X
    n, D = xg.shape
    L = n // T
    DT = S * HEAD_DIM
    FT = we_f.shape[1]
    fs = FT // S
    rows = D // S
    mt, mo, me, ms = rows // R, HEAD_DIM // R, rows // R, fs // R
    W = max(D, 3 * DT, FT)
    sds = jax.ShapeDtypeStruct
    vmem = pltpu.VMEM
    dma = pltpu.SemaphoreType.DMA
    outs = [
        sds((L, D), bf16), sds((L, D), bf16), sds((T * rows, 3 * DT), bf16), sds((rows, D), bf16),
        sds((rows, F), bf16), sds((F // S, D), bf16), sds((16, W), f32),
    ]

    def bufs(count, B, m, cols, lo, landing):
        made = [vmem((count * R * B * m, cols), bf16)] if lo else []
        return made + [
            vmem((count * B * m, cols), f32), vmem((count * (R - 1) * B * m, cols), bf16),
            vmem((count * B * m, cols), bf16), vmem((landing * S * m, cols), bf16), vmem((landing * m, cols), bf16),
        ]

    scratch = [
        vmem((2 * L, D), bf16), vmem((n, D), bf16), vmem((n, D), bf16), vmem((n, FT), bf16), vmem((n, FT), bf16),
        vmem((D, FT), bf16), vmem((FT, D), bf16), vmem((DT, D), bf16),
        vmem((DT, n), bf16),
    ]
    scratch += bufs(1, S, mt, 3 * DT // 2, False, 1) * 2 + bufs(1, S, mo, D, False, 1)
    scratch += bufs(S, S, me, fs, True, S) + bufs(S, 1, ms, D, True, 1)
    scratch += [
        vmem((2 * L, D), bf16), vmem((X * L, D), bf16), vmem((X * L, D), bf16), vmem((2 * L, D), bf16),
        vmem((L, D), bf16), vmem((L, D), bf16), vmem((16, W), f32), vmem((2 + R - 1 + S - 1, 16, W), f32),
    ]
    for count in (1, 1, S, S, 1):
        scratch += grad_sems(count, R, X, S)
    scratch += [dma((15,)), dma((2, 3, 2)), dma((2 + R - 1 + S - 1,)), dma((2 + R - 1 + S - 1,)), vmem((L, D), f32)]
    body = lambda *refs: feed_kernel(R, X, S, L, D, FT, *refs)
    return pl.pallas_call(
        body,
        name="feed_phase",
        out_shape=outs,
        in_specs=[ANY] * 6 + [VM] + [ANY] * 6 + [VM, ANY],
        out_specs=[ANY] * 6 + [VM],
        scratch_shapes=scratch,
        compiler_params=pltpu.CompilerParams(
            collective_id=2, has_side_effects=True, vmem_limit_bytes=67_000_000
        ),
    )(xg, dyg, wt_f, wo_f, we_f, ws_f, vecs, ctxT, gt, wtl, wth, wol, woh, tbg, n2)


def adam_kernel(S, T, heads, *refs):
    g_ref, w_ref, m_ref, v_ref, g_o, w_o, m_o, v_o = refs

    def one(at, g):
        new_w, _, new_m, new_v = adam_step(w_ref[:, at], g, m_ref[:, at], v_ref[:, at], True)
        g_o[:, at] = g
        w_o[:, at] = new_w
        m_o[:, at] = new_m
        v_o[:, at] = new_v

    if not heads:
        one(slice(None), g_ref[...].astype(f32))
        return
    lane = lax.broadcasted_iota(jnp.int32, (1, 128), 1)
    DT = S * HEAD_DIM
    for j in range(3):
        for p in range(S):
            src = j * DT + (p // 2) * 128
            for u in range(T // 2):
                low = g_ref[2 * u, :, src : src + 128].astype(f32)
                high = g_ref[2 * u + 1, :, src : src + 128].astype(f32)
                if p % 2 == 1:
                    low = pltpu.roll(low, HEAD_DIM, 1)
                else:
                    high = pltpu.roll(high, HEAD_DIM, 1)
                to = ((j * S + p) * T + 2 * u) * HEAD_DIM
                one(slice(to, to + 128), jnp.where(lane < HEAD_DIM, low, high))


def adam_matrix(S, T, g, w, m, v, heads, rows_each):
    n, cols = w.shape
    spec = pl.BlockSpec((rows_each, cols), lambda i: (i, 0))
    g_spec = pl.BlockSpec((T, rows_each, g.shape[-1]), lambda i: (0, i, 0)) if heads else spec
    return pl.pallas_call(
        lambda *refs: adam_kernel(S, T, heads, *refs),
        name="adam_matrix",
        grid=(n // rows_each,),
        out_shape=[jax.ShapeDtypeStruct((n, cols), f32)] * 4,
        in_specs=[g_spec, spec, spec, spec],
        out_specs=[spec] * 4,
        compiler_params=pltpu.CompilerParams(vmem_limit_bytes=40 * 1024 * 1024),
    )(g, w, m, v)


TP = ("tx", "core")


def make_step(R, X, S):
    T = 2 * X

    def step(*args):
        x, dy = args[0], args[1]
        masters, momenta, variances = args[2:14], args[14:26], args[26:38]
        L, D = x.shape
        H = D // HEAD_DIM
        t = lax.axis_index(TP)
        z = lax.axis_index("shard")
        rep = lax.axis_index("rep")
        wt, wo, we, ws = masters[4], masters[6], masters[8], masters[10]
        rows = wt.shape[0]
        F = we.shape[1]
        fs = F // S // T
        HT = H // T

        eb_own = lax.dynamic_slice_in_dim(masters[9], t * fs, fs, 0)
        packed = [masters[i] for i in (0, 1, 2, 3, 7, 11)] + [eb_own, masters[5]]
        wide, at, flat = SMALL_ROWS * 128, 0, 0.0
        for v in packed:
            flat = flat + lax.pad(v, jnp.float32(0), [(at, wide - at - v.shape[0], 0)])
            at += v.shape[0]
        small = lax.reduce_precision(flat, 8, 7).reshape(SMALL_ROWS, 128)

        passed = attention_phase(R, X, S, x, dy, wt, wo, we, ws, small, jnp.asarray(rotary_tables(L)))
        out, in_grad, wt_s, wo_s, we_s, ws_s, vec = feed_phase(R, X, S, F, *passed)
        wt_s = wt_s.reshape(T, rows, -1)
        DT, FT = S * HEAD_DIM, F // T
        tb_g = vec[5 : 5 + T, : 3 * DT].reshape(T, 3, S, HEAD_DIM).transpose(1, 2, 0, 3).reshape(-1)
        eb_g = vec[5 + T : 5 + 2 * T, :FT].reshape(T, S, fs).transpose(1, 0, 2).reshape(-1)

        def own(v):
            return lax.dynamic_slice_in_dim(v, z * (v.shape[0] // S), v.shape[0] // S, 0)

        vown = [own(vec[i, :D]) for i in range(5)] + [own(tb_g), own(eb_g)]
        done = {}
        for i, g, each in ((4, wt_s, 64), (6, wo_s, 128), (8, we_s, 64), (10, ws_s, 256)):
            each = min(each, g.shape[-2])
            done[i] = adam_matrix(S, T, g, masters[i], momenta[i], variances[i], i == 4, each)
        summed = [
            vown[0], vown[1], vown[2], vown[3], None, vown[5], None, vown[4], None, vown[6], None, vown[4],
        ]
        updated, ones, twos = [], [], []
        for i in range(12):
            if i in done:
                summed[i] = done[i][0]
                for kept, val in zip((updated, ones, twos), done[i][1:]):
                    kept.append(val)
                continue
            new_weight, delta, m_new, v_new = adam_step(
                masters[i], summed[i], momenta[i], variances[i], i in (4, 6, 8, 10)
            )
            updated.append(delta if i in (0, 2) else new_weight)
            ones.append(m_new)
            twos.append(v_new)
        return (out, in_grad, *summed, *updated, *ones, *twos)

    return step


def solution(mesh):
    G, S = mesh.shape["grp"], mesh.shape["shard"]
    X = 2 if S <= 4 else 1
    R = G // (2 * X)
    full = Mesh(mesh.devices.reshape(R, X, 2, S), ("rep", "tx", "core", "shard"))
    tok = P(("rep", "tx", "core", "shard"), None)
    vecs, mats = P("shard"), P("shard", None)
    group = tuple(mats if i in (4, 6, 8, 10) else vecs for i in range(12))
    return jax.shard_map(
        make_step(R, X, S),
        mesh=full,
        in_specs=(tok, tok) + group * 3,
        out_specs=(tok, tok) + group * 4,
        check_vma=False,
    )
```
